32 devices in a mesh: groups: 2 (over x), inst: 4 (over z), tp: 4 (over y, core).
Axes of the slice: x: 2, y: 2, z: 4, core: 2. Of those that a mesh axis runs over, the one named last changes fastest.
Arguments:
- qkv_first: bfloat16 [48, 10240], P(('groups', 'inst'), 'tp'), parts along dimension 0, may hold values from -5 to 5
- qkv_second: bfloat16 [48, 10240], P(('groups', 'inst'), 'tp'), parts along dimension 0, may hold values from -5 to 5
- w_out: bfloat16 [8192, 8192], P(None, 'tp'), may hold values from -0.5 to 0.5
- kv_cache: bfloat16 [512, 2, 16, 1024], P(('groups', 'inst', 'tp')), parts along dimension 0, may hold values from -4096 to 4096
- lengths: int32 [48], P('groups'), parts along dimension 0, may hold values from 4 to 126, as said below
- page_table: int32 [48, 8], P(('groups', 'inst')), parts along dimension 0, may hold values from -1 to 63, as said below
- moves: int32 [8, 2], P('groups'), parts along dimension 0, may hold values from 0 to 23, as said below
- dest_pages: int32 [8, 8], P('groups'), parts along dimension 0, may hold values from 0 to 63, as said below
Outputs:
- out_first: bfloat16 [48, 8192], P(('groups', 'inst'), 'tp'), parts along dimension 0
- out_second: bfloat16 [48, 8192], P(('groups', 'inst'), 'tp'), parts along dimension 0
- kv_out: bfloat16 [512, 2, 16, 1024], P(('groups', 'inst', 'tp')), parts along dimension 0
The draws below stay inside these ranges and needn't reach their ends.
There are 2 independent parts, one for each index of `groups`. The reference program is written for one: setup_inputs(seed, part) draws one part's arguments, and reference() takes and returns one part's arrays. A program takes and returns all parts, laid end to end along the dimension named above; an argument that names none is the same for every part. Nothing has to cross between parts.
Inputs may be any that keep to these rules, and one draw needn't show every extreme that they name: Half of the instances, drawn afresh, are heavy: lengths of their requests run from 64 to 126, those of the other instances from 4 to 16. Entry j of request r is a page of its instance's pool for j < ceil((lengths[r] + 2) / 16) and -1 after; such a page p has floor(p / 16) = j mod (4); no pool page is named twice by page_table and dest_pages together. Row i moves request moves[i, 0], a number from 0 to 23, to instance moves[i, 1], a number from 0 to 3; every heavy instance sends exactly one request to every other instance, those are the light ones, and a moved request's length is at least (7) * 16 - 1. `dest_pages`: entry j of row i, for every j < 8, is a page p of the destination's pool that page_table leaves free, with floor(p / 16) = j mod (4).
All inputs are finite; a program needn't handle non-finite values.
Results may differ from the reference program's by a relative error of at most 0.015.
Values may be sent and summed in bfloat16 or wider, within the bound.
No kernel may reach another device: no remote copies, remote signals or barrier semaphores. Data moves between devices by JAX's collectives and lax.ppermute only.
A program may use at most 64 MiB of HBM per device.

```python
import math
from functools import partial
import jax
import jax.numpy as jnp
from jax import lax

D = 8192
QUERY_HEADS = 64
KEY_VALUE_HEADS = 8
HEAD_SIZE = 128
PAGE_POSITIONS = 16
MP = 2
R_INST = 6
QKV = 10240
REQUEST_PAGES = 8
POOL_DEV = 16
POOL_INST = 64
STORE_PAGES = 256
R = 24
MOVED_REQUESTS = 4


def permuted(sub_key, count):
    return jax.random.permutation(sub_key, count)


def layout(key):
    base_key = jax.random.fold_in(key, 7001)
    key_order, key_slots, key_heavy, key_light, key_long, key_pool, key_shuffle = jax.random.split(base_key, 7)
    inst_count = R // R_INST
    rank_count = REQUEST_PAGES // MP
    half_count = inst_count // 2
    page_extent = REQUEST_PAGES * PAGE_POSITIONS
    inst_order = jax.random.permutation(key_order, inst_count).astype(jnp.int32)
    heavy_flag = jnp.zeros((inst_count,), jnp.int32).at[inst_order[:half_count]].set(1)
    slot_order = jax.vmap(partial(permuted, count=R_INST))(jax.random.split(key_slots, inst_count)).astype(jnp.int32)
    slot_place = jnp.argsort(slot_order, axis=1).astype(jnp.int32)
    heavy_len = jax.random.randint(key_heavy, (inst_count, R_INST), page_extent // 2, page_extent - 1)
    light_len = jax.random.randint(key_light, (inst_count, R_INST), 4, page_extent // 8 + 1)
    long_len = jax.random.randint(key_long, (inst_count, R_INST), (REQUEST_PAGES - 1) * PAGE_POSITIONS - 1, page_extent - 1)
    is_heavy = heavy_flag[:, None] == 1
    moved_flag = is_heavy & (slot_place < half_count)
    lengths = jnp.where(moved_flag, long_len, jnp.where(is_heavy, heavy_len, light_len)).astype(jnp.int32)
    pool_order = jax.vmap(partial(permuted, count=POOL_DEV))(jax.random.split(key_pool, inst_count * rank_count))
    pool_order = pool_order.reshape(inst_count, rank_count, POOL_DEV).astype(jnp.int32)
    page_ids = jnp.arange(REQUEST_PAGES, dtype=jnp.int32)
    page_rank = page_ids % rank_count
    page_depth = page_ids // rank_count
    slot_ids = jnp.arange(R_INST, dtype=jnp.int32)
    inst_ids = jnp.arange(inst_count, dtype=jnp.int32)
    local_index = slot_ids[:, None] * MP + page_depth[None, :]
    local_page = pool_order[inst_ids[:, None, None], page_rank[None, None, :], local_index[None, :, :]]
    needed = (lengths + 2 + PAGE_POSITIONS - 1) // PAGE_POSITIONS
    table = jnp.where(page_ids[None, None, :] < needed[:, :, None], page_rank[None, None, :] * POOL_DEV + local_page, -1)
    table = table.reshape(R, REQUEST_PAGES).astype(jnp.int32)
    heavy_pos = jnp.arange(half_count, dtype=jnp.int32)[:, None]
    light_pos = jnp.arange(half_count, dtype=jnp.int32)[None, :]
    heavy_inst = inst_order[heavy_pos[:, 0]][:, None]
    light_inst = inst_order[half_count + light_pos[0]][None, :]
    moved_slot = slot_order[heavy_inst, light_pos]
    request_ids = jnp.broadcast_to(heavy_inst * R_INST + moved_slot, (half_count, half_count))
    dest_inst = jnp.broadcast_to(light_inst, (half_count, half_count))
    incoming = (R_INST + heavy_pos[:, :, None]) * MP + page_depth[None, None, :]
    incoming = jnp.broadcast_to(incoming, (half_count, half_count, REQUEST_PAGES))
    dest_local = pool_order[dest_inst[:, :, None], page_rank[None, None, :], incoming]
    dest_table = page_rank[None, None, :] * POOL_DEV + dest_local
    shuffle = jax.random.permutation(key_shuffle, MOVED_REQUESTS)
    moves = jnp.stack([request_ids.reshape(-1), dest_inst.reshape(-1)], axis=1)[shuffle].astype(jnp.int32)
    dest_table = dest_table.reshape(MOVED_REQUESTS, REQUEST_PAGES)[shuffle].astype(jnp.int32)
    return (lengths.reshape(R), table, moves, dest_table)


def token_drawn(key, which):
    step_key = jax.random.fold_in(key, 9100 + which)
    key_body = jax.random.fold_in(step_key, 1)
    return jnp.clip(jax.random.normal(key_body, (R, QKV), jnp.float32), -5.0, 5.0)


def draw_qkv_first(key, part):
    return token_drawn(key, 1).astype(jnp.bfloat16)


def draw_qkv_second(key, part):
    return token_drawn(key, 2).astype(jnp.bfloat16)


def draw_kv_cache(key, part):
    store_key = jax.random.fold_in(key, 9300)
    memory_shape = (STORE_PAGES, 2, PAGE_POSITIONS, KEY_VALUE_HEADS * HEAD_SIZE)
    return jnp.clip(jax.random.normal(store_key, memory_shape, jnp.float32), -5.0, 5.0).astype(jnp.bfloat16)


def draw_lengths(key, part):
    return layout(key)[0]


def draw_page_table(key, part):
    return layout(key)[1]


def draw_moves(key, part):
    return layout(key)[2]


def draw_dest_pages(key, part):
    return layout(key)[3]


def levels(rng, dims, cuts, least, top_value):
    def one(position, parts):
        steps = jax.random.uniform(jax.random.fold_in(jax.random.fold_in(rng, 6), position), (parts,), jnp.float32, least / len(cuts), top_value / len(cuts))
        return jnp.repeat(jnp.exp(steps), dims[position] // parts).reshape((-1,) + (1,) * (len(dims) - position - 1))

    factor_of = one(*cuts[0])
    for cut in cuts[1:]:
        factor_of = factor_of * one(*cut)
    return factor_of


def bell_draw(key, dims, width, bound, shards=(), kind=jnp.bfloat16):
    entries = jax.random.normal(key, dims, jnp.float32) * width
    if len(shards) > 0:
        entries = levels(key, dims, shards, -0.22, 0.18) * entries
    return jnp.clip(entries, min=-bound, max=bound).astype(kind)


def setup_inputs(seed: int = 0, part: int = 0) -> dict:
    seeds = jax.random.split(jax.random.key(seed), 9)
    part_keys = jax.random.split(jax.random.fold_in(seeds[8], part), 9)
    return {
        "qkv_first": draw_qkv_first(jax.random.fold_in(jax.random.fold_in(seeds[8], part), 71), part),
        "qkv_second": draw_qkv_second(jax.random.fold_in(jax.random.fold_in(seeds[8], part), 71), part),
        "w_out": bell_draw(seeds[2], (QUERY_HEADS * HEAD_SIZE, D), HEAD_SIZE ** -0.5, 0.5, ((1, 4),)),
        "kv_cache": draw_kv_cache(jax.random.fold_in(jax.random.fold_in(seeds[8], part), 71), part),
        "lengths": draw_lengths(jax.random.fold_in(jax.random.fold_in(seeds[8], part), 71), part),
        "page_table": draw_page_table(jax.random.fold_in(jax.random.fold_in(seeds[8], part), 71), part),
        "moves": draw_moves(jax.random.fold_in(jax.random.fold_in(seeds[8], part), 71), part),
        "dest_pages": draw_dest_pages(jax.random.fold_in(jax.random.fold_in(seeds[8], part), 71), part),
    }


def attend(single_query, page_tile, live_count):
    group_width = QUERY_HEADS // KEY_VALUE_HEADS
    gathered_keys = page_tile[:, 0].reshape(REQUEST_PAGES * PAGE_POSITIONS, KEY_VALUE_HEADS, HEAD_SIZE).astype(jnp.float32)
    gathered_values = page_tile[:, 1].reshape(REQUEST_PAGES * PAGE_POSITIONS, KEY_VALUE_HEADS, HEAD_SIZE).astype(jnp.float32)
    heads_of_query = single_query.astype(jnp.float32).reshape(KEY_VALUE_HEADS, group_width, HEAD_SIZE)
    logit_scores = jnp.einsum('kgd,tkd->kgt', heads_of_query, gathered_keys, precision=lax.Precision.HIGHEST) / math.sqrt(HEAD_SIZE)
    visible = jnp.arange(REQUEST_PAGES * PAGE_POSITIONS, dtype=jnp.int32) < live_count
    logit_scores = jnp.where(visible[None, None, :], logit_scores, -jnp.inf)
    row_top = lax.optimization_barrier(jnp.max(logit_scores, axis=2, keepdims=True))
    exponent = jnp.where(visible[None, None, :], jnp.exp(logit_scores - row_top), 0.0)
    row_total = lax.optimization_barrier(jnp.sum(exponent, axis=2))
    weights = lax.optimization_barrier(exponent.astype(jnp.bfloat16)).astype(jnp.float32)
    summed = jnp.einsum('kgt,tkd->kgd', weights, gathered_values, precision=lax.Precision.HIGHEST)
    return (summed / row_total[:, :, None]).reshape(QUERY_HEADS * HEAD_SIZE).astype(jnp.bfloat16)

def write_tokens(paged_memory, token_rows, store_rows, positions):
    kv_start = QUERY_HEADS * HEAD_SIZE
    key_value_width = KEY_VALUE_HEADS * HEAD_SIZE
    new_keys = token_rows[:, kv_start:kv_start + key_value_width]
    new_values = token_rows[:, kv_start + key_value_width:kv_start + 2 * key_value_width]
    page_index = (positions // PAGE_POSITIONS).astype(jnp.int32)
    target_rows = jnp.take_along_axis(store_rows, page_index[:, None], axis=1)[:, 0]
    offsets = (positions % PAGE_POSITIONS).astype(jnp.int32)
    paged_memory = paged_memory.at[target_rows, 0, offsets].set(new_keys)
    paged_memory = paged_memory.at[target_rows, 1, offsets].set(new_values)
    return paged_memory

def decode_layer(paged_memory, token_rows, store_rows, counts, w_out):

    def attend_one(request):
        single_query, index_row, live_count = request
        page_tile = paged_memory[jnp.maximum(index_row, 0)]
        return attend(single_query, page_tile, live_count)
    mixed = lax.map(attend_one, (token_rows[:, :QUERY_HEADS * HEAD_SIZE], store_rows, counts))
    return jnp.dot(mixed, w_out, preferred_element_type=jnp.float32).astype(jnp.bfloat16)

def reference(qkv_first, qkv_second, w_out, kv_cache, lengths, page_table, moves, dest_pages):
    home_rows = jnp.arange(R, dtype=jnp.int32) // R_INST * POOL_INST
    store_rows = jnp.where(page_table >= 0, page_table + home_rows[:, None], -1).astype(jnp.int32)
    paged_memory = write_tokens(kv_cache, qkv_first, store_rows, lengths)
    out_first = decode_layer(paged_memory, qkv_first, store_rows, lengths + 1, w_out)
    movers = moves[:, 0]
    source_instances = store_rows[movers]
    targets = (moves[:, 1][:, None] * POOL_INST + dest_pages).astype(jnp.int32)
    paged_memory = paged_memory.at[targets.reshape(-1)].set(paged_memory[source_instances.reshape(-1)])
    paged_memory = paged_memory.at[source_instances.reshape(-1)].set(jnp.zeros((MOVED_REQUESTS * REQUEST_PAGES, 2, PAGE_POSITIONS, KEY_VALUE_HEADS * HEAD_SIZE), jnp.bfloat16))
    store_rows = store_rows.at[movers].set(targets)
    paged_memory = write_tokens(paged_memory, qkv_second, store_rows, lengths + 1)
    out_second = decode_layer(paged_memory, qkv_second, store_rows, lengths + 2, w_out)
    return (out_first, out_second, paged_memory)
```

```python
import functools
import math

import jax
import jax.numpy as jnp
from jax import lax
from jax.experimental import pallas as pl
from jax.experimental.pallas import tpu as pltpu
from jax.sharding import PartitionSpec as P

HEAD_SIZE = 128
NEG_LARGE = -1e30
BF16 = jnp.bfloat16
F32 = jnp.float32
VMEM = pltpu.VMEM
SMEM = pltpu.SMEM
MB = 1 << 20


def spec(space):
    return pl.BlockSpec(memory_space=space)


def in_vmem(x):
    return pltpu.with_memory_space_constraint(x, pltpu.VMEM)


def rounded_up(x, to):
    return -(-x // to) * to


def split_bf16(x):
    high = x.astype(BF16)
    rest = x - high.astype(F32)
    middle = rest.astype(BF16)
    low = (rest - middle.astype(F32)).astype(BF16)
    return high, middle, low


def stats_of(ref, width):
    pieces = [ref[:, width + k * 128 : width + (k + 1) * 128].astype(F32) for k in range(3)]
    return pieces[0] + pieces[1] + pieces[2]


def put_stats(ref, width, stats):
    for k, piece in enumerate(split_bf16(stats)):
        ref[:, width + k * 128 : width + (k + 1) * 128] = piece


def attend_kernel(dims, *refs):
    n, inst_count, rows_of, q_heads, kv_heads, per_rank = dims
    lengths, table, moves = refs[:3]
    pieces = refs[3 : 3 + 2 * n]
    kv_in = refs[3 + 2 * n]
    send_ref, keep_ref, stats_ref, kv_out, outgoing = refs[4 + 2 * n : 9 + 2 * n]
    rows_scr, pages, source, sems = refs[9 + 2 * n :]
    pool, _, extent, kv_width = kv_in.shape
    step_rows = rows_scr.shape[0] // 2
    all_rows = 2 * step_rows
    positions = pool * extent
    group = q_heads // kv_heads
    q_width = q_heads * HEAD_SIZE
    width = pieces[0].shape[1]
    me = lax.axis_index("tp")
    inst = lax.axis_index("inst")

    rows_scr[...] = jnp.zeros_like(rows_scr)
    for d in range(n):
        start = pl.multiple_of((me ^ d) * width, 128)
        for step in range(2):
            rows_scr[step * step_rows : step * step_rows + rows_of, pl.ds(start, width)] = pieces[
                2 * d + step
            ][...]

    pages[0:pool] = kv_in[...]
    pages[pool] = jnp.zeros_like(pages[pool])
    fresh = rows_scr[:, q_width:].astype(F32)
    row_id = lax.broadcasted_iota(jnp.int32, (extent, kv_width), 0)
    first_page = me * pool
    for step in range(2):
        for r in range(rows_of):
            position = lengths[inst * rows_of + r] + step
            local = table[r, lax.div(position, extent)] - first_page
            mine = (local >= 0) & (local < pool)
            slot = jnp.clip(local, 0, pool - 1)
            target = jnp.where(mine, lax.rem(position, extent), -1)
            for kv in range(2):
                new = fresh[
                    step * step_rows + r : step * step_rows + r + 1,
                    kv * kv_width : (kv + 1) * kv_width,
                ]
                old = pages[slot, kv].astype(F32)
                pages[slot, kv] = jnp.where(row_id == target, new, old).astype(BF16)

    for p in range(pool):
        source[p] = p
    move_count = moves.shape[0]
    for i in range(move_count):
        request = moves[i, 0]
        mine = lax.div(request, rows_of) == inst
        row = jnp.where(mine, request - inst * rows_of, 0)
        shift = lax.rem(moves[i, 1] - inst + inst_count, inst_count)

        @pl.when(mine)
        def _():
            for j in range(per_rank):
                local = table[row, me + n * j] - first_page
                source[local] = pool
                pltpu.make_async_copy(pages.at[local], outgoing.at[shift - 1, j], sems.at[1]).start()

    for p in range(pool):
        pltpu.make_async_copy(pages.at[source[p]], kv_out.at[p], sems.at[0]).start()

    lane = lax.broadcasted_iota(jnp.int32, (all_rows, positions), 1)
    page_of = lax.div(lane, extent)
    offset = lax.rem(lane, extent)
    row = lax.broadcasted_iota(jnp.int32, (all_rows, positions), 0)
    row_of = lax.rem(row, step_rows)
    count = jnp.zeros((all_rows, positions), jnp.int32)
    place = jnp.full((all_rows, positions), 1 << 30, jnp.int32)
    for r in range(rows_of):
        here = row_of == r
        count = jnp.where(here, lengths[inst * rows_of + r] + 1, count)
        for j in range(per_rank):
            number = me + n * j
            place = jnp.where(
                here & (page_of == table[r, number] - first_page), number * extent + offset, place
            )
    visible = (place < count + lax.div(row, step_rows))[None]

    half = kv_heads // 2
    half_heads = q_heads // 2
    side = lax.rem(me, 2)
    lane128 = lax.broadcasted_iota(jnp.int32, (all_rows, 128), 1)
    scale = 1.0 / math.sqrt(HEAD_SIZE)
    stats = [jnp.zeros((all_rows, 128), F32) for _ in range(2)]
    for i in range(kv_heads):
        kept = i // half
        g = jnp.where(kept == 1, side, 1 - side) * half + i % half
        q = jnp.concatenate(
            [
                rows_scr[:, pl.ds(pl.multiple_of((g * group + h) * HEAD_SIZE, 128), HEAD_SIZE)]
                for h in range(group)
            ],
            axis=0,
        )
        columns = pl.ds(pl.multiple_of(g * HEAD_SIZE, 128), HEAD_SIZE)
        keys = pages[0:pool, 0, :, columns].reshape(positions, HEAD_SIZE)
        values = pages[0:pool, 1, :, columns].reshape(positions, HEAD_SIZE)
        scores = lax.dot_general(q, keys, (((1,), (1,)), ((), ())), preferred_element_type=F32)
        scores = jnp.where(visible, (scores * scale).reshape(group, all_rows, positions), NEG_LARGE)
        top = jnp.max(scores, axis=2, keepdims=True)
        exponent = jnp.where(visible, jnp.exp(scores - top), 0.0)
        total = jnp.sum(exponent, axis=2, keepdims=True)
        summed = jnp.dot(
            exponent.astype(BF16).reshape(group * all_rows, positions),
            values,
            preferred_element_type=F32,
        )
        for h in range(group):
            head = (i % half) * group + h
            part = summed[h * all_rows : (h + 1) * all_rows]
            out_columns = slice(head * HEAD_SIZE, (head + 1) * HEAD_SIZE)
            if kept:
                keep_ref[:, out_columns] = part
            else:
                send_ref[:, out_columns] = part.astype(BF16)
            stats[kept] = jnp.where(lane128 == head, top[h], stats[kept])
            stats[kept] = jnp.where(lane128 == half_heads + head, total[h], stats[kept])
    put_stats(send_ref, half_heads * HEAD_SIZE, stats[0])
    stats_ref[...] = stats[1]

    for p in range(pool):
        pltpu.make_async_copy(pages.at[0], kv_out.at[p], sems.at[0]).wait()
    for i in range(move_count):
        mine = lax.div(moves[i, 0], rows_of) == inst

        @pl.when(mine)
        def _():
            for j in range(per_rank):
                pltpu.make_async_copy(pages.at[0], outgoing.at[0, j], sems.at[1]).wait()


def joined(acc_ref, stats_ref, other_ref, half_heads):
    width = half_heads * HEAD_SIZE
    mine = stats_ref[...]
    theirs = stats_of(other_ref, width)
    lane = lax.broadcasted_iota(jnp.int32, mine.shape, 1)
    top = jnp.maximum(mine, theirs)
    scale_mine = jnp.exp(mine - top)
    scale_theirs = jnp.exp(theirs - top)
    total = mine * pltpu.roll(scale_mine, half_heads, 1) + theirs * pltpu.roll(
        scale_theirs, half_heads, 1
    )
    stats = jnp.where(lane < half_heads, top, total)
    for h in range(half_heads):
        columns = slice(h * HEAD_SIZE, (h + 1) * HEAD_SIZE)
        part = acc_ref[:, columns] * scale_mine[:, h : h + 1] + other_ref[:, columns].astype(
            F32
        ) * scale_theirs[:, h : h + 1]
        yield columns, part, stats, h


def merge_kernel(half_heads, acc_ref, stats_ref, other_ref, acc_out, stats_out, send_ref):
    for columns, part, stats, _ in joined(acc_ref, stats_ref, other_ref, half_heads):
        acc_out[:, columns] = part
        send_ref[:, columns] = part.astype(BF16)
    stats_out[...] = stats
    put_stats(send_ref, half_heads * HEAD_SIZE, stats)


def finish_kernel(half_heads, acc_ref, stats_ref, other_ref, mixed_ref):
    for columns, part, stats, h in joined(acc_ref, stats_ref, other_ref, half_heads):
        mixed_ref[:, columns] = (part / stats[:, half_heads + h : half_heads + h + 1]).astype(BF16)


def project_kernel(mixed_ref, w_ref, acc_ref):
    side = lax.rem(lax.axis_index("tp"), 2)
    depth = mixed_ref.shape[1]
    start = pl.multiple_of(side * depth, 128)
    tile = 256

    @pl.loop(0, w_ref.shape[1] // tile)
    def _(t):
        columns = pl.ds(pl.multiple_of(t * tile, tile), tile)
        acc_ref[:, columns] = jnp.dot(
            mixed_ref[...], w_ref[pl.ds(start, depth), columns], preferred_element_type=F32
        )


def finish_project_kernel(dims, *refs):
    n, inst_count, rows_of, per_rank = dims
    moves, dest, mixed_ref, w_ref, acc_ref = refs[:5]
    arrived = refs[5 : 4 + inst_count]
    first_ref, second_ref, kv_out = refs[5 + inst_count : 8 + inst_count]
    held, sems = refs[8 + inst_count :]
    me = lax.axis_index("tp")
    inst = lax.axis_index("inst")
    pool = kv_out.shape[0]
    side = lax.rem(me, 2)
    depth = mixed_ref.shape[1]
    start = pl.multiple_of((1 - side) * depth, 128)
    step_rows = mixed_ref.shape[0] // 2
    tile = 256

    loads = [
        pltpu.make_async_copy(a, held.at[k], sems.at[0]) for k, a in enumerate(arrived)
    ]
    for load in loads:
        load.start()

    @pl.loop(0, w_ref.shape[1] // tile)
    def _(t):
        columns = pl.ds(pl.multiple_of(t * tile, tile), tile)
        total = acc_ref[:, columns] + jnp.dot(
            mixed_ref[...], w_ref[pl.ds(start, depth), columns], preferred_element_type=F32
        )
        first_ref[:, columns] = total[:rows_of].astype(BF16)
        second_ref[:, columns] = total[step_rows : step_rows + rows_of].astype(BF16)

    for load in loads:
        load.wait()

    def each(act):
        for i in range(moves.shape[0]):

            @pl.when(moves[i, 1] == inst)
            def _():
                origin = lax.div(moves[i, 0], rows_of)
                shift = lax.rem(inst - origin + inst_count, inst_count)
                for j in range(per_rank):
                    page = dest[i, me + n * j] - me * pool
                    act(pltpu.make_async_copy(held.at[shift - 1, j], kv_out.at[page], sems.at[1]))

    each(lambda copy: copy.start())
    each(lambda copy: copy.wait())


def local(qkv_first, qkv_second, w_out, kv_cache, lengths, page_table, moves, dest_pages):
    n = lax.axis_size("tp")
    inst_count = lax.axis_size("inst")
    rows_of, max_pages = page_table.shape
    per_rank = max_pages // n
    pool, _, extent, kv_width = kv_cache.shape
    q_width = w_out.shape[0]
    q_heads = q_width // HEAD_SIZE
    kv_heads = kv_width // HEAD_SIZE
    half_heads = q_heads // 2
    width = half_heads * HEAD_SIZE
    packed = width + 3 * 128
    step_rows = rounded_up(rows_of, 8)
    all_rows = 2 * step_rows
    out_columns = w_out.shape[1]

    def swap(x, d):
        return lax.ppermute(x, "tp", [(i, i ^ d) for i in range(n)])

    pieces = [qkv_first, qkv_second]
    for d in range(1, n):
        pieces += [swap(qkv_first, d), swap(qkv_second, d)]

    small = pltpu.CompilerParams(vmem_limit_bytes=12 * MB)
    send, acc, stats, kv_mid, outgoing = pl.pallas_call(
        functools.partial(
            attend_kernel, (n, inst_count, rows_of, q_heads, kv_heads, per_rank)
        ),
        out_shape=(
            jax.ShapeDtypeStruct((all_rows, packed), BF16),
            jax.ShapeDtypeStruct((all_rows, width), F32),
            jax.ShapeDtypeStruct((all_rows, 128), F32),
            jax.ShapeDtypeStruct(kv_cache.shape, BF16),
            jax.ShapeDtypeStruct((inst_count - 1, per_rank) + kv_cache.shape[1:], BF16),
        ),
        in_specs=[spec(SMEM)] * 3 + [spec(VMEM)] * (2 * n + 1),
        out_specs=(spec(VMEM),) * 3 + (spec(pltpu.HBM),) * 2,
        scratch_shapes=[
            pltpu.VMEM((all_rows, q_width + 2 * kv_width), BF16),
            pltpu.VMEM((pool + 1,) + kv_cache.shape[1:], BF16),
            pltpu.SMEM((pool,), jnp.int32),
            pltpu.SemaphoreType.DMA((2,)),
        ],
        compiler_params=small,
        name="attend",
    )(lengths, page_table, moves, *pieces, in_vmem(kv_cache))

    arrived = [
        lax.ppermute(
            outgoing[s - 1], "inst", [(i, (i + s) % inst_count) for i in range(inst_count)]
        )
        for s in range(1, inst_count)
    ]

    stages = [1]
    while 2 * stages[-1] < n:
        stages.append(2 * stages[-1])
    for d in stages[:-1]:
        acc, stats, send = pl.pallas_call(
            functools.partial(merge_kernel, half_heads),
            out_shape=(
                jax.ShapeDtypeStruct((all_rows, width), F32),
                jax.ShapeDtypeStruct((all_rows, 128), F32),
                jax.ShapeDtypeStruct((all_rows, packed), BF16),
            ),
            in_specs=[spec(VMEM)] * 3,
            out_specs=(spec(VMEM),) * 3,
            compiler_params=small,
            name=f"merge{d}",
        )(acc, stats, swap(send, d))
    mixed = pl.pallas_call(
        functools.partial(finish_kernel, half_heads),
        out_shape=jax.ShapeDtypeStruct((all_rows, width), BF16),
        in_specs=[spec(VMEM)] * 3,
        out_specs=spec(VMEM),
        compiler_params=small,
        name="finish",
    )(acc, stats, swap(send, stages[-1]))
    other = swap(mixed, 1)
    w_near = in_vmem(w_out)
    partial = pl.pallas_call(
        project_kernel,
        out_shape=jax.ShapeDtypeStruct((all_rows, out_columns), F32),
        in_specs=[spec(VMEM)] * 2,
        out_specs=spec(VMEM),
        compiler_params=small,
        cost_estimate=pl.CostEstimate(
            flops=2 * all_rows * width * out_columns, bytes_accessed=0, transcendentals=0
        ),
        name="project",
    )(mixed, w_near)
    return pl.pallas_call(
        functools.partial(finish_project_kernel, (n, inst_count, rows_of, per_rank)),
        out_shape=(
            jax.ShapeDtypeStruct((rows_of, out_columns), BF16),
            jax.ShapeDtypeStruct((rows_of, out_columns), BF16),
            jax.ShapeDtypeStruct(kv_cache.shape, BF16),
        ),
        in_specs=[spec(SMEM)] * 2 + [spec(VMEM)] * 3 + [spec(pltpu.HBM)] * inst_count,
        out_specs=(spec(VMEM), spec(VMEM), spec(pltpu.HBM)),
        scratch_shapes=[
            pltpu.VMEM((inst_count - 1, per_rank) + kv_cache.shape[1:], BF16),
            pltpu.SemaphoreType.DMA((2,)),
        ],
        input_output_aliases={4 + inst_count: 2},
        compiler_params=small,
        name="finish_project",
    )(moves, dest_pages, other, w_near, partial, *arrived, kv_mid)


def solution(mesh):
    placed = (
        P(("groups", "inst"), "tp"),
        P(("groups", "inst"), "tp"),
        P(None, "tp"),
        P(("groups", "inst", "tp"), None, None, None),
        P("groups"),
        P(("groups", "inst"), None),
        P("groups", None),
        P("groups", None),
    )
    return jax.shard_map(
        local,
        mesh=mesh,
        in_specs=placed,
        out_specs=(
            P(("groups", "inst"), "tp"),
            P(("groups", "inst"), "tp"),
            P(("groups", "inst", "tp"), None, None, None),
        ),
        check_vma=False,
    )
```

```python
import functools
import math

import jax
import jax.numpy as jnp
from jax import lax
from jax.experimental import pallas as pl
from jax.experimental.pallas import tpu as pltpu
from jax.sharding import PartitionSpec as P

HEAD_SIZE = 128
NEG_LARGE = -1e30
BF16 = jnp.bfloat16
F32 = jnp.float32
VMEM = pltpu.VMEM
SMEM = pltpu.SMEM
MB = 1 << 20
TILE = 256


def spec(space):
    return pl.BlockSpec(memory_space=space)


def in_hbm(x):
    return pltpu.with_memory_space_constraint(x, pltpu.HBM)


def shape(dims, dtype=BF16):
    return jax.ShapeDtypeStruct(dims, dtype)


def cost(micros):
    return pl.CostEstimate(flops=int(micros * 1e6), bytes_accessed=0, transcendentals=0)


def rounded_up(x, to):
    return -(-x // to) * to


def split_bf16(x):
    high = x.astype(BF16)
    rest = x - high.astype(F32)
    middle = rest.astype(BF16)
    low = (rest - middle.astype(F32)).astype(BF16)
    return high, middle, low


def stats_of(ref, width):
    pieces = [ref[:, width + k * 128 : width + (k + 1) * 128].astype(F32) for k in range(3)]
    return pieces[0] + pieces[1] + pieces[2]


def put_stats(ref, width, stats):
    for k, piece in enumerate(split_bf16(stats)):
        ref[:, width + k * 128 : width + (k + 1) * 128] = piece


def places(shape, row_axis, extent, step_rows, rows_of, n, per_rank, me, pool, table, lengths, inst):
    at = lax.broadcasted_iota(jnp.int32, shape, 1 - row_axis)
    row = lax.broadcasted_iota(jnp.int32, shape, row_axis)
    step = lax.div(row, step_rows)
    row_of = row - step * step_rows
    page_of = lax.div(at, extent)
    offset = at - page_of * extent
    newest = jnp.full(shape, -1, jnp.int32)
    place = jnp.full(shape, 1 << 30, jnp.int32)
    for r in range(rows_of):
        here = row_of == r
        newest = jnp.where(here, lengths[inst * rows_of + r], newest)
        for j in range(per_rank):
            number = me + n * j
            local = table[r, number] - me * pool
            place = jnp.where(here & (page_of == local), number * extent + offset, place)
    return place, newest + step


def prepare_kernel(dims, *refs):
    n, rows_of, per_rank = dims
    w_hbm, kv_hbm, first_hbm, second_hbm, lengths_hbm, table_hbm = refs[:6]
    w_ref, pages_ref, first_ref, second_ref, visible_ref, spread_ref, hit_ref = refs[6:13]
    lengths, table, sems = refs[13:]
    me = lax.axis_index("tp")
    inst = lax.axis_index("inst")
    pool, _, extent, _ = pages_ref.shape
    all_rows = spread_ref.shape[1]
    positions = pool * extent
    small = [
        pltpu.make_async_copy(lengths_hbm, lengths, sems.at[0]),
        pltpu.make_async_copy(table_hbm, table, sems.at[1]),
    ]
    half = w_hbm.shape[0] // 2
    start = pl.multiple_of(lax.rem(me, 2) * half, 128)
    large = [
        pltpu.make_async_copy(kv_hbm, pages_ref, sems.at[2]),
        pltpu.make_async_copy(first_hbm, first_ref, sems.at[3]),
        pltpu.make_async_copy(second_hbm, second_ref, sems.at[4]),
        pltpu.make_async_copy(w_hbm.at[pl.ds(start, w_ref.shape[0])], w_ref, sems.at[5]),
    ]
    for copy in small + large:
        copy.start()
    for copy in small:
        copy.wait()
    about = (extent, all_rows // 2, rows_of, n, per_rank, me, pool, table, lengths, inst)
    place, newest = places((all_rows, positions), 0, *about)
    visible_ref[...] = (place <= newest).astype(jnp.int32)
    place, newest = places((positions, all_rows), 1, *about)
    spread = (place == newest).astype(F32)
    spread_ref[...] = spread.astype(BF16)
    hit_ref[...] = jnp.broadcast_to(jnp.sum(spread, axis=1, keepdims=True), hit_ref.shape)
    for copy in large:
        copy.wait()


def attend_kernel(dims, *refs):
    n, inst_count, rows_of, q_heads, kv_heads, per_rank = dims
    table_hbm, moves_hbm, w_hbm = refs[:3]
    pieces = refs[3 : 3 + 2 * n]
    kv_in, visible_ref, spread_ref, hit_ref = refs[3 + 2 * n : 7 + 2 * n]
    send_ref, keep_ref, stats_ref, w_ref, kv_out = refs[7 + 2 * n : 12 + 2 * n]
    outgoing = refs[12 + 2 * n : 11 + 2 * n + inst_count]
    rows_scr, pages, table, moves, source, sems = refs[11 + 2 * n + inst_count :]
    pool, _, extent, kv_width = kv_in.shape
    step_rows = rows_scr.shape[0] // 2
    all_rows = 2 * step_rows
    positions = pool * extent
    group = q_heads // kv_heads
    q_width = q_heads * HEAD_SIZE
    width = pieces[0].shape[1]
    me = lax.axis_index("tp")
    inst = lax.axis_index("inst")
    first_page = me * pool

    tables = [
        pltpu.make_async_copy(table_hbm, table, sems.at[2]),
        pltpu.make_async_copy(moves_hbm, moves, sems.at[3]),
    ]
    for copy in tables:
        copy.start()
    start = pl.multiple_of(lax.rem(me, 2) * (w_hbm.shape[0] // 2) + w_hbm.shape[0] // 4, 128)
    w_copy = pltpu.make_async_copy(w_hbm.at[pl.ds(start, w_ref.shape[0])], w_ref, sems.at[4])
    w_copy.start()

    rows_scr[...] = jnp.zeros_like(rows_scr)
    for d in range(n):
        start = pl.multiple_of((me ^ d) * width, 128)
        for step in range(2):
            rows_scr[step * step_rows : step * step_rows + rows_of, pl.ds(start, width)] = pieces[
                2 * d + step
            ][...]

    pages[pool] = jnp.zeros_like(pages[pool])
    hit = hit_ref[...] > 0.0
    for kv in range(2):
        for c in range(0, kv_width, 128):
            columns = slice(c, c + 128)
            begin = q_width + kv * kv_width + c
            placed = jnp.dot(
                spread_ref[...], rows_scr[:, begin : begin + 128], preferred_element_type=F32
            )
            old = kv_in[:, kv, :, columns].reshape(positions, 128).astype(F32)
            new = jnp.where(hit, placed, old).astype(BF16)
            pages[0:pool, kv, :, columns] = new.reshape(pool, extent, 128)

    for copy in tables:
        copy.wait()
    for p in range(pool):
        source[p] = p
    move_count = moves.shape[1]
    for i in range(move_count):
        request = moves[0, i]
        mine = lax.div(request, rows_of) == inst
        row = jnp.where(mine, request - inst * rows_of, 0)
        shift = lax.rem(moves[1, i] - inst + inst_count, inst_count)

        @pl.when(mine)
        def _():
            for j in range(per_rank):
                source[table[row, me + n * j] - first_page] = pool

        for s in range(1, inst_count):

            @pl.when(mine & (shift == s))
            def _():
                for j in range(per_rank):
                    local = table[row, me + n * j] - first_page
                    pltpu.make_async_copy(pages.at[local], outgoing[s - 1].at[j], sems.at[1]).start()

    for p in range(pool):
        pltpu.make_async_copy(pages.at[source[p]], kv_out.at[p], sems.at[0]).start()

    visible = (visible_ref[...] > 0)[None]
    half = kv_heads // 2
    half_heads = q_heads // 2
    side = lax.rem(me, 2)
    lane128 = lax.broadcasted_iota(jnp.int32, (all_rows, 128), 1)
    scale = 1.0 / math.sqrt(HEAD_SIZE)
    stats = [jnp.zeros((all_rows, 128), F32) for _ in range(2)]
    for i in range(kv_heads):
        kept = i // half
        g = jnp.where(kept == 1, side, 1 - side) * half + i % half
        q = jnp.concatenate(
            [
                rows_scr[:, pl.ds(pl.multiple_of((g * group + h) * HEAD_SIZE, 128), HEAD_SIZE)]
                for h in range(group)
            ],
            axis=0,
        )
        columns = pl.ds(pl.multiple_of(g * HEAD_SIZE, 128), HEAD_SIZE)
        keys = pages[0:pool, 0, :, columns].reshape(positions, HEAD_SIZE)
        values = pages[0:pool, 1, :, columns].reshape(positions, HEAD_SIZE)
        scores = lax.dot_general(q, keys, (((1,), (1,)), ((), ())), preferred_element_type=F32)
        scores = jnp.where(visible, (scores * scale).reshape(group, all_rows, positions), NEG_LARGE)
        top = jnp.max(scores, axis=2, keepdims=True)
        exponent = jnp.where(visible, jnp.exp(scores - top), 0.0)
        total = jnp.sum(exponent, axis=2, keepdims=True)
        summed = jnp.dot(
            exponent.astype(BF16).reshape(group * all_rows, positions),
            values,
            preferred_element_type=F32,
        )
        for h in range(group):
            head = (i % half) * group + h
            part = summed[h * all_rows : (h + 1) * all_rows]
            out_columns = slice(head * HEAD_SIZE, (head + 1) * HEAD_SIZE)
            if kept:
                keep_ref[:, out_columns] = part
            else:
                send_ref[:, out_columns] = part.astype(BF16)
            stats[kept] = jnp.where(lane128 == head, top[h], stats[kept])
            stats[kept] = jnp.where(lane128 == half_heads + head, total[h], stats[kept])
    put_stats(send_ref, half_heads * HEAD_SIZE, stats[0])
    stats_ref[...] = stats[1]

    for p in range(pool):
        pltpu.make_async_copy(pages.at[0], kv_out.at[p], sems.at[0]).wait()
    for i in range(move_count):
        mine = lax.div(moves[0, i], rows_of) == inst

        @pl.when(mine)
        def _():
            for j in range(per_rank):
                pltpu.make_async_copy(pages.at[0], outgoing[0].at[j], sems.at[1]).wait()
    w_copy.wait()


def joined(acc_ref, stats_ref, other_ref, half_heads):
    width = half_heads * HEAD_SIZE
    mine = stats_ref[...]
    theirs = stats_of(other_ref, width)
    lane = lax.broadcasted_iota(jnp.int32, mine.shape, 1)
    top = jnp.maximum(mine, theirs)
    scale_mine = jnp.exp(mine - top)
    scale_theirs = jnp.exp(theirs - top)
    total = mine * pltpu.roll(scale_mine, half_heads, 1) + theirs * pltpu.roll(
        scale_theirs, half_heads, 1
    )
    stats = jnp.where(lane < half_heads, top, total)
    for h in range(half_heads):
        columns = slice(h * HEAD_SIZE, (h + 1) * HEAD_SIZE)
        part = acc_ref[:, columns] * scale_mine[:, h : h + 1] + other_ref[:, columns].astype(
            F32
        ) * scale_theirs[:, h : h + 1]
        yield columns, part, stats, h


def merge_kernel(half_heads, acc_ref, stats_ref, other_ref, acc_out, stats_out, send_ref):
    for columns, part, stats, _ in joined(acc_ref, stats_ref, other_ref, half_heads):
        acc_out[:, columns] = part
        send_ref[:, columns] = part.astype(BF16)
    stats_out[...] = stats
    put_stats(send_ref, half_heads * HEAD_SIZE, stats)


def finish_kernel(half_heads, acc_ref, stats_ref, other_ref, mixed_ref):
    for columns, part, stats, h in joined(acc_ref, stats_ref, other_ref, half_heads):
        mixed_ref[:, columns] = (part / stats[:, half_heads + h : half_heads + h + 1]).astype(BF16)


def project_kernel(mixed_ref, near_ref, far_ref, w_hbm, acc_ref, w_ref, sem):
    me = lax.axis_index("tp")
    start = pl.multiple_of((1 - lax.rem(me, 2)) * (w_hbm.shape[0] // 2), 128)
    w_copy = pltpu.make_async_copy(w_hbm.at[pl.ds(start, w_ref.shape[0])], w_ref, sem)
    w_copy.start()
    depth = near_ref.shape[0]

    @pl.loop(0, acc_ref.shape[1] // TILE)
    def _(t):
        columns = pl.ds(pl.multiple_of(t * TILE, TILE), TILE)
        acc_ref[:, columns] = jnp.dot(
            mixed_ref[:, :depth], near_ref[:, columns], preferred_element_type=F32
        ) + jnp.dot(mixed_ref[:, depth:], far_ref[:, columns], preferred_element_type=F32)

    w_copy.wait()


def finish_project_kernel(dims, *refs):
    n, inst_count, rows_of, per_rank = dims
    moves, dest, mixed_ref, near_ref, far_ref, acc_ref = refs[:6]
    arrived = refs[6 : 5 + inst_count]
    first_ref, second_ref, kv_out = refs[6 + inst_count : 9 + inst_count]
    held, sems = refs[9 + inst_count :]
    me = lax.axis_index("tp")
    inst = lax.axis_index("inst")
    pool = kv_out.shape[0]
    step_rows = mixed_ref.shape[0] // 2
    depth = near_ref.shape[0]

    loads = [pltpu.make_async_copy(a, held.at[k], sems.at[0]) for k, a in enumerate(arrived)]
    for load in loads:
        load.start()
    for load in loads:
        load.wait()

    def each(act):
        for i in range(moves.shape[1]):

            @pl.when(moves[1, i] == inst)
            def _():
                origin = lax.div(moves[0, i], rows_of)
                shift = lax.rem(inst - origin + inst_count, inst_count)
                for j in range(per_rank):
                    page = dest[i, me + n * j] - me * pool
                    act(pltpu.make_async_copy(held.at[shift - 1, j], kv_out.at[page], sems.at[1]))

    each(lambda copy: copy.start())

    @pl.loop(0, acc_ref.shape[1] // TILE)
    def _(t):
        columns = pl.ds(pl.multiple_of(t * TILE, TILE), TILE)
        total = (
            acc_ref[:, columns]
            + jnp.dot(mixed_ref[:, :depth], near_ref[:, columns], preferred_element_type=F32)
            + jnp.dot(mixed_ref[:, depth:], far_ref[:, columns], preferred_element_type=F32)
        )
        first_ref[:, columns] = total[:rows_of].astype(BF16)
        second_ref[:, columns] = total[step_rows : step_rows + rows_of].astype(BF16)

    each(lambda copy: copy.wait())


def stage_kernel(w_hbm, after_ref, w_ref, sem):
    me = lax.axis_index("tp")
    half = w_hbm.shape[0] // 2
    start = pl.multiple_of((1 - lax.rem(me, 2)) * half + half // 2, 128)
    w_copy = pltpu.make_async_copy(w_hbm.at[pl.ds(start, w_ref.shape[0])], w_ref, sem)
    w_copy.start()
    w_copy.wait()


def local(qkv_first, qkv_second, w_out, kv_cache, lengths, page_table, moves, dest_pages):
    n = lax.axis_size("tp")
    inst_count = lax.axis_size("inst")
    moves = moves.T
    rows_of, max_pages = page_table.shape
    per_rank = max_pages // n
    pool, _, extent, kv_width = kv_cache.shape
    q_width = w_out.shape[0]
    q_heads = q_width // HEAD_SIZE
    kv_heads = kv_width // HEAD_SIZE
    half_heads = q_heads // 2
    width = half_heads * HEAD_SIZE
    packed = width + 3 * 128
    step_rows = rounded_up(rows_of, 8)
    all_rows = 2 * step_rows
    out_columns = w_out.shape[1]

    def swap(x, d):
        return lax.ppermute(x, "tp", [(i, i ^ d) for i in range(n)])

    small = pltpu.CompilerParams(vmem_limit_bytes=8 * MB)
    quarter = width // 2
    w_far = in_hbm(w_out)
    w_part = shape((quarter, out_columns))
    positions = pool * extent
    dma = pltpu.SemaphoreType.DMA

    got = []
    for d in range(1, n):
        got += [swap(qkv_first, d), swap(qkv_second, d)]
    w_near0, pages, own_first, own_second, visible, spread, hit = pl.pallas_call(
        functools.partial(prepare_kernel, (n, rows_of, per_rank)),
        out_shape=(
            w_part,
            shape(kv_cache.shape),
            shape(qkv_first.shape),
            shape(qkv_second.shape),
            shape((all_rows, positions), jnp.int32),
            shape((positions, all_rows)),
            shape((positions, 128), F32),
        ),
        in_specs=[spec(pltpu.HBM)] * 6,
        out_specs=(spec(VMEM),) * 7,
        scratch_shapes=[
            pltpu.SMEM(lengths.shape, jnp.int32),
            pltpu.SMEM(page_table.shape, jnp.int32),
            dma((6,)),
        ],
        compiler_params=small,
        cost_estimate=cost(3),
        name="prepare",
    )(w_far, in_hbm(kv_cache), in_hbm(qkv_first), in_hbm(qkv_second), in_hbm(lengths), in_hbm(page_table))

    send, acc, stats, w_near1, kv_mid, *outgoing = pl.pallas_call(
        functools.partial(attend_kernel, (n, inst_count, rows_of, q_heads, kv_heads, per_rank)),
        out_shape=(
            shape((all_rows, packed)),
            shape((all_rows, width), F32),
            shape((all_rows, 128), F32),
            w_part,
            shape(kv_cache.shape),
        )
        + (shape((per_rank,) + kv_cache.shape[1:]),) * (inst_count - 1),
        in_specs=[spec(pltpu.HBM)] * 3 + [spec(VMEM)] * (2 * n + 4),
        out_specs=(spec(VMEM),) * 4 + (spec(pltpu.HBM),) * inst_count,
        scratch_shapes=[
            pltpu.VMEM((all_rows, q_width + 2 * kv_width), BF16),
            pltpu.VMEM((pool + 1,) + kv_cache.shape[1:], BF16),
            pltpu.SMEM(page_table.shape, jnp.int32),
            pltpu.SMEM(moves.shape, jnp.int32),
            pltpu.SMEM((pool,), jnp.int32),
            dma((5,)),
        ],
        compiler_params=small,
        cost_estimate=cost(3),
        name="attend",
    )(
        in_hbm(page_table),
        in_hbm(moves),
        w_far,
        own_first,
        own_second,
        *got,
        pages,
        visible,
        spread,
        hit,
    )

    stages = [1]
    while 2 * stages[-1] < n:
        stages.append(2 * stages[-1])
    for d in stages[:-1]:
        acc, stats, send = pl.pallas_call(
            functools.partial(merge_kernel, half_heads),
            out_shape=(
                shape((all_rows, width), F32),
                shape((all_rows, 128), F32),
                shape((all_rows, packed)),
            ),
            in_specs=[spec(VMEM)] * 3,
            out_specs=(spec(VMEM),) * 3,
            compiler_params=small,
            cost_estimate=cost(0.3),
            name=f"merge{d}",
        )(acc, stats, swap(send, d))
    theirs = swap(send, stages[-1])
    arrived = [
        lax.ppermute(
            outgoing[s - 1], "inst", [(i, (i + s) % inst_count) for i in range(inst_count)]
        )
        for s in range(1, inst_count)
    ]
    w_other1 = pl.pallas_call(
        stage_kernel,
        out_shape=w_part,
        in_specs=[spec(pltpu.HBM), spec(VMEM)],
        out_specs=spec(VMEM),
        scratch_shapes=[dma],
        compiler_params=small,
        cost_estimate=cost(2.5),
        name="stage",
    )(w_far, stats)
    mixed = pl.pallas_call(
        functools.partial(finish_kernel, half_heads),
        out_shape=shape((all_rows, width)),
        in_specs=[spec(VMEM)] * 3,
        out_specs=spec(VMEM),
        compiler_params=small,
        cost_estimate=cost(0.4),
        name="finish",
    )(acc, stats, theirs)
    other = swap(mixed, 1)
    partial, w_other0 = pl.pallas_call(
        project_kernel,
        out_shape=(shape((all_rows, out_columns), F32), w_part),
        in_specs=[spec(VMEM)] * 3 + [spec(pltpu.HBM)],
        out_specs=(spec(VMEM),) * 2,
        scratch_shapes=[dma],
        compiler_params=small,
        cost_estimate=cost(3),
        name="project",
    )(mixed, w_near0, w_near1, w_far)
    return pl.pallas_call(
        functools.partial(finish_project_kernel, (n, inst_count, rows_of, per_rank)),
        out_shape=(
            shape((rows_of, out_columns)),
            shape((rows_of, out_columns)),
            shape(kv_cache.shape),
        ),
        in_specs=[spec(SMEM)] * 2 + [spec(VMEM)] * 4 + [spec(pltpu.HBM)] * inst_count,
        out_specs=(spec(VMEM), spec(VMEM), spec(pltpu.HBM)),
        scratch_shapes=[
            pltpu.VMEM((inst_count - 1, per_rank) + kv_cache.shape[1:], BF16),
            dma((2,)),
        ],
        input_output_aliases={5 + inst_count: 2},
        compiler_params=small,
        cost_estimate=cost(3),
        name="finish_project",
    )(moves, dest_pages, other, w_other0, w_other1, partial, *arrived, kv_mid)


def solution(mesh):
    placed = (
        P(("groups", "inst"), "tp"),
        P(("groups", "inst"), "tp"),
        P(None, "tp"),
        P(("groups", "inst", "tp"), None, None, None),
        P("groups"),
        P(("groups", "inst"), None),
        P("groups", None),
        P("groups", None),
    )
    return jax.shard_map(
        local,
        mesh=mesh,
        in_specs=placed,
        out_specs=(
            P(("groups", "inst"), "tp"),
            P(("groups", "inst"), "tp"),
            P(("groups", "inst", "tp"), None, None, None),
        ),
        check_vma=False,
    )
```

```python
import functools
import math

import jax
import jax.numpy as jnp
from jax import lax
from jax.experimental import pallas as pl
from jax.experimental.pallas import tpu as pltpu
from jax.sharding import PartitionSpec as P

HEAD_SIZE = 128
LANES = 128
NEG_LARGE = -1e30
BF16 = jnp.bfloat16
F32 = jnp.float32
I32 = jnp.int32
VMEM = pltpu.VMEM
HBM = pltpu.HBM
TILE = 256
PARTS = 2
CHUNKS = 8
copy_of = pltpu.make_async_copy


def spec(space):
    return pl.BlockSpec(memory_space=space)


def in_hbm(x):
    return pltpu.with_memory_space_constraint(x, HBM)


def shape(dims, dtype=BF16):
    return jax.ShapeDtypeStruct(dims, dtype)


def run(kernel, name, micros, ins, outs, scratch, args, aliases=None, after=(), limit=8):
    count = len(ins)

    def body(*refs):
        kernel(*refs[:count], *refs[count + len(after) :])

    ins = list(ins) + [pl.ANY] * len(after)
    args = list(args) + list(after)
    return pl.pallas_call(
        body,
        out_shape=tuple(s for s, _ in outs),
        in_specs=[spec(space) for space in ins],
        out_specs=tuple(spec(space) for _, space in outs),
        scratch_shapes=scratch,
        input_output_aliases=aliases or {},
        compiler_params=pltpu.CompilerParams(vmem_limit_bytes=limit << 20),
        cost_estimate=pl.CostEstimate(
            flops=int(micros * 3e8), bytes_accessed=0, transcendentals=0
        ),
        name=name,
    )(*args)


def behind(x, token):
    return lax.optimization_barrier((x, token))[0]


def rounded_up(x, to):
    return -(-x // to) * to


class Sizes:
    def __init__(self, n, inst_count, rows_of, per_rank, kv_shape, w_shape):
        self.n = n
        self.inst_count = inst_count
        self.rows_of = rows_of
        self.per_rank = per_rank
        self.pool, _, self.extent, self.kv_width = kv_shape
        self.q_width, self.out_columns = w_shape
        self.q_heads = self.q_width // HEAD_SIZE
        self.kv_heads = self.kv_width // HEAD_SIZE
        self.group = self.q_heads // self.kv_heads
        self.step_rows = rounded_up(rows_of, 8)
        self.all_rows = 2 * self.step_rows
        self.positions = self.pool * self.extent
        self.part_groups = self.kv_heads // (2 * PARTS)
        self.part_heads = self.part_groups * self.group
        self.part_width = self.part_heads * HEAD_SIZE
        self.packed = self.part_width + LANES
        self.chunk_rows = self.q_width // CHUNKS
        self.at_offset = 2 * rows_of
        self.at_source = 4 * rows_of
        self.at_send = self.at_source + self.pool
        self.at_place = self.at_send + (inst_count - 1) * per_rank
        self.plan_rows = rounded_up(
            -(-(self.at_place + (inst_count - 1) * per_rank) // LANES), 8
        )


def w_chunk(w_hbm, k):
    rows = w_hbm.shape[0] // CHUNKS
    side = lax.rem(lax.axis_index("tp"), 2)
    half = side if k < CHUNKS // 2 else 1 - side
    start = half * (w_hbm.shape[0] // 2) + (k % (CHUNKS // 2)) * rows
    return w_hbm.at[pl.ds(pl.multiple_of(start, LANES), rows)]


def w_copies(w_hbm, chunks, refs, sems, first):
    return [copy_of(w_chunk(w_hbm, k), ref, sems.at[first + i]) for i, (k, ref) in enumerate(zip(chunks, refs))]


def prepare_kernel(z, chunks, *refs):
    w_hbm, kv_hbm, first_hbm, second_hbm, lengths_hbm, table_hbm, moves_hbm, dest_hbm = refs[:8]
    pages, first_ref, second_ref, visible_ref, plan_ref = refs[8:13]
    w_refs = refs[13 : 13 + len(chunks)]
    lengths, table, moves, dest, plan, sems = refs[13 + len(chunks) :]
    me = lax.axis_index("tp")
    inst = lax.axis_index("inst")
    small = [
        copy_of(lengths_hbm, lengths, sems.at[0]),
        copy_of(table_hbm, table, sems.at[1]),
        copy_of(moves_hbm, moves, sems.at[2]),
        copy_of(dest_hbm, dest, sems.at[3]),
    ]
    large = [
        copy_of(kv_hbm, pages.at[pl.ds(0, z.pool)], sems.at[4]),
        copy_of(first_hbm, first_ref, sems.at[5]),
        copy_of(second_hbm, second_ref, sems.at[6]),
    ] + w_copies(w_hbm, chunks, w_refs, sems, 7)
    for copy in small + large:
        copy.start()
    pages[z.pool] = jnp.zeros_like(pages[z.pool])
    for copy in small:
        copy.wait()

    grid = (z.all_rows, z.positions)
    at = lax.broadcasted_iota(I32, grid, 1)
    row = lax.broadcasted_iota(I32, grid, 0)
    step = lax.div(row, z.step_rows)
    row_of = row - step * z.step_rows
    page_of = lax.div(at, z.extent)
    offset = at - page_of * z.extent
    newest = jnp.full(grid, -1, I32)
    place = jnp.full(grid, 1 << 30, I32)
    for r in range(z.rows_of):
        here = row_of == r
        newest = jnp.where(here, lengths[inst * z.rows_of + r], newest)
        for j in range(z.per_rank):
            number = me + z.n * j
            local = table[r, number] - me * z.pool
            place = jnp.where(here & (page_of == local), number * z.extent + offset, place)
    visible_ref[...] = (place <= newest + step).astype(I32)

    for k in range(2):
        for r in range(z.rows_of):
            position = lengths[inst * z.rows_of + r] + k
            local = table[r, lax.div(position, z.extent)] - me * z.pool
            mine = (local >= 0) & (local < z.pool)
            plan[k * z.rows_of + r] = jnp.where(mine, local, z.pool + 1)
            plan[z.at_offset + k * z.rows_of + r] = lax.rem(position, z.extent)
    for p in range(z.pool):
        plan[z.at_source + p] = p
    for k in range(2 * (z.inst_count - 1) * z.per_rank):
        plan[z.at_send + k] = -1
    for i in range(moves.shape[1]):
        request = moves[0, i]
        target = moves[1, i]
        origin = lax.div(request, z.rows_of)
        shift = lax.rem(target - origin + z.inst_count, z.inst_count)

        @pl.when((origin == inst) & (shift > 0))
        def _():
            for j in range(z.per_rank):
                local = table[request - inst * z.rows_of, me + z.n * j] - me * z.pool
                plan[z.at_source + local] = z.pool
                plan[z.at_send + (shift - 1) * z.per_rank + j] = local

        @pl.when((target == inst) & (shift > 0))
        def _():
            for j in range(z.per_rank):
                plan[z.at_place + (shift - 1) * z.per_rank + j] = dest[i, me + z.n * j] - me * z.pool

    where = lax.broadcasted_iota(I32, plan_ref.shape, 0) * LANES + lax.broadcasted_iota(
        I32, plan_ref.shape, 1
    )
    packed = jnp.zeros(plan_ref.shape, I32)
    for k in range(z.at_place + (z.inst_count - 1) * z.per_rank):
        packed = jnp.where(where == k, plan[k], packed)
    plan_ref[...] = packed
    for copy in large:
        copy.wait()


def read(plan, k):
    return plan[k // LANES, k % LANES]


def attend_part(z, part, rows, pages, visible, send_ref, keep_ref, stats_ref):
    side = lax.rem(lax.axis_index("tp"), 2)
    half = z.kv_heads // 2
    lane = lax.broadcasted_iota(I32, (z.all_rows, LANES), 1)
    scale = 1.0 / math.sqrt(HEAD_SIZE)
    stats = [jnp.zeros((z.all_rows, LANES), F32) for _ in range(2)]
    for i in range(2 * z.part_groups):
        kept, k = divmod(i, z.part_groups)
        g = (side if kept else 1 - side) * half + part * z.part_groups + k
        q = jnp.concatenate(
            [
                rows[:, pl.ds(pl.multiple_of((g * z.group + h) * HEAD_SIZE, LANES), HEAD_SIZE)]
                for h in range(z.group)
            ],
            axis=0,
        )
        columns = pl.ds(pl.multiple_of(g * HEAD_SIZE, LANES), HEAD_SIZE)
        keys = pages[0 : z.pool, 0, :, columns].reshape(z.positions, HEAD_SIZE)
        values = pages[0 : z.pool, 1, :, columns].reshape(z.positions, HEAD_SIZE)
        scores = lax.dot_general(q, keys, (((1,), (1,)), ((), ())), preferred_element_type=F32)
        scores = (scores * scale).reshape(z.group, z.all_rows, z.positions)
        scores = jnp.where(visible, scores, NEG_LARGE)
        top = jnp.max(scores, axis=2, keepdims=True)
        exponent = jnp.where(visible, jnp.exp(scores - top), 0.0)
        total = jnp.sum(exponent, axis=2, keepdims=True)
        summed = jnp.dot(
            exponent.astype(BF16).reshape(z.group * z.all_rows, z.positions),
            values,
            preferred_element_type=F32,
        )
        for h in range(z.group):
            head = k * z.group + h
            piece = summed[h * z.all_rows : (h + 1) * z.all_rows]
            out_columns = slice(head * HEAD_SIZE, (head + 1) * HEAD_SIZE)
            if kept:
                keep_ref[:, out_columns] = piece
            else:
                send_ref[:, out_columns] = piece.astype(BF16)
            stats[kept] = jnp.where(lane == head, top[h], stats[kept])
            stats[kept] = jnp.where(lane == z.part_heads + head, total[h], stats[kept])
    put_stats(z, send_ref, stats[0])
    stats_ref[...] = stats[1]


def put_stats(z, ref, stats):
    used = 2 * z.part_heads
    lane = lax.broadcasted_iota(I32, stats.shape, 1)
    high = stats.astype(BF16).astype(F32)
    rest = stats - high
    middle = rest.astype(BF16).astype(F32)
    low = rest - middle
    pieces = jnp.where(
        lane < used,
        high,
        jnp.where(lane < 2 * used, pltpu.roll(middle, used, 1), pltpu.roll(low, 2 * used, 1)),
    )
    ref[:, z.part_width :] = pieces.astype(BF16)


def get_stats(z, ref):
    used = 2 * z.part_heads
    pieces = ref[:, z.part_width :].astype(F32)
    lane = lax.broadcasted_iota(I32, pieces.shape, 1)
    stats = (
        pieces
        + pltpu.roll(pieces, LANES - used, 1)
        + pltpu.roll(pieces, LANES - 2 * used, 1)
    )
    return jnp.where(lane < used, stats, 0.0)


def attend_first_kernel(z, chunks, *refs):
    m = 2 * z.n
    w_hbm, plan_vmem, visible_ref, pages_in = refs[:4]
    pieces = refs[4 : 4 + m]
    send_ref, keep_ref, stats_ref, rows, pages, kv_out = refs[4 + m : 10 + m]
    outgoing = refs[10 + m : 9 + m + z.inst_count]
    w_refs = refs[9 + m + z.inst_count : 9 + m + z.inst_count + len(chunks)]
    plan, sems = refs[9 + m + z.inst_count + len(chunks) :]
    me = lax.axis_index("tp")
    width = pieces[0].shape[1]
    plan_copy = copy_of(plan_vmem, plan, sems.at[0])
    plan_copy.start()
    w_loads = w_copies(w_hbm, chunks, w_refs, sems, 3)
    for copy in w_loads:
        copy.start()
    rows[...] = jnp.zeros_like(rows)
    for d in range(z.n):
        start = pl.multiple_of((me ^ d) * width, LANES)
        for k in range(2):
            rows[k * z.step_rows : k * z.step_rows + z.rows_of, pl.ds(start, width)] = pieces[
                2 * d + k
            ][...]
    plan_copy.wait()

    fresh = rows[:, z.q_width :].astype(F32)
    row_id = lax.broadcasted_iota(I32, (z.extent, z.kv_width), 0)
    for k in range(2):
        for r in range(z.rows_of):
            slot = read(plan, k * z.rows_of + r)
            here = row_id == read(plan, z.at_offset + k * z.rows_of + r)
            line = k * z.step_rows + r
            for kv in range(2):
                new = fresh[line : line + 1, kv * z.kv_width : (kv + 1) * z.kv_width]
                old = pages[slot, kv].astype(F32)
                pages[slot, kv] = jnp.where(here, new, old).astype(BF16)

    def sends(act):
        for s in range(z.inst_count - 1):
            for j in range(z.per_rank):
                slot = read(plan, z.at_send + s * z.per_rank + j)

                @pl.when(slot >= 0)
                def _():
                    act(copy_of(pages.at[slot], outgoing[s].at[j], sems.at[1]))

    sends(lambda copy: copy.start())
    writes = [
        copy_of(pages.at[read(plan, z.at_source + p)], kv_out.at[p], sems.at[2])
        for p in range(z.pool)
    ]
    for copy in writes:
        copy.start()
    visible = (visible_ref[...] > 0)[None]
    attend_part(z, 0, rows, pages, visible, send_ref, keep_ref, stats_ref)
    sends(lambda copy: copy.wait())
    for copy in writes + w_loads:
        copy.wait()


def attend_more_kernel(z, part, chunks, *refs):
    w_hbm, visible_ref, rows, pages, send_ref, keep_ref, stats_ref = refs[:7]
    w_refs = refs[7 : 7 + len(chunks)]
    (sems,) = refs[7 + len(chunks) :]
    w_loads = w_copies(w_hbm, chunks, w_refs, sems, 0)
    for copy in w_loads:
        copy.start()
    visible = (visible_ref[...] > 0)[None]
    attend_part(z, part, rows, pages, visible, send_ref, keep_ref, stats_ref)
    for copy in w_loads:
        copy.wait()


def joined(z, acc_ref, stats_ref, other_ref):
    mine = stats_ref[...]
    theirs = get_stats(z, other_ref)
    lane = lax.broadcasted_iota(I32, mine.shape, 1)
    top = jnp.maximum(mine, theirs)
    scale_mine = jnp.exp(mine - top)
    scale_theirs = jnp.exp(theirs - top)
    total = mine * pltpu.roll(scale_mine, z.part_heads, 1) + theirs * pltpu.roll(
        scale_theirs, z.part_heads, 1
    )
    stats = jnp.where(
        lane < z.part_heads, top, jnp.where(lane < 2 * z.part_heads, total, 0.0)
    )
    for h in range(z.part_heads):
        columns = slice(h * HEAD_SIZE, (h + 1) * HEAD_SIZE)
        piece = acc_ref[:, columns] * scale_mine[:, h : h + 1] + other_ref[:, columns].astype(
            F32
        ) * scale_theirs[:, h : h + 1]
        yield columns, piece, stats, h


def merge_kernel(z, acc_ref, stats_ref, other_ref, acc_out, stats_out, send_ref):
    for columns, piece, stats, _ in joined(z, acc_ref, stats_ref, other_ref):
        acc_out[:, columns] = piece
        send_ref[:, columns] = piece.astype(BF16)
    stats_out[...] = stats
    put_stats(z, send_ref, stats)


def finish_kernel(z, acc_ref, stats_ref, other_ref, mixed_ref):
    for columns, piece, stats, h in joined(z, acc_ref, stats_ref, other_ref):
        total = stats[:, z.part_heads + h : z.part_heads + h + 1]
        mixed_ref[:, columns] = (piece / total).astype(BF16)


def stage_kernel(chunks, w_hbm, *refs):
    loads = w_copies(w_hbm, chunks, refs[: len(chunks)], refs[-1], 0)
    for copy in loads:
        copy.start()
    for copy in loads:
        copy.wait()


def product(mixed, w_refs, columns):
    rows = w_refs[0].shape[0]
    total = None
    for i, w in enumerate(w_refs):
        part = jnp.dot(
            mixed[:, i * rows : (i + 1) * rows], w[:, columns], preferred_element_type=F32
        )
        total = part if total is None else total + part
    return total


def column_tiles(width, body):
    @pl.loop(0, width // TILE)
    def _(t):
        body(pl.ds(pl.multiple_of(t * TILE, TILE), TILE))


def project_kernel(z, used, chunks, has_acc, *refs):
    w_hbm, mixed = refs[:2]
    w_used = refs[2 : 2 + used]
    acc_in = refs[2 + used] if has_acc else None
    acc_ref = refs[2 + used + has_acc]
    w_refs = refs[3 + used + has_acc : -1]
    loads = w_copies(w_hbm, chunks, w_refs, refs[-1], 0)
    for copy in loads:
        copy.start()

    def body(columns):
        total = product(mixed, w_used, columns)
        if has_acc:
            total += acc_in[:, columns]
        acc_ref[:, columns] = total

    column_tiles(z.out_columns, body)
    for copy in loads:
        copy.wait()


def last_kernel(z, held, chunks, *refs):
    w_hbm, acc_in = refs[:2]
    mixed = refs[2 : 2 + PARTS]
    w_held = refs[2 + PARTS : 2 + PARTS + held]
    first_ref, second_ref, token, w_late, acc, sems = refs[2 + PARTS + held :]
    token[...] = jnp.zeros_like(token)
    loads = w_copies(w_hbm, chunks, [w_late.at[i] for i in range(len(chunks))], sems, 0)
    for copy in loads:
        copy.start()
    per_part = CHUNKS // (2 * PARTS)
    rows = z.chunk_rows

    def mixed_of(k):
        return mixed[k // per_part][:, (k % per_part) * rows : (k % per_part + 1) * rows]

    def early(columns):
        total = acc_in[:, columns]
        for k in range(held):
            total += jnp.dot(mixed_of(k), w_held[k][:, columns], preferred_element_type=F32)
        acc[:, columns] = total

    column_tiles(z.out_columns, early)
    for copy in loads:
        copy.wait()

    def late(columns):
        total = acc[:, columns]
        for i in range(len(chunks)):
            total += jnp.dot(
                mixed_of(held + i), w_late[i, :, columns], preferred_element_type=F32
            )
        first_ref[:, columns] = total[: z.rows_of].astype(BF16)
        second_ref[:, columns] = total[z.step_rows : z.step_rows + z.rows_of].astype(BF16)

    column_tiles(z.out_columns, late)


def place_kernel(z, *refs):
    plan_vmem = refs[0]
    arrived = refs[1 : z.inst_count]
    kv_out, plan, sems = refs[1 + z.inst_count :]
    plan_copy = copy_of(plan_vmem, plan, sems.at[0])
    plan_copy.start()
    plan_copy.wait()

    def each(act):
        for s in range(z.inst_count - 1):
            for j in range(z.per_rank):
                slot = read(plan, z.at_place + s * z.per_rank + j)

                @pl.when(slot >= 0)
                def _():
                    act(copy_of(arrived[s].at[j], kv_out.at[slot], sems.at[1]))

    each(lambda copy: copy.start())
    each(lambda copy: copy.wait())


def local(qkv_first, qkv_second, w_out, kv_cache, lengths, page_table, moves, dest_pages):
    n = lax.axis_size("tp")
    inst_count = lax.axis_size("inst")
    moves = moves.T
    rows_of, max_pages = page_table.shape
    z = Sizes(n, inst_count, rows_of, max_pages // n, kv_cache.shape, w_out.shape)
    smem = pltpu.SMEM
    dma = pltpu.SemaphoreType.DMA
    w_hbm = in_hbm(w_out)
    chunk = (shape((z.chunk_rows, z.out_columns)), VMEM)
    page = kv_cache.shape[1:]

    def swap(x, d):
        return lax.ppermute(x, "tp", [(i, i ^ d) for i in range(n)])

    stages = []
    while (1 << len(stages)) < n:
        stages.append(1 << len(stages))

    w = {}
    took = (0,)
    pages, own_first, own_second, visible, plan, *loaded = run(
        functools.partial(prepare_kernel, z, took),
        "prepare",
        2,
        [HBM] * 8,
        [
            (shape((z.pool + 2,) + page), VMEM),
            (shape(qkv_first.shape), VMEM),
            (shape(qkv_second.shape), VMEM),
            (shape((z.all_rows, z.positions), I32), VMEM),
            (shape((z.plan_rows, LANES), I32), VMEM),
        ]
        + [chunk] * len(took),
        [
            smem(lengths.shape, I32),
            smem(page_table.shape, I32),
            smem(moves.shape, I32),
            smem(dest_pages.shape, I32),
            smem((z.plan_rows * LANES,), I32),
            dma((7 + len(took),)),
        ],
        [w_hbm]
        + [
            in_hbm(x)
            for x in (kv_cache, qkv_first, qkv_second, lengths, page_table, moves, dest_pages)
        ],
    )
    w.update(zip(took, loaded))

    have = {0: (qkv_first, qkv_second)}
    for d in stages[1:] + stages[:1]:
        for e, pair in list(have.items()):
            if d == 1 and e:
                pair = tuple(behind(x, plan) for x in pair)
            have[e ^ d] = tuple(swap(x, d) for x in pair)
    have[0] = (own_first, own_second)
    pieces = [x for d in range(n) for x in have[d]]

    took = (1, 2)
    partial_out = [
        (shape((z.all_rows, z.packed)), VMEM),
        (shape((z.all_rows, z.part_width), F32), VMEM),
        (shape((z.all_rows, LANES), F32), VMEM),
    ]
    send, acc, stats = [None] * PARTS, [None] * PARTS, [None] * PARTS
    results = run(
        functools.partial(attend_first_kernel, z, took),
        "attend0",
        2,
        [HBM] + [VMEM] * (3 + 2 * n),
        partial_out
        + [
            (shape((z.all_rows, z.q_width + 2 * z.kv_width)), VMEM),
            (shape(pages.shape), VMEM),
            (shape(kv_cache.shape), HBM),
        ]
        + [(shape((z.per_rank,) + page), VMEM)] * (inst_count - 1)
        + [chunk] * len(took),
        [smem((z.plan_rows, LANES), I32), dma((3 + len(took),))],
        [w_hbm, plan, visible, pages, *pieces],
        aliases={3: 4},
    )
    send[0], acc[0], stats[0], rows, pages, kv_mid = results[:6]
    outgoing = results[6 : 5 + inst_count]
    w.update(zip(took, results[5 + inst_count :]))

    theirs = [None] * PARTS
    theirs[0] = swap(send[0], 1)
    took = (3,)
    for part in range(1, PARTS):
        send[part], acc[part], stats[part], *loaded = run(
            functools.partial(attend_more_kernel, z, part, took),
            f"attend{part}",
            1.5,
            [HBM] + [VMEM] * 3,
            partial_out + [chunk] * len(took),
            [dma((len(took),))],
            [w_hbm, visible, rows, pages],
        )
        w.update(zip(took, loaded))
        theirs[part] = swap(send[part], 1)

    for d in stages[1:]:
        for part in range(PARTS):
            acc[part], stats[part], send[part] = run(
                functools.partial(merge_kernel, z),
                f"merge{d}_{part}",
                0.2,
                [VMEM] * 3,
                [partial_out[1], partial_out[2], partial_out[0]],
                [],
                [acc[part], stats[part], theirs[part]],
            )
            theirs[part] = swap(send[part], d)

    outgoing = [behind(x, stats[PARTS - 1]) for x in outgoing]
    arrived = [
        lax.ppermute(
            outgoing[s - 1], "inst", [(i, (i + s) % inst_count) for i in range(inst_count)]
        )
        for s in range(1, inst_count)
    ]
    took = (4,)
    w.update(
        zip(
            took,
            run(
                functools.partial(stage_kernel, took),
                "stage",
                1.5,
                [HBM],
                [chunk] * len(took),
                [dma((len(took),))],
                [w_hbm],
                after=[stats[PARTS - 1]],
            ),
        )
    )

    total = None
    mixed, others = [], []
    per_part = CHUNKS // (2 * PARTS)
    for part in range(PARTS):
        (ready,) = run(
            functools.partial(finish_kernel, z),
            f"finish{part}",
            0.3,
            [VMEM] * 3,
            [(shape((z.all_rows, z.part_width)), VMEM)],
            [],
            [acc[part], stats[part], theirs[part]],
            after=[] if total is None else [total],
        )
        others.append(swap(ready, 1))
        took = (5 + part,)
        weights = [w[part * per_part + k] for k in range(per_part)]
        before = [] if total is None else [total]
        total, *loaded = run(
            functools.partial(project_kernel, z, per_part, took, len(before)),
            f"project{part}",
            1.6,
            [HBM] + [VMEM] * (1 + per_part + len(before)),
            [(shape((z.all_rows, z.out_columns), F32), VMEM)] + [chunk] * len(took),
            [dma((len(took),))],
            [w_hbm, ready, *weights, *before],
        )
        w.update(zip(took, loaded))

    held = [w[k] for k in range(CHUNKS // 2, CHUNKS) if k in w]
    late = tuple(range(CHUNKS // 2 + len(held), CHUNKS))
    out_first, out_second, token = run(
        functools.partial(last_kernel, z, len(held), late),
        "last",
        3,
        [HBM] + [VMEM] * (1 + PARTS + len(held)),
        [(shape((rows_of, z.out_columns)), VMEM)] * 2 + [(shape((8, LANES), I32), VMEM)],
        [
            pltpu.VMEM((max(len(late), 1), z.chunk_rows, z.out_columns), BF16),
            pltpu.VMEM((z.all_rows, z.out_columns), F32),
            dma((max(len(late), 1),)),
        ],
        [w_hbm, total, *others, *held],
    )
    (kv_out,) = run(
        functools.partial(place_kernel, z),
        "place",
        1,
        [VMEM] * inst_count + [HBM],
        [(shape(kv_cache.shape), HBM)],
        [smem((z.plan_rows, LANES), I32), dma((2,))],
        [plan, *arrived, kv_mid],
        aliases={inst_count: 0},
        after=[token],
    )
    return out_first, out_second, kv_out


def solution(mesh):
    placed = (
        P(("groups", "inst"), "tp"),
        P(("groups", "inst"), "tp"),
        P(None, "tp"),
        P(("groups", "inst", "tp"), None, None, None),
        P("groups"),
        P(("groups", "inst"), None),
        P("groups", None),
        P("groups", None),
    )
    return jax.shard_map(
        local,
        mesh=mesh,
        in_specs=placed,
        out_specs=(
            P(("groups", "inst"), "tp"),
            P(("groups", "inst"), "tp"),
            P(("groups", "inst", "tp"), None, None, None),
        ),
        check_vma=False,
    )
```

```python
import functools
import math

import jax
import jax.numpy as jnp
from jax import lax
from jax.experimental import pallas as pl
from jax.experimental.pallas import tpu as pltpu
from jax.sharding import PartitionSpec as P

HEAD_SIZE = 128
LANES = 128
NEG_LARGE = -1e30
BF16 = jnp.bfloat16
F32 = jnp.float32
I32 = jnp.int32
VMEM = pltpu.VMEM
HBM = pltpu.HBM
TILE = 256
PARTS = 1
CHUNKS = 8
FLOPS = 3e8
BYTES = 0
copy_of = pltpu.make_async_copy


def spec(space):
    return pl.BlockSpec(memory_space=space)


def in_hbm(x):
    return pltpu.with_memory_space_constraint(x, HBM)


def shape(dims, dtype=BF16):
    return jax.ShapeDtypeStruct(dims, dtype)


def run(kernel, micros, ins, outs, scratch, args, aliases=None, after=(), limit=8):
    count = len(ins)

    def body(*refs):
        kernel(*refs[:count], *refs[count + len(after) :])

    ins = list(ins) + [pl.ANY] * len(after)
    args = list(args) + list(after)
    return pl.pallas_call(
        body,
        out_shape=tuple(s for s, _ in outs),
        in_specs=[spec(space) for space in ins],
        out_specs=tuple(spec(space) for _, space in outs),
        scratch_shapes=scratch,
        input_output_aliases=aliases or {},
        compiler_params=pltpu.CompilerParams(vmem_limit_bytes=limit << 20),
        cost_estimate=pl.CostEstimate(
            flops=int(micros * FLOPS), bytes_accessed=int(micros * BYTES), transcendentals=0
        ),
    )(*args)


def behind(x, token):
    return lax.optimization_barrier((x, token))[0]


def rounded_up(x, to):
    return -(-x // to) * to


class Sizes:
    def __init__(self, n, inst_count, rows_of, per_rank, kv_shape, w_shape):
        self.n = n
        self.inst_count = inst_count
        self.rows_of = rows_of
        self.per_rank = per_rank
        self.pool, _, self.extent, self.kv_width = kv_shape
        self.q_width, self.out_columns = w_shape
        self.q_heads = self.q_width // HEAD_SIZE
        self.kv_heads = self.kv_width // HEAD_SIZE
        self.group = self.q_heads // self.kv_heads
        self.step_rows = rounded_up(rows_of, 8)
        self.all_rows = 2 * self.step_rows
        self.positions = self.pool * self.extent
        self.part_groups = self.kv_heads // (2 * PARTS)
        self.part_heads = self.part_groups * self.group
        self.part_width = self.part_heads * HEAD_SIZE
        self.per_tile = LANES // (2 * self.part_heads)
        self.packed = self.part_width + LANES * -(-3 // self.per_tile)
        self.chunk_rows = self.q_width // CHUNKS
        self.early = 2
        while self.early * (self.q_width + 2 * self.kv_width) < n * 2 * self.kv_width:
            self.early *= 2
        self.at_offset = 2 * rows_of
        self.at_source = 4 * rows_of
        self.at_place = self.at_source + self.pool
        self.plan_rows = rounded_up(
            -(-(self.at_place + (inst_count - 1) * per_rank) // LANES), 8
        )


def w_copies(w_hbm, chunks, refs, sems, first=0):
    rows = w_hbm.shape[0] // CHUNKS
    side = lax.rem(lax.axis_index("tp"), 2)
    copies = []
    for i, k in enumerate(chunks):
        half = side if k < CHUNKS // 2 else 1 - side
        start = half * (w_hbm.shape[0] // 2) + (k % (CHUNKS // 2)) * rows
        source = w_hbm.at[pl.ds(pl.multiple_of(start, LANES), rows)]
        copies.append(copy_of(source, refs[i], sems.at[first + i]))
    return copies


def prepare_kernel(z, chunks, *refs):
    m = 2 * z.early
    w_hbm, kv_hbm, lengths_hbm, table_hbm, moves_hbm, dest_hbm, first_hbm, second_hbm = refs[:8]
    pieces = (None, None) + refs[8 : 6 + m]
    pages, rows, visible_ref, plan_ref = refs[6 + m : 10 + m]
    outgoing = refs[10 + m : 9 + m + z.inst_count]
    w_refs = refs[9 + m + z.inst_count : 9 + m + z.inst_count + len(chunks)]
    first, second, lengths, table, moves, dest, plan, sems = refs[9 + m + z.inst_count + len(chunks) :]
    me = lax.axis_index("tp")
    inst = lax.axis_index("inst")
    small = [
        copy_of(table_hbm, table, sems.at[1]),
        copy_of(moves_hbm, moves, sems.at[2]),
        copy_of(lengths_hbm, lengths, sems.at[0]),
        copy_of(dest_hbm, dest, sems.at[3]),
    ]
    own = [copy_of(first_hbm, first, sems.at[5]), copy_of(second_hbm, second, sems.at[6])]
    kv_copy = copy_of(kv_hbm, pages.at[pl.ds(0, z.pool)], sems.at[4])
    for copy in small + own + [kv_copy]:
        copy.start()
    pages[z.pool] = jnp.zeros_like(pages[z.pool])
    rows[...] = jnp.zeros_like(rows)
    for copy in small:
        copy.wait()

    def sends(i, act):
        request = moves[0, i]
        origin = lax.div(request, z.rows_of)
        slot = lax.bitwise_xor(moves[1, i], origin)
        row = request - inst * z.rows_of
        for s in range(1, z.inst_count):

            @pl.when((origin == inst) & (slot == s))
            def _():
                for j in range(z.per_rank):
                    local = table[row, me + z.n * j] - me * z.pool
                    act(copy_of(kv_hbm.at[local], outgoing[s - 1].at[j], sems.at[7]))

    for i in range(moves.shape[1]):
        sends(i, lambda copy: copy.start())
    w_loads = w_copies(w_hbm, chunks, w_refs, sems, 8)
    for copy in w_loads:
        copy.start()

    grid = (z.all_rows, z.positions)
    at = lax.broadcasted_iota(I32, grid, 1)
    row = lax.broadcasted_iota(I32, grid, 0)
    step = lax.div(row, z.step_rows)
    row_of = row - step * z.step_rows
    page_of = lax.div(at, z.extent)
    offset = at - page_of * z.extent
    newest = jnp.full(grid, -1, I32)
    place = jnp.full(grid, 1 << 30, I32)
    for r in range(z.rows_of):
        here = row_of == r
        newest = jnp.where(here, lengths[inst * z.rows_of + r], newest)
        for j in range(z.per_rank):
            number = me + z.n * j
            local = table[r, number] - me * z.pool
            place = jnp.where(here & (page_of == local), number * z.extent + offset, place)
    visible_ref[...] = (place <= newest + step).astype(I32)

    for k in range(2):
        for r in range(z.rows_of):
            position = lengths[inst * z.rows_of + r] + k
            local = table[r, lax.div(position, z.extent)] - me * z.pool
            mine = (local >= 0) & (local < z.pool)
            plan[k * z.rows_of + r] = jnp.where(mine, local, z.pool + 1)
            plan[z.at_offset + k * z.rows_of + r] = lax.rem(position, z.extent)
    for p in range(z.pool):
        plan[z.at_source + p] = p
    for k in range((z.inst_count - 1) * z.per_rank):
        plan[z.at_place + k] = -1
    for i in range(moves.shape[1]):
        request = moves[0, i]
        target = moves[1, i]
        origin = lax.div(request, z.rows_of)
        slot = lax.bitwise_xor(target, origin)

        @pl.when((origin == inst) & (slot > 0))
        def _():
            for j in range(z.per_rank):
                local = table[request - inst * z.rows_of, me + z.n * j] - me * z.pool
                plan[z.at_source + local] = z.pool

        @pl.when((target == inst) & (slot > 0))
        def _():
            for j in range(z.per_rank):
                plan[z.at_place + (slot - 1) * z.per_rank + j] = dest[i, me + z.n * j] - me * z.pool

    where = lax.broadcasted_iota(I32, plan_ref.shape, 0) * LANES + lax.broadcasted_iota(
        I32, plan_ref.shape, 1
    )
    packed = jnp.zeros(plan_ref.shape, I32)
    for k in range(z.at_place + (z.inst_count - 1) * z.per_rank):
        packed = jnp.where(where == k, plan[k], packed)
    plan_ref[...] = packed

    for copy in own:
        copy.wait()
    put_pieces(z, rows, range(z.early), (first, second) + pieces[2:])
    fresh = rows[:, z.q_width :].astype(F32)
    line_id = lax.broadcasted_iota(I32, fresh.shape, 0)
    row_id = lax.broadcasted_iota(I32, (z.extent, z.kv_width), 0)
    for i in range(moves.shape[1]):
        sends(i, lambda copy: copy.wait())
    for i in range(moves.shape[1]):
        request = moves[0, i]
        origin = lax.div(request, z.rows_of)
        slot = lax.bitwise_xor(moves[1, i], origin)
        r = request - inst * z.rows_of
        for s in range(1, z.inst_count):

            @pl.when((origin == inst) & (slot == s) & (me >= z.n - 2))
            def _():
                for k in range(2):
                    position = lengths[request] + k
                    number = lax.div(position, z.extent)
                    chosen = line_id == k * z.step_rows + r
                    new = jnp.sum(jnp.where(chosen, fresh, 0.0), axis=0, keepdims=True)
                    target = jnp.where(
                        number == me + z.n * (z.per_rank - 1), lax.rem(position, z.extent), -1
                    )
                    for kv in range(2):
                        old = outgoing[s - 1][z.per_rank - 1, kv].astype(F32)
                        outgoing[s - 1][z.per_rank - 1, kv] = jnp.where(
                            row_id == target, new[:, kv * z.kv_width : (kv + 1) * z.kv_width], old
                        ).astype(BF16)

    for copy in [kv_copy] + w_loads:
        copy.wait()


def put_pieces(z, rows, which, pieces):
    me = lax.axis_index("tp")
    width = pieces[0].shape[1]
    for i, d in enumerate(which):
        start = pl.multiple_of((me ^ d) * width, LANES)
        for k in range(2):
            rows[k * z.step_rows : k * z.step_rows + z.rows_of, pl.ds(start, width)] = pieces[
                2 * i + k
            ][...]


def read(plan, k):
    return plan[k // LANES, k % LANES]


def attend_part(z, part, rows, pages, visible, send_ref, keep_ref, stats_ref):
    side = lax.rem(lax.axis_index("tp"), 2)
    half = z.kv_heads // 2
    lane = lax.broadcasted_iota(I32, (z.all_rows, LANES), 1)
    scale = 1.0 / math.sqrt(HEAD_SIZE)
    stats = [jnp.zeros((z.all_rows, LANES), F32) for _ in range(2)]
    for i in range(2 * z.part_groups):
        kept, k = divmod(i, z.part_groups)
        g = (side if kept else 1 - side) * half + part * z.part_groups + k
        q = jnp.concatenate(
            [
                rows[:, pl.ds(pl.multiple_of((g * z.group + h) * HEAD_SIZE, LANES), HEAD_SIZE)]
                for h in range(z.group)
            ],
            axis=0,
        )
        columns = pl.ds(pl.multiple_of(g * HEAD_SIZE, LANES), HEAD_SIZE)
        keys = pages[0 : z.pool, 0, :, columns].reshape(z.positions, HEAD_SIZE)
        values = pages[0 : z.pool, 1, :, columns].reshape(z.positions, HEAD_SIZE)
        scores = lax.dot_general(q, keys, (((1,), (1,)), ((), ())), preferred_element_type=F32)
        scores = (scores * scale).reshape(z.group, z.all_rows, z.positions)
        scores = jnp.where(visible, scores, NEG_LARGE)
        top = jnp.max(scores, axis=2, keepdims=True)
        exponent = jnp.where(visible, jnp.exp(scores - top), 0.0)
        total = jnp.sum(exponent, axis=2, keepdims=True)
        summed = jnp.dot(
            exponent.astype(BF16).reshape(z.group * z.all_rows, z.positions),
            values,
            preferred_element_type=F32,
        )
        for h in range(z.group):
            head = k * z.group + h
            piece = summed[h * z.all_rows : (h + 1) * z.all_rows]
            out_columns = slice(head * HEAD_SIZE, (head + 1) * HEAD_SIZE)
            if kept:
                keep_ref[:, out_columns] = piece
            else:
                send_ref[:, out_columns] = piece.astype(BF16)
            stats[kept] = jnp.where(lane == head, top[h], stats[kept])
            stats[kept] = jnp.where(lane == z.part_heads + head, total[h], stats[kept])
    put_stats(z, send_ref, stats[0])
    stats_ref[...] = stats[1]


def put_stats(z, ref, stats):
    used = 2 * z.part_heads
    lane = lax.broadcasted_iota(I32, stats.shape, 1)
    rest = stats
    tiles = {}
    for k in range(3):
        term = rest.astype(BF16).astype(F32)
        rest = rest - term
        tile, at = divmod(k, z.per_tile)
        if at:
            term = jnp.where(lane < at * used, tiles[tile], pltpu.roll(term, at * used, 1))
        tiles[tile] = term
    for tile, value in tiles.items():
        start = z.part_width + tile * LANES
        ref[:, start : start + LANES] = value.astype(BF16)


def get_stats(z, ref):
    used = 2 * z.part_heads
    stats = 0.0
    for k in range(3):
        tile, at = divmod(k, z.per_tile)
        start = z.part_width + tile * LANES
        term = ref[:, start : start + LANES].astype(F32)
        stats += pltpu.roll(term, LANES - at * used, 1) if at else term
    lane = lax.broadcasted_iota(I32, stats.shape, 1)
    return jnp.where(lane < used, stats, 0.0)


def attend_kernel(z, chunks, *refs):
    m = 2 * (z.n - z.early)
    w_hbm, plan_vmem, visible_ref, _, _ = refs[:5]
    pieces = refs[5 : 5 + m]
    send_ref, keep_ref, stats_ref, rows, pages, kv_out = refs[5 + m : 11 + m]
    w_refs = refs[11 + m : 11 + m + len(chunks)]
    plan, sems = refs[11 + m + len(chunks) :]
    w_loads = w_copies(w_hbm, chunks, w_refs, sems, 2)
    for copy in w_loads:
        copy.start()
    plan_copy = copy_of(plan_vmem, plan, sems.at[0])
    plan_copy.start()
    put_pieces(z, rows, range(z.early, z.n), pieces)
    plan_copy.wait()

    fresh = rows[:, z.q_width :].astype(F32)
    row_id = lax.broadcasted_iota(I32, (z.extent, z.kv_width), 0)
    for k in range(2):
        for r in range(z.rows_of):
            slot = read(plan, k * z.rows_of + r)
            here = row_id == read(plan, z.at_offset + k * z.rows_of + r)
            line = k * z.step_rows + r
            for kv in range(2):
                new = fresh[line : line + 1, kv * z.kv_width : (kv + 1) * z.kv_width]
                old = pages[slot, kv].astype(F32)
                pages[slot, kv] = jnp.where(here, new, old).astype(BF16)

    writes = [
        copy_of(pages.at[read(plan, z.at_source + p)], kv_out.at[p], sems.at[1])
        for p in range(z.pool)
    ]
    for copy in writes:
        copy.start()
    visible = (visible_ref[...] > 0)[None]
    attend_part(z, 0, rows, pages, visible, send_ref, keep_ref, stats_ref)
    for copy in writes + w_loads:
        copy.wait()


def joined(z, acc_ref, stats_ref, other_ref):
    mine = stats_ref[...]
    theirs = get_stats(z, other_ref)
    lane = lax.broadcasted_iota(I32, mine.shape, 1)
    top = jnp.maximum(mine, theirs)
    scale_mine = jnp.exp(mine - top)
    scale_theirs = jnp.exp(theirs - top)
    total = mine * pltpu.roll(scale_mine, z.part_heads, 1) + theirs * pltpu.roll(
        scale_theirs, z.part_heads, 1
    )
    stats = jnp.where(
        lane < z.part_heads, top, jnp.where(lane < 2 * z.part_heads, total, 0.0)
    )
    for h in range(z.part_heads):
        columns = slice(h * HEAD_SIZE, (h + 1) * HEAD_SIZE)
        piece = acc_ref[:, columns] * scale_mine[:, h : h + 1] + other_ref[:, columns].astype(
            F32
        ) * scale_theirs[:, h : h + 1]
        yield columns, piece, stats, h


def merge_kernel(z, acc_ref, stats_ref, other_ref, acc_out, stats_out, send_ref):
    for columns, piece, stats, _ in joined(z, acc_ref, stats_ref, other_ref):
        acc_out[:, columns] = piece
        send_ref[:, columns] = piece.astype(BF16)
    stats_out[...] = stats
    put_stats(z, send_ref, stats)


def finish_kernel(z, acc_ref, stats_ref, other_ref, mixed_ref):
    for columns, piece, stats, h in joined(z, acc_ref, stats_ref, other_ref):
        total = stats[:, z.part_heads + h : z.part_heads + h + 1]
        mixed_ref[:, columns] = (piece / total).astype(BF16)


def stage_kernel(chunks, w_hbm, *refs):
    loads = w_copies(w_hbm, chunks, refs, refs[-1])
    for copy in loads:
        copy.start()
    for copy in loads:
        copy.wait()


def column_tiles(width, body):
    @pl.loop(0, width // TILE)
    def _(t):
        body(pl.ds(pl.multiple_of(t * TILE, TILE), TILE))


def product(z, mixed, weights, columns, first=0):
    total = None
    for i, w in enumerate(weights):
        begin = (first + i) * z.chunk_rows
        term = jnp.dot(
            mixed[:, begin : begin + z.chunk_rows], w[:, columns], preferred_element_type=F32
        )
        total = term if total is None else total + term
    return total


def project_kernel(z, chunks, *refs):
    half = CHUNKS // 2
    w_hbm, mixed = refs[:2]
    weights = refs[2 : 2 + half]
    acc_ref = refs[2 + half]
    loads = w_copies(w_hbm, chunks, refs[3 + half :], refs[-1])
    for copy in loads:
        copy.start()

    def body(columns):
        acc_ref[:, columns] = product(z, mixed, weights, columns)

    column_tiles(z.out_columns, body)
    for copy in loads:
        copy.wait()


def last_kernel(z, held, chunks, *refs):
    w_hbm, acc_in, mixed, plan_vmem = refs[:4]
    weights = refs[4 : 4 + held]
    arrived = refs[4 + held : 3 + held + z.inst_count]
    first_ref, second_ref, kv_out, late, acc, plan, sems = refs[4 + held + z.inst_count :]
    plan_copy = copy_of(plan_vmem, plan, sems.at[0])
    plan_copy.start()
    late_refs = [late.at[i] for i in range(len(chunks))]
    loads = w_copies(w_hbm, chunks, late_refs, sems, 2)
    for copy in loads:
        copy.start()
    plan_copy.wait()

    def placed(act):
        for s in range(z.inst_count - 1):
            for j in range(z.per_rank):
                slot = read(plan, z.at_place + s * z.per_rank + j)

                @pl.when(slot >= 0)
                def _():
                    act(copy_of(arrived[s].at[j], kv_out.at[slot], sems.at[1]))

    placed(lambda copy: copy.start())

    def early(columns):
        acc[:, columns] = acc_in[:, columns] + product(z, mixed, weights, columns)

    column_tiles(z.out_columns, early)
    for i, copy in enumerate(loads):
        copy.wait()

        def body(columns):
            total = acc[:, columns] + product(z, mixed, [late_refs[i]], columns, held + i)
            if i < len(loads) - 1:
                acc[:, columns] = total
            else:
                first_ref[:, columns] = total[: z.rows_of].astype(BF16)
                second_ref[:, columns] = total[z.step_rows : z.step_rows + z.rows_of].astype(BF16)

        column_tiles(z.out_columns, body)
    placed(lambda copy: copy.wait())


def steps(qkv_first, qkv_second, w_out, kv_cache, lengths, page_table, moves, dest_pages):
    n = lax.axis_size("tp")
    inst_count = lax.axis_size("inst")
    moves = moves.T
    rows_of, max_pages = page_table.shape
    z = Sizes(n, inst_count, rows_of, max_pages // n, kv_cache.shape, w_out.shape)
    smem = pltpu.SMEM
    dma = pltpu.SemaphoreType.DMA
    page = kv_cache.shape[1:]

    def swap(x, d):
        return lax.ppermute(x, "tp", [(i, i ^ d) for i in range(n)])

    stages = []
    while (1 << len(stages)) < n:
        stages.append(1 << len(stages))

    w_hbm = in_hbm(w_out)
    chunk = (shape((z.chunk_rows, z.out_columns)), VMEM)
    have = {0: (qkv_first, qkv_second)}
    for d in range(1, z.early):
        have[d] = tuple(swap(x, d) for x in have[0])
    far = [d for d in stages if d >= z.early]
    for d in far:
        have[d] = tuple(swap(x, d) for x in have[0])
    pages, rows, visible, plan, *more = run(
        functools.partial(prepare_kernel, z, (0,)),
        2,
        [HBM] * 8 + [VMEM] * (2 * z.early - 2),
        [
            (shape((z.pool + 2,) + page), VMEM),
            (shape((z.all_rows, z.q_width + 2 * z.kv_width)), VMEM),
            (shape((z.all_rows, z.positions), I32), VMEM),
            (shape((z.plan_rows, LANES), I32), VMEM),
        ]
        + [(shape((z.per_rank,) + page), VMEM)] * (inst_count - 1)
        + [chunk],
        [
            pltpu.VMEM(qkv_first.shape, BF16),
            pltpu.VMEM(qkv_second.shape, BF16),
            smem(lengths.shape, I32),
            smem(page_table.shape, I32),
            smem(moves.shape, I32),
            smem(dest_pages.shape, I32),
            smem((z.plan_rows * LANES,), I32),
            dma((9,)),
        ],
        [w_hbm]
        + [
            in_hbm(x)
            for x in (kv_cache, lengths, page_table, moves, dest_pages, qkv_first, qkv_second)
        ]
        + [x for d in range(1, z.early) for x in have[d]],
    )
    outgoing, weights = more[:-1], more[-1:]
    for d in far:
        for e in range(1, d):
            have[d ^ e] = tuple(swap(behind(x, plan), e) for x in have[d])
    arrived = []
    for s in range(1, inst_count):
        arrived.append(
            lax.ppermute(outgoing[s - 1], "inst", [(i, i ^ s) for i in range(inst_count)])
        )

    send, acc, stats, _, _, kv_mid, *loaded = run(
        functools.partial(attend_kernel, z, (1,)),
        2,
        [HBM] + [VMEM] * (4 + 2 * (n - z.early)),
        [
            (shape((z.all_rows, z.packed)), VMEM),
            (shape((z.all_rows, z.part_width), F32), VMEM),
            (shape((z.all_rows, LANES), F32), VMEM),
            (shape(rows.shape), VMEM),
            (shape(pages.shape), VMEM),
            (shape(kv_cache.shape), HBM),
            chunk,
        ],
        [smem((z.plan_rows, LANES), I32), dma((3,))],
        [w_hbm, plan, visible, pages, rows] + [x for d in range(z.early, n) for x in have[d]],
        aliases={3: 4, 4: 3},
    )
    weights += loaded
    for d in stages[:-1]:
        acc, stats, send = run(
            functools.partial(merge_kernel, z),
            0.2,
            [VMEM] * 3,
            [
                (shape((z.all_rows, z.part_width), F32), VMEM),
                (shape((z.all_rows, LANES), F32), VMEM),
                (shape((z.all_rows, z.packed)), VMEM),
            ],
            [],
            [acc, stats, swap(send, d)],
        )
    theirs = swap(send, stages[-1])
    weights += run(
        functools.partial(stage_kernel, (2, 3)),
        3,
        [HBM],
        [chunk] * 2,
        [dma((2,))],
        [w_hbm],
        after=[stats],
    )
    (mixed,) = run(
        functools.partial(finish_kernel, z),
        0.3,
        [VMEM] * 3,
        [(shape((z.all_rows, z.part_width)), VMEM)],
        [],
        [acc, stats, theirs],
        after=weights[-1:],
    )
    other = swap(mixed, 1)
    total, *held = run(
        functools.partial(project_kernel, z, (4, 5)),
        3.4,
        [HBM] + [VMEM] * (1 + CHUNKS // 2),
        [(shape((z.all_rows, z.out_columns), F32), VMEM)] + [chunk] * 2,
        [dma((2,))],
        [w_hbm, mixed, *weights],
    )
    return tuple(
        run(
            functools.partial(last_kernel, z, 2, (6, 7)),
            3.4,
            [HBM] + [VMEM] * (4 + inst_count) + [HBM],
            [(shape((rows_of, z.out_columns)), VMEM)] * 2 + [(shape(kv_cache.shape), HBM)],
            [
                pltpu.VMEM((2, z.chunk_rows, z.out_columns), BF16),
                pltpu.VMEM((z.all_rows, z.out_columns), F32),
                smem((z.plan_rows, LANES), I32),
                dma((4,)),
            ],
            [w_hbm, total, other, plan, *held, *arrived, kv_mid],
            aliases={5 + inst_count: 2},
            limit=12,
        )
    )


def solution(mesh):
    placed = (
        P(("groups", "inst"), "tp"),
        P(("groups", "inst"), "tp"),
        P(None, "tp"),
        P(("groups", "inst", "tp"), None, None, None),
        P("groups"),
        P(("groups", "inst"), None),
        P("groups", None),
        P("groups", None),
    )
    return jax.shard_map(
        steps,
        mesh=mesh,
        in_specs=placed,
        out_specs=(
            P(("groups", "inst"), "tp"),
            P(("groups", "inst"), "tp"),
            P(("groups", "inst", "tp"), None, None, None),
        ),
        check_vma=False,
    )
```

```python
import functools
import math

import jax
import jax.numpy as jnp
from jax import lax
from jax.experimental import pallas as pl
from jax.experimental.pallas import tpu as pltpu
from jax.sharding import PartitionSpec as P

HEAD_SIZE = 128
LANES = 128
NEG_LARGE = -1e30
BF16 = jnp.bfloat16
F32 = jnp.float32
I32 = jnp.int32
VMEM = pltpu.VMEM
HBM = pltpu.HBM
TILE = 512
WIDE = 1024
PARTS = 1
CHUNKS = 8
FLOPS = 3e8
BYTES = 0
copy_of = pltpu.make_async_copy


def spec(space):
    return pl.BlockSpec(memory_space=space)


def in_hbm(x):
    return pltpu.with_memory_space_constraint(x, HBM)


def shape(dims, dtype=BF16):
    return jax.ShapeDtypeStruct(dims, dtype)


def run(kernel, micros, ins, outs, scratch, args, aliases=None, after=(), limit=8):
    count = len(ins)

    def body(*refs):
        kernel(*refs[:count], *refs[count + len(after) :])

    ins = list(ins) + [pl.ANY] * len(after)
    args = list(args) + list(after)
    return pl.pallas_call(
        body,
        out_shape=tuple(s for s, _ in outs),
        in_specs=[spec(space) for space in ins],
        out_specs=tuple(spec(space) for _, space in outs),
        scratch_shapes=scratch,
        input_output_aliases=aliases or {},
        compiler_params=pltpu.CompilerParams(vmem_limit_bytes=limit << 20),
        cost_estimate=pl.CostEstimate(
            flops=int(micros * FLOPS), bytes_accessed=int(micros * BYTES), transcendentals=0
        ),
    )(*args)


def behind(x, token):
    return lax.optimization_barrier((x, token))[0]


def rounded_up(x, to):
    return -(-x // to) * to


class Sizes:
    def __init__(self, n, inst_count, rows_of, per_rank, kv_shape, w_shape):
        self.n = n
        self.inst_count = inst_count
        self.rows_of = rows_of
        self.per_rank = per_rank
        self.pool, _, self.extent, self.kv_width = kv_shape
        self.q_width, self.out_columns = w_shape
        self.q_heads = self.q_width // HEAD_SIZE
        self.kv_heads = self.kv_width // HEAD_SIZE
        self.group = self.q_heads // self.kv_heads
        self.step_rows = rounded_up(rows_of, 8)
        self.all_rows = 2 * self.step_rows
        self.positions = self.pool * self.extent
        self.part_groups = self.kv_heads // (2 * PARTS)
        self.part_heads = self.part_groups * self.group
        self.part_width = self.part_heads * HEAD_SIZE
        self.per_tile = LANES // (2 * self.part_heads)
        self.packed = self.part_width + LANES * -(-3 // self.per_tile)
        self.chunk_rows = self.q_width // CHUNKS
        self.early = 2
        while self.early * (self.q_width + 2 * self.kv_width) < n * 2 * self.kv_width:
            self.early *= 2
        self.at_offset = 2 * rows_of
        self.at_source = 4 * rows_of
        self.at_place = self.at_source + self.pool
        self.plan_rows = rounded_up(
            -(-(self.at_place + (inst_count - 1) * per_rank) // LANES), 8
        )


def w_copies(w_hbm, chunks, refs, sems, first=0):
    rows = w_hbm.shape[0] // CHUNKS
    side = lax.rem(lax.axis_index("tp"), 2)
    copies = []
    for i, k in enumerate(chunks):
        half = side if k < CHUNKS // 2 else 1 - side
        start = half * (w_hbm.shape[0] // 2) + (k % (CHUNKS // 2)) * rows
        source = w_hbm.at[pl.ds(pl.multiple_of(start, LANES), rows)]
        copies.append(copy_of(source, refs[i], sems.at[first + i]))
    return copies


def prepare_kernel(z, chunks, *refs):
    m = 2 * z.early
    w_hbm, kv_hbm, lengths_hbm, table_hbm, moves_hbm, dest_hbm, first_hbm, second_hbm = refs[:8]
    pieces = (None, None) + refs[8 : 6 + m]
    pages, rows, visible_ref, plan_ref = refs[6 + m : 10 + m]
    outgoing = refs[10 + m : 9 + m + z.inst_count]
    w_refs = refs[9 + m + z.inst_count : 9 + m + z.inst_count + len(chunks)]
    first, second, lengths, table, moves, dest, plan, sems = refs[9 + m + z.inst_count + len(chunks) :]
    me = lax.axis_index("tp")
    inst = lax.axis_index("inst")
    small = [
        copy_of(table_hbm, table, sems.at[1]),
        copy_of(moves_hbm, moves, sems.at[2]),
        copy_of(lengths_hbm, lengths, sems.at[0]),
        copy_of(dest_hbm, dest, sems.at[3]),
    ]
    own = [copy_of(first_hbm, first, sems.at[5]), copy_of(second_hbm, second, sems.at[6])]
    kv_copy = copy_of(kv_hbm, pages.at[pl.ds(0, z.pool)], sems.at[4])
    for copy in small + own + [kv_copy]:
        copy.start()
    pages[z.pool] = jnp.zeros_like(pages[z.pool])
    rows[...] = jnp.zeros_like(rows)
    for copy in small:
        copy.wait()

    def sends(i, act):
        request = moves[0, i]
        origin = lax.div(request, z.rows_of)
        slot = lax.bitwise_xor(moves[1, i], origin)
        row = request - inst * z.rows_of
        for s in range(1, z.inst_count):

            @pl.when((origin == inst) & (slot == s))
            def _():
                for j in range(z.per_rank):
                    local = table[row, me + z.n * j] - me * z.pool
                    act(copy_of(kv_hbm.at[local], outgoing[s - 1].at[j], sems.at[7]))

    for i in range(moves.shape[1]):
        sends(i, lambda copy: copy.start())
    w_loads = w_copies(w_hbm, chunks, w_refs, sems, 8)
    for copy in w_loads:
        copy.start()

    grid = (z.all_rows, z.positions)
    at = lax.broadcasted_iota(I32, grid, 1)
    row = lax.broadcasted_iota(I32, grid, 0)
    step = lax.div(row, z.step_rows)
    row_of = row - step * z.step_rows
    page_of = lax.div(at, z.extent)
    offset = at - page_of * z.extent
    newest = jnp.full(grid, -1, I32)
    place = jnp.full(grid, 1 << 30, I32)
    for r in range(z.rows_of):
        here = row_of == r
        newest = jnp.where(here, lengths[inst * z.rows_of + r], newest)
        for j in range(z.per_rank):
            number = me + z.n * j
            local = table[r, number] - me * z.pool
            place = jnp.where(here & (page_of == local), number * z.extent + offset, place)
    visible_ref[...] = (place <= newest + step).astype(I32)

    for k in range(2):
        for r in range(z.rows_of):
            position = lengths[inst * z.rows_of + r] + k
            local = table[r, lax.div(position, z.extent)] - me * z.pool
            mine = (local >= 0) & (local < z.pool)
            plan[k * z.rows_of + r] = jnp.where(mine, local, z.pool + 1)
            plan[z.at_offset + k * z.rows_of + r] = lax.rem(position, z.extent)
    for p in range(z.pool):
        plan[z.at_source + p] = p
    for k in range((z.inst_count - 1) * z.per_rank):
        plan[z.at_place + k] = -1
    for i in range(moves.shape[1]):
        request = moves[0, i]
        target = moves[1, i]
        origin = lax.div(request, z.rows_of)
        slot = lax.bitwise_xor(target, origin)

        @pl.when((origin == inst) & (slot > 0))
        def _():
            for j in range(z.per_rank):
                local = table[request - inst * z.rows_of, me + z.n * j] - me * z.pool
                plan[z.at_source + local] = z.pool

        @pl.when((target == inst) & (slot > 0))
        def _():
            for j in range(z.per_rank):
                plan[z.at_place + (slot - 1) * z.per_rank + j] = dest[i, me + z.n * j] - me * z.pool

    where = lax.broadcasted_iota(I32, plan_ref.shape, 0) * LANES + lax.broadcasted_iota(
        I32, plan_ref.shape, 1
    )
    packed = jnp.zeros(plan_ref.shape, I32)
    for k in range(z.at_place + (z.inst_count - 1) * z.per_rank):
        packed = jnp.where(where == k, plan[k], packed)
    plan_ref[...] = packed

    for copy in own:
        copy.wait()
    put_pieces(z, rows, range(z.early), (first, second) + pieces[2:])
    fresh = rows[:, z.q_width :].astype(F32)
    line_id = lax.broadcasted_iota(I32, fresh.shape, 0)
    row_id = lax.broadcasted_iota(I32, (z.extent, z.kv_width), 0)
    for i in range(moves.shape[1]):
        sends(i, lambda copy: copy.wait())
    for i in range(moves.shape[1]):
        request = moves[0, i]
        origin = lax.div(request, z.rows_of)
        slot = lax.bitwise_xor(moves[1, i], origin)
        r = request - inst * z.rows_of
        for s in range(1, z.inst_count):

            @pl.when((origin == inst) & (slot == s) & (me >= z.n - 2))
            def _():
                for k in range(2):
                    position = lengths[request] + k
                    number = lax.div(position, z.extent)
                    chosen = line_id == k * z.step_rows + r
                    new = jnp.sum(jnp.where(chosen, fresh, 0.0), axis=0, keepdims=True)
                    target = jnp.where(
                        number == me + z.n * (z.per_rank - 1), lax.rem(position, z.extent), -1
                    )
                    for kv in range(2):
                        old = outgoing[s - 1][z.per_rank - 1, kv].astype(F32)
                        outgoing[s - 1][z.per_rank - 1, kv] = jnp.where(
                            row_id == target, new[:, kv * z.kv_width : (kv + 1) * z.kv_width], old
                        ).astype(BF16)

    for copy in [kv_copy] + w_loads:
        copy.wait()


def put_pieces(z, rows, which, pieces):
    me = lax.axis_index("tp")
    width = pieces[0].shape[1]
    for i, d in enumerate(which):
        start = pl.multiple_of((me ^ d) * width, LANES)
        for k in range(2):
            rows[k * z.step_rows : k * z.step_rows + z.rows_of, pl.ds(start, width)] = pieces[
                2 * i + k
            ][...]


def read(plan, k):
    return plan[k // LANES, k % LANES]


def attend_part(z, part, rows, pages, visible, send_ref, keep_ref, stats_ref):
    side = lax.rem(lax.axis_index("tp"), 2)
    half = z.kv_heads // 2
    lane = lax.broadcasted_iota(I32, (z.all_rows, LANES), 1)
    scale = 1.0 / math.sqrt(HEAD_SIZE)
    stats = [jnp.zeros((z.all_rows, LANES), F32) for _ in range(2)]
    for i in range(2 * z.part_groups):
        kept, k = divmod(i, z.part_groups)
        g = (side if kept else 1 - side) * half + part * z.part_groups + k
        q = jnp.concatenate(
            [
                rows[:, pl.ds(pl.multiple_of((g * z.group + h) * HEAD_SIZE, LANES), HEAD_SIZE)]
                for h in range(z.group)
            ],
            axis=0,
        )
        columns = pl.ds(pl.multiple_of(g * HEAD_SIZE, LANES), HEAD_SIZE)
        keys = pages[0 : z.pool, 0, :, columns].reshape(z.positions, HEAD_SIZE)
        values = pages[0 : z.pool, 1, :, columns].reshape(z.positions, HEAD_SIZE)
        scores = lax.dot_general(q, keys, (((1,), (1,)), ((), ())), preferred_element_type=F32)
        scores = (scores * scale).reshape(z.group, z.all_rows, z.positions)
        scores = jnp.where(visible, scores, NEG_LARGE)
        top = jnp.max(scores, axis=2, keepdims=True)
        exponent = jnp.where(visible, jnp.exp(scores - top), 0.0)
        total = jnp.sum(exponent, axis=2, keepdims=True)
        summed = jnp.dot(
            exponent.astype(BF16).reshape(z.group * z.all_rows, z.positions),
            values,
            preferred_element_type=F32,
        )
        for h in range(z.group):
            head = k * z.group + h
            piece = summed[h * z.all_rows : (h + 1) * z.all_rows]
            out_columns = slice(head * HEAD_SIZE, (head + 1) * HEAD_SIZE)
            if kept:
                keep_ref[:, out_columns] = piece
            else:
                send_ref[:, out_columns] = piece.astype(BF16)
            stats[kept] = jnp.where(lane == head, top[h], stats[kept])
            stats[kept] = jnp.where(lane == z.part_heads + head, total[h], stats[kept])
    put_stats(z, send_ref, stats[0])
    stats_ref[...] = stats[1]


def put_stats(z, ref, stats):
    used = 2 * z.part_heads
    lane = lax.broadcasted_iota(I32, stats.shape, 1)
    rest = stats
    tiles = {}
    for k in range(3):
        term = rest.astype(BF16).astype(F32)
        rest = rest - term
        tile, at = divmod(k, z.per_tile)
        if at:
            term = jnp.where(lane < at * used, tiles[tile], pltpu.roll(term, at * used, 1))
        tiles[tile] = term
    for tile, value in tiles.items():
        start = z.part_width + tile * LANES
        ref[:, start : start + LANES] = value.astype(BF16)


def get_stats(z, ref):
    used = 2 * z.part_heads
    stats = 0.0
    for k in range(3):
        tile, at = divmod(k, z.per_tile)
        start = z.part_width + tile * LANES
        term = ref[:, start : start + LANES].astype(F32)
        stats += pltpu.roll(term, LANES - at * used, 1) if at else term
    lane = lax.broadcasted_iota(I32, stats.shape, 1)
    return jnp.where(lane < used, stats, 0.0)


def attend_kernel(z, chunks, *refs):
    m = 2 * (z.n - z.early)
    w_hbm, plan_vmem, visible_ref, _, _ = refs[:5]
    pieces = refs[5 : 5 + m]
    send_ref, keep_ref, stats_ref, rows, pages, kv_out = refs[5 + m : 11 + m]
    w_refs = refs[11 + m : 11 + m + len(chunks)]
    plan, sems = refs[11 + m + len(chunks) :]
    w_loads = w_copies(w_hbm, chunks, w_refs, sems, 2)
    for copy in w_loads:
        copy.start()
    plan_copy = copy_of(plan_vmem, plan, sems.at[0])
    plan_copy.start()
    put_pieces(z, rows, range(z.early, z.n), pieces)
    plan_copy.wait()

    fresh = rows[:, z.q_width :].astype(F32)
    row_id = lax.broadcasted_iota(I32, (z.extent, z.kv_width), 0)
    for k in range(2):
        for r in range(z.rows_of):
            slot = read(plan, k * z.rows_of + r)
            here = row_id == read(plan, z.at_offset + k * z.rows_of + r)
            line = k * z.step_rows + r
            for kv in range(2):
                new = fresh[line : line + 1, kv * z.kv_width : (kv + 1) * z.kv_width]
                old = pages[slot, kv].astype(F32)
                pages[slot, kv] = jnp.where(here, new, old).astype(BF16)

    writes = [
        copy_of(pages.at[read(plan, z.at_source + p)], kv_out.at[p], sems.at[1])
        for p in range(z.pool)
    ]
    for copy in writes:
        copy.start()
    visible = (visible_ref[...] > 0)[None]
    attend_part(z, 0, rows, pages, visible, send_ref, keep_ref, stats_ref)
    for copy in writes + w_loads:
        copy.wait()


def joined(z, acc_ref, stats_ref, other_ref):
    mine = stats_ref[...]
    theirs = get_stats(z, other_ref)
    lane = lax.broadcasted_iota(I32, mine.shape, 1)
    top = jnp.maximum(mine, theirs)
    scale_mine = jnp.exp(mine - top)
    scale_theirs = jnp.exp(theirs - top)
    total = mine * pltpu.roll(scale_mine, z.part_heads, 1) + theirs * pltpu.roll(
        scale_theirs, z.part_heads, 1
    )
    stats = jnp.where(
        lane < z.part_heads, top, jnp.where(lane < 2 * z.part_heads, total, 0.0)
    )
    for h in range(z.part_heads):
        columns = slice(h * HEAD_SIZE, (h + 1) * HEAD_SIZE)
        piece = acc_ref[:, columns] * scale_mine[:, h : h + 1] + other_ref[:, columns].astype(
            F32
        ) * scale_theirs[:, h : h + 1]
        yield columns, piece, stats, h


def merge_kernel(z, acc_ref, stats_ref, other_ref, acc_out, stats_out, send_ref):
    for columns, piece, stats, _ in joined(z, acc_ref, stats_ref, other_ref):
        acc_out[:, columns] = piece
        send_ref[:, columns] = piece.astype(BF16)
    stats_out[...] = stats
    put_stats(z, send_ref, stats)


def finish_kernel(z, acc_ref, stats_ref, other_ref, mixed_ref):
    for columns, piece, stats, h in joined(z, acc_ref, stats_ref, other_ref):
        total = stats[:, z.part_heads + h : z.part_heads + h + 1]
        mixed_ref[:, columns] = (piece / total).astype(BF16)


def stage_kernel(chunks, w_hbm, *refs):
    loads = w_copies(w_hbm, chunks, refs, refs[-1])
    for copy in loads:
        copy.start()
    for copy in loads:
        copy.wait()


def column_tiles(width, body, tile=TILE):
    tile = min(tile, width)

    @pl.loop(0, width // tile)
    def _(t):
        body(pl.ds(pl.multiple_of(t * tile, tile), tile))


def product(z, mixed, weights, columns, first=0):
    total = None
    for i, w in enumerate(weights):
        begin = (first + i) * z.chunk_rows
        term = jnp.dot(
            mixed[:, begin : begin + z.chunk_rows], w[:, columns], preferred_element_type=F32
        )
        total = term if total is None else total + term
    return total


def project_kernel(z, chunks, *refs):
    half = CHUNKS // 2
    w_hbm, mixed = refs[:2]
    weights = refs[2 : 2 + half]
    acc_ref = refs[2 + half]
    loads = w_copies(w_hbm, chunks, refs[3 + half :], refs[-1])
    for copy in loads:
        copy.start()

    def body(columns):
        acc_ref[:, columns] = product(z, mixed, weights, columns)

    column_tiles(z.out_columns, body)
    for copy in loads:
        copy.wait()


def last_kernel(z, held, chunks, *refs):
    w_hbm, acc_in, mixed, plan_vmem = refs[:4]
    weights = refs[4 : 4 + held]
    arrived = refs[4 + held : 3 + held + z.inst_count]
    first_ref, second_ref, kv_out, late, acc, plan, sems = refs[4 + held + z.inst_count :]
    plan_copy = copy_of(plan_vmem, plan, sems.at[0])
    plan_copy.start()
    late_refs = [late.at[i] for i in range(len(chunks))]
    loads = w_copies(w_hbm, chunks, late_refs, sems, 2)
    for copy in loads:
        copy.start()
    plan_copy.wait()

    def placed(act):
        for s in range(z.inst_count - 1):
            for j in range(z.per_rank):
                slot = read(plan, z.at_place + s * z.per_rank + j)

                @pl.when(slot >= 0)
                def _():
                    act(copy_of(arrived[s].at[j], kv_out.at[slot], sems.at[1]))

    placed(lambda copy: copy.start())

    def early(columns):
        acc[:, columns] = acc_in[:, columns] + product(z, mixed, weights, columns)

    column_tiles(z.out_columns, early)
    for i, copy in enumerate(loads):
        copy.wait()

        def body(columns):
            total = acc[:, columns] + product(z, mixed, [late_refs[i]], columns, held + i)
            if i < len(loads) - 1:
                acc[:, columns] = total
            else:
                first_ref[:, columns] = total[: z.rows_of].astype(BF16)
                second_ref[:, columns] = total[z.step_rows : z.step_rows + z.rows_of].astype(BF16)

        column_tiles(z.out_columns, body, min(WIDE, z.out_columns))
    placed(lambda copy: copy.wait())


def steps(qkv_first, qkv_second, w_out, kv_cache, lengths, page_table, moves, dest_pages):
    n = lax.axis_size("tp")
    inst_count = lax.axis_size("inst")
    moves = moves.T
    rows_of, max_pages = page_table.shape
    z = Sizes(n, inst_count, rows_of, max_pages // n, kv_cache.shape, w_out.shape)
    smem = pltpu.SMEM
    dma = pltpu.SemaphoreType.DMA
    page = kv_cache.shape[1:]

    def swap(x, d):
        return lax.ppermute(x, "tp", [(i, i ^ d) for i in range(n)])

    stages = []
    while (1 << len(stages)) < n:
        stages.append(1 << len(stages))

    w_hbm = in_hbm(w_out)
    chunk = (shape((z.chunk_rows, z.out_columns)), VMEM)
    have = {0: (qkv_first, qkv_second)}
    for d in range(1, z.early):
        have[d] = tuple(swap(x, d) for x in have[0])
    far = [d for d in stages if d >= z.early]
    for d in far:
        have[d] = tuple(swap(x, d) for x in have[0])
    pages, rows, visible, plan, *more = run(
        functools.partial(prepare_kernel, z, (0,)),
        2,
        [HBM] * 8 + [VMEM] * (2 * z.early - 2),
        [
            (shape((z.pool + 2,) + page), VMEM),
            (shape((z.all_rows, z.q_width + 2 * z.kv_width)), VMEM),
            (shape((z.all_rows, z.positions), I32), VMEM),
            (shape((z.plan_rows, LANES), I32), VMEM),
        ]
        + [(shape((z.per_rank,) + page), VMEM)] * (inst_count - 1)
        + [chunk],
        [
            pltpu.VMEM(qkv_first.shape, BF16),
            pltpu.VMEM(qkv_second.shape, BF16),
            smem(lengths.shape, I32),
            smem(page_table.shape, I32),
            smem(moves.shape, I32),
            smem(dest_pages.shape, I32),
            smem((z.plan_rows * LANES,), I32),
            dma((9,)),
        ],
        [w_hbm]
        + [
            in_hbm(x)
            for x in (kv_cache, lengths, page_table, moves, dest_pages, qkv_first, qkv_second)
        ]
        + [x for d in range(1, z.early) for x in have[d]],
    )
    outgoing, weights = more[:-1], more[-1:]
    for d in far:
        for e in range(1, d):
            have[d ^ e] = tuple(swap(behind(x, plan), e) for x in have[d])
    arrived = []
    for s in range(1, inst_count):
        arrived.append(
            lax.ppermute(outgoing[s - 1], "inst", [(i, i ^ s) for i in range(inst_count)])
        )

    send, acc, stats, _, _, kv_mid, *loaded = run(
        functools.partial(attend_kernel, z, (1,)),
        2,
        [HBM] + [VMEM] * (4 + 2 * (n - z.early)),
        [
            (shape((z.all_rows, z.packed)), VMEM),
            (shape((z.all_rows, z.part_width), F32), VMEM),
            (shape((z.all_rows, LANES), F32), VMEM),
            (shape(rows.shape), VMEM),
            (shape(pages.shape), VMEM),
            (shape(kv_cache.shape), HBM),
            chunk,
        ],
        [smem((z.plan_rows, LANES), I32), dma((3,))],
        [w_hbm, plan, visible, pages, rows] + [x for d in range(z.early, n) for x in have[d]],
        aliases={3: 4, 4: 3},
    )
    weights += loaded
    for d in stages[:-1]:
        acc, stats, send = run(
            functools.partial(merge_kernel, z),
            0.2,
            [VMEM] * 3,
            [
                (shape((z.all_rows, z.part_width), F32), VMEM),
                (shape((z.all_rows, LANES), F32), VMEM),
                (shape((z.all_rows, z.packed)), VMEM),
            ],
            [],
            [acc, stats, swap(send, d)],
        )
    theirs = swap(send, stages[-1])
    weights += run(
        functools.partial(stage_kernel, (2, 3, 4)),
        3,
        [HBM],
        [chunk] * 3,
        [dma((3,))],
        [w_hbm],
        after=[stats],
    )
    (mixed,) = run(
        functools.partial(finish_kernel, z),
        0.3,
        [VMEM] * 3,
        [(shape((z.all_rows, z.part_width)), VMEM)],
        [],
        [acc, stats, theirs],
        after=weights[-1:],
    )
    other = swap(mixed, 1)
    total, *held = run(
        functools.partial(project_kernel, z, (5, 6)),
        3.4,
        [HBM] + [VMEM] * (1 + CHUNKS // 2),
        [(shape((z.all_rows, z.out_columns), F32), VMEM)] + [chunk] * 2,
        [dma((2,))],
        [w_hbm, mixed, *weights[:-1]],
    )
    held = weights[-1:] + held
    return tuple(
        run(
            functools.partial(last_kernel, z, 3, (7,)),
            3.4,
            [HBM] + [VMEM] * (5 + inst_count) + [HBM],
            [(shape((rows_of, z.out_columns)), VMEM)] * 2 + [(shape(kv_cache.shape), HBM)],
            [
                pltpu.VMEM((1, z.chunk_rows, z.out_columns), BF16),
                pltpu.VMEM((z.all_rows, z.out_columns), F32),
                smem((z.plan_rows, LANES), I32),
                dma((3,)),
            ],
            [w_hbm, total, other, plan, *held, *arrived, kv_mid],
            aliases={6 + inst_count: 2},
            limit=12,
        )
    )


def solution(mesh):
    placed = (
        P(("groups", "inst"), "tp"),
        P(("groups", "inst"), "tp"),
        P(None, "tp"),
        P(("groups", "inst", "tp"), None, None, None),
        P("groups"),
        P(("groups", "inst"), None),
        P("groups", None),
        P("groups", None),
    )
    return jax.shard_map(
        steps,
        mesh=mesh,
        in_specs=placed,
        out_specs=(
            P(("groups", "inst"), "tp"),
            P(("groups", "inst"), "tp"),
            P(("groups", "inst", "tp"), None, None, None),
        ),
        check_vma=False,
    )
```

```python
import functools
import math

import jax
import jax.numpy as jnp
from jax import lax
from jax.experimental import pallas as pl
from jax.experimental.pallas import tpu as pltpu
from jax.sharding import PartitionSpec as P

HEAD_SIZE = 128
LANES = 128
NEG_LARGE = -1e30
BF16 = jnp.bfloat16
F32 = jnp.float32
I32 = jnp.int32
VMEM = pltpu.VMEM
HBM = pltpu.HBM
TILE = 512
WIDE = 1024
PARTS = 1
PREPARE = 0.05
CHUNKS = 8
FLOPS = 3e8
BYTES = 0
copy_of = pltpu.make_async_copy


def spec(space):
    return pl.BlockSpec(memory_space=space)


def in_hbm(x):
    return pltpu.with_memory_space_constraint(x, HBM)


def shape(dims, dtype=BF16):
    return jax.ShapeDtypeStruct(dims, dtype)


def run(kernel, micros, ins, outs, scratch, args, aliases=None, after=(), limit=8):
    count = len(ins)

    def body(*refs):
        kernel(*refs[:count], *refs[count + len(after) :])

    ins = list(ins) + [pl.ANY] * len(after)
    args = list(args) + list(after)
    return pl.pallas_call(
        body,
        out_shape=tuple(s for s, _ in outs),
        in_specs=[spec(space) for space in ins],
        out_specs=tuple(spec(space) for _, space in outs),
        scratch_shapes=scratch,
        input_output_aliases=aliases or {},
        compiler_params=pltpu.CompilerParams(vmem_limit_bytes=limit << 20),
        cost_estimate=pl.CostEstimate(
            flops=int(micros * FLOPS), bytes_accessed=int(micros * BYTES), transcendentals=0
        ),
    )(*args)


def behind(x, token):
    return lax.optimization_barrier((x, token))[0]


def rounded_up(x, to):
    return -(-x // to) * to


class Sizes:
    def __init__(self, n, inst_count, rows_of, per_rank, kv_shape, w_shape):
        self.n = n
        self.inst_count = inst_count
        self.rows_of = rows_of
        self.per_rank = per_rank
        self.pool, _, self.extent, self.kv_width = kv_shape
        self.q_width, self.out_columns = w_shape
        self.q_heads = self.q_width // HEAD_SIZE
        self.kv_heads = self.kv_width // HEAD_SIZE
        self.group = self.q_heads // self.kv_heads
        self.step_rows = rounded_up(rows_of, 8)
        self.all_rows = 2 * self.step_rows
        self.positions = self.pool * self.extent
        self.part_groups = self.kv_heads // (2 * PARTS)
        self.part_heads = self.part_groups * self.group
        self.part_width = self.part_heads * HEAD_SIZE
        self.per_tile = LANES // (2 * self.part_heads)
        self.packed = self.part_width + LANES * -(-3 // self.per_tile)
        self.chunk_rows = self.q_width // CHUNKS
        self.early = 2
        while self.early * (self.q_width + 2 * self.kv_width) < n * 2 * self.kv_width:
            self.early *= 2
        self.at_offset = 2 * rows_of
        self.at_source = 4 * rows_of
        self.at_place = self.at_source + self.pool
        self.plan_rows = rounded_up(
            -(-(self.at_place + (inst_count - 1) * per_rank) // LANES), 8
        )


def w_copies(w_hbm, chunks, refs, sems, first=0):
    rows = w_hbm.shape[0] // CHUNKS
    side = lax.rem(lax.axis_index("tp"), 2)
    copies = []
    for i, k in enumerate(chunks):
        half = side if k < CHUNKS // 2 else 1 - side
        start = half * (w_hbm.shape[0] // 2) + (k % (CHUNKS // 2)) * rows
        source = w_hbm.at[pl.ds(pl.multiple_of(start, LANES), rows)]
        copies.append(copy_of(source, refs[i], sems.at[first + i]))
    return copies


def prepare_kernel(z, chunks, *refs):
    m = 2 * z.early
    w_hbm, kv_hbm, lengths_hbm, table_hbm, moves_hbm, dest_hbm, first_hbm, second_hbm = refs[:8]
    pieces = (None, None) + refs[8 : 6 + m]
    pages, rows, visible_ref, plan_ref = refs[6 + m : 10 + m]
    outgoing = refs[10 + m : 9 + m + z.inst_count]
    w_refs = refs[9 + m + z.inst_count : 9 + m + z.inst_count + len(chunks)]
    first, second, lengths, table, moves, dest, plan, sems = refs[9 + m + z.inst_count + len(chunks) :]
    me = lax.axis_index("tp")
    inst = lax.axis_index("inst")
    small = [
        copy_of(table_hbm, table, sems.at[1]),
        copy_of(moves_hbm, moves, sems.at[2]),
        copy_of(lengths_hbm, lengths, sems.at[0]),
        copy_of(dest_hbm, dest, sems.at[3]),
    ]
    own = [copy_of(first_hbm, first, sems.at[5]), copy_of(second_hbm, second, sems.at[6])]
    kv_copy = copy_of(kv_hbm, pages.at[pl.ds(0, z.pool)], sems.at[4])
    for copy in small + own + [kv_copy]:
        copy.start()
    pages[z.pool] = jnp.zeros_like(pages[z.pool])
    rows[...] = jnp.zeros_like(rows)
    for copy in small:
        copy.wait()

    def sends(i, act):
        request = moves[0, i]
        origin = lax.div(request, z.rows_of)
        slot = lax.bitwise_xor(moves[1, i], origin)
        row = request - inst * z.rows_of
        for s in range(1, z.inst_count):

            @pl.when((origin == inst) & (slot == s))
            def _():
                for j in range(z.per_rank):
                    local = table[row, me + z.n * j] - me * z.pool
                    act(copy_of(kv_hbm.at[local], outgoing[s - 1].at[j], sems.at[7]))

    for i in range(moves.shape[1]):
        sends(i, lambda copy: copy.start())
    w_loads = w_copies(w_hbm, chunks, w_refs, sems, 8)
    for copy in w_loads:
        copy.start()

    grid = (z.all_rows, z.positions)
    at = lax.broadcasted_iota(I32, grid, 1)
    row = lax.broadcasted_iota(I32, grid, 0)
    step = lax.div(row, z.step_rows)
    row_of = row - step * z.step_rows
    page_of = lax.div(at, z.extent)
    offset = at - page_of * z.extent
    newest = jnp.full(grid, -1, I32)
    place = jnp.full(grid, 1 << 30, I32)
    for r in range(z.rows_of):
        here = row_of == r
        newest = jnp.where(here, lengths[inst * z.rows_of + r], newest)
        for j in range(z.per_rank):
            number = me + z.n * j
            local = table[r, number] - me * z.pool
            place = jnp.where(here & (page_of == local), number * z.extent + offset, place)
    visible_ref[...] = (place <= newest + step).astype(I32)

    for k in range(2):
        for r in range(z.rows_of):
            position = lengths[inst * z.rows_of + r] + k
            local = table[r, lax.div(position, z.extent)] - me * z.pool
            mine = (local >= 0) & (local < z.pool)
            plan[k * z.rows_of + r] = jnp.where(mine, local, z.pool + 1)
            plan[z.at_offset + k * z.rows_of + r] = lax.rem(position, z.extent)
    for p in range(z.pool):
        plan[z.at_source + p] = p
    for k in range((z.inst_count - 1) * z.per_rank):
        plan[z.at_place + k] = -1
    for i in range(moves.shape[1]):
        request = moves[0, i]
        target = moves[1, i]
        origin = lax.div(request, z.rows_of)
        slot = lax.bitwise_xor(target, origin)

        @pl.when((origin == inst) & (slot > 0))
        def _():
            for j in range(z.per_rank):
                local = table[request - inst * z.rows_of, me + z.n * j] - me * z.pool
                plan[z.at_source + local] = z.pool

        @pl.when((target == inst) & (slot > 0))
        def _():
            for j in range(z.per_rank):
                plan[z.at_place + (slot - 1) * z.per_rank + j] = dest[i, me + z.n * j] - me * z.pool

    where = lax.broadcasted_iota(I32, plan_ref.shape, 0) * LANES + lax.broadcasted_iota(
        I32, plan_ref.shape, 1
    )
    packed = jnp.zeros(plan_ref.shape, I32)
    for k in range(z.at_place + (z.inst_count - 1) * z.per_rank):
        packed = jnp.where(where == k, plan[k], packed)
    plan_ref[...] = packed

    for copy in own:
        copy.wait()
    put_pieces(z, rows, range(z.early), (first, second) + pieces[2:])
    fresh = rows[:, z.q_width :].astype(F32)
    line_id = lax.broadcasted_iota(I32, fresh.shape, 0)
    row_id = lax.broadcasted_iota(I32, (z.extent, z.kv_width), 0)
    for i in range(moves.shape[1]):
        sends(i, lambda copy: copy.wait())
    for i in range(moves.shape[1]):
        request = moves[0, i]
        origin = lax.div(request, z.rows_of)
        slot = lax.bitwise_xor(moves[1, i], origin)
        r = request - inst * z.rows_of
        for s in range(1, z.inst_count):

            @pl.when((origin == inst) & (slot == s) & (me >= z.n - 2))
            def _():
                for k in range(2):
                    position = lengths[request] + k
                    number = lax.div(position, z.extent)
                    chosen = line_id == k * z.step_rows + r
                    new = jnp.sum(jnp.where(chosen, fresh, 0.0), axis=0, keepdims=True)
                    target = jnp.where(
                        number == me + z.n * (z.per_rank - 1), lax.rem(position, z.extent), -1
                    )
                    for kv in range(2):
                        old = outgoing[s - 1][z.per_rank - 1, kv].astype(F32)
                        outgoing[s - 1][z.per_rank - 1, kv] = jnp.where(
                            row_id == target, new[:, kv * z.kv_width : (kv + 1) * z.kv_width], old
                        ).astype(BF16)

    for copy in [kv_copy] + w_loads:
        copy.wait()


def put_pieces(z, rows, which, pieces):
    me = lax.axis_index("tp")
    width = pieces[0].shape[1]
    for i, d in enumerate(which):
        start = pl.multiple_of((me ^ d) * width, LANES)
        for k in range(2):
            rows[k * z.step_rows : k * z.step_rows + z.rows_of, pl.ds(start, width)] = pieces[
                2 * i + k
            ][...]


def read(plan, k):
    return plan[k // LANES, k % LANES]


def attend_part(z, part, rows, pages, visible, send_ref, keep_ref, stats_ref):
    side = lax.rem(lax.axis_index("tp"), 2)
    half = z.kv_heads // 2
    lane = lax.broadcasted_iota(I32, (z.all_rows, LANES), 1)
    scale = 1.0 / math.sqrt(HEAD_SIZE)
    stats = [jnp.zeros((z.all_rows, LANES), F32) for _ in range(2)]
    for i in range(2 * z.part_groups):
        kept, k = divmod(i, z.part_groups)
        g = (side if kept else 1 - side) * half + part * z.part_groups + k
        q = jnp.concatenate(
            [
                rows[:, pl.ds(pl.multiple_of((g * z.group + h) * HEAD_SIZE, LANES), HEAD_SIZE)]
                for h in range(z.group)
            ],
            axis=0,
        )
        columns = pl.ds(pl.multiple_of(g * HEAD_SIZE, LANES), HEAD_SIZE)
        keys = pages[0 : z.pool, 0, :, columns].reshape(z.positions, HEAD_SIZE)
        values = pages[0 : z.pool, 1, :, columns].reshape(z.positions, HEAD_SIZE)
        scores = lax.dot_general(q, keys, (((1,), (1,)), ((), ())), preferred_element_type=F32)
        scores = (scores * scale).reshape(z.group, z.all_rows, z.positions)
        scores = jnp.where(visible, scores, NEG_LARGE)
        top = jnp.max(scores, axis=2, keepdims=True)
        exponent = jnp.where(visible, jnp.exp(scores - top), 0.0)
        total = jnp.sum(exponent, axis=2, keepdims=True)
        summed = jnp.dot(
            exponent.astype(BF16).reshape(z.group * z.all_rows, z.positions),
            values,
            preferred_element_type=F32,
        )
        for h in range(z.group):
            head = k * z.group + h
            piece = summed[h * z.all_rows : (h + 1) * z.all_rows]
            out_columns = slice(head * HEAD_SIZE, (head + 1) * HEAD_SIZE)
            if kept:
                keep_ref[:, out_columns] = piece
            else:
                send_ref[:, out_columns] = piece.astype(BF16)
            stats[kept] = jnp.where(lane == head, top[h], stats[kept])
            stats[kept] = jnp.where(lane == z.part_heads + head, total[h], stats[kept])
    put_stats(z, send_ref, stats[0])
    stats_ref[...] = stats[1]


def put_stats(z, ref, stats):
    used = 2 * z.part_heads
    lane = lax.broadcasted_iota(I32, stats.shape, 1)
    rest = stats
    tiles = {}
    for k in range(3):
        term = rest.astype(BF16).astype(F32)
        rest = rest - term
        tile, at = divmod(k, z.per_tile)
        if at:
            term = jnp.where(lane < at * used, tiles[tile], pltpu.roll(term, at * used, 1))
        tiles[tile] = term
    for tile, value in tiles.items():
        start = z.part_width + tile * LANES
        ref[:, start : start + LANES] = value.astype(BF16)


def get_stats(z, ref):
    used = 2 * z.part_heads
    stats = 0.0
    for k in range(3):
        tile, at = divmod(k, z.per_tile)
        start = z.part_width + tile * LANES
        term = ref[:, start : start + LANES].astype(F32)
        stats += pltpu.roll(term, LANES - at * used, 1) if at else term
    lane = lax.broadcasted_iota(I32, stats.shape, 1)
    return jnp.where(lane < used, stats, 0.0)


def attend_kernel(z, chunks, *refs):
    m = 2 * (z.n - z.early)
    w_hbm, plan_vmem, visible_ref, _, _ = refs[:5]
    pieces = refs[5 : 5 + m]
    send_ref, keep_ref, stats_ref, rows, pages, kv_out = refs[5 + m : 11 + m]
    w_refs = refs[11 + m : 11 + m + len(chunks)]
    plan, sems = refs[11 + m + len(chunks) :]
    w_loads = w_copies(w_hbm, chunks, w_refs, sems, 2)
    for copy in w_loads:
        copy.start()
    plan_copy = copy_of(plan_vmem, plan, sems.at[0])
    plan_copy.start()
    put_pieces(z, rows, range(z.early, z.n), pieces)
    plan_copy.wait()

    fresh = rows[:, z.q_width :].astype(F32)
    row_id = lax.broadcasted_iota(I32, (z.extent, z.kv_width), 0)
    for k in range(2):
        for r in range(z.rows_of):
            slot = read(plan, k * z.rows_of + r)
            here = row_id == read(plan, z.at_offset + k * z.rows_of + r)
            line = k * z.step_rows + r
            for kv in range(2):
                new = fresh[line : line + 1, kv * z.kv_width : (kv + 1) * z.kv_width]
                old = pages[slot, kv].astype(F32)
                pages[slot, kv] = jnp.where(here, new, old).astype(BF16)

    writes = [
        copy_of(pages.at[read(plan, z.at_source + p)], kv_out.at[p], sems.at[1])
        for p in range(z.pool)
    ]
    for copy in writes:
        copy.start()
    visible = (visible_ref[...] > 0)[None]
    attend_part(z, 0, rows, pages, visible, send_ref, keep_ref, stats_ref)
    for copy in writes + w_loads:
        copy.wait()


def joined(z, acc_ref, stats_ref, other_ref):
    mine = stats_ref[...]
    theirs = get_stats(z, other_ref)
    lane = lax.broadcasted_iota(I32, mine.shape, 1)
    top = jnp.maximum(mine, theirs)
    scale_mine = jnp.exp(mine - top)
    scale_theirs = jnp.exp(theirs - top)
    total = mine * pltpu.roll(scale_mine, z.part_heads, 1) + theirs * pltpu.roll(
        scale_theirs, z.part_heads, 1
    )
    stats = jnp.where(
        lane < z.part_heads, top, jnp.where(lane < 2 * z.part_heads, total, 0.0)
    )
    for h in range(z.part_heads):
        columns = slice(h * HEAD_SIZE, (h + 1) * HEAD_SIZE)
        piece = acc_ref[:, columns] * scale_mine[:, h : h + 1] + other_ref[:, columns].astype(
            F32
        ) * scale_theirs[:, h : h + 1]
        yield columns, piece, stats, h


def merge_kernel(z, acc_ref, stats_ref, other_ref, acc_out, stats_out, send_ref):
    for columns, piece, stats, _ in joined(z, acc_ref, stats_ref, other_ref):
        acc_out[:, columns] = piece
        send_ref[:, columns] = piece.astype(BF16)
    stats_out[...] = stats
    put_stats(z, send_ref, stats)


def finish_kernel(z, acc_ref, stats_ref, other_ref, mixed_ref):
    for columns, piece, stats, h in joined(z, acc_ref, stats_ref, other_ref):
        total = stats[:, z.part_heads + h : z.part_heads + h + 1]
        mixed_ref[:, columns] = (piece / total).astype(BF16)


def stage_kernel(chunks, w_hbm, *refs):
    loads = w_copies(w_hbm, chunks, refs, refs[-1])
    for copy in loads:
        copy.start()
    for copy in loads:
        copy.wait()


def column_tiles(width, body, tile=TILE):
    tile = min(tile, width)

    @pl.loop(0, width // tile)
    def _(t):
        body(pl.ds(pl.multiple_of(t * tile, tile), tile))


def product(z, mixed, weights, columns, first=0):
    total = None
    for i, w in enumerate(weights):
        begin = (first + i) * z.chunk_rows
        term = jnp.dot(
            mixed[:, begin : begin + z.chunk_rows], w[:, columns], preferred_element_type=F32
        )
        total = term if total is None else total + term
    return total


def project_kernel(z, chunks, *refs):
    half = CHUNKS // 2
    w_hbm, mixed = refs[:2]
    weights = refs[2 : 2 + half]
    acc_ref = refs[2 + half]
    loads = w_copies(w_hbm, chunks, refs[3 + half :], refs[-1])
    for copy in loads:
        copy.start()

    def body(columns):
        acc_ref[:, columns] = product(z, mixed, weights, columns)

    column_tiles(z.out_columns, body)
    for copy in loads:
        copy.wait()


def last_kernel(z, held, chunks, *refs):
    w_hbm, acc_in, mixed, plan_vmem = refs[:4]
    weights = refs[4 : 4 + held]
    arrived = refs[4 + held : 3 + held + z.inst_count]
    first_ref, second_ref, kv_out, late, acc, plan, sems = refs[4 + held + z.inst_count :]
    plan_copy = copy_of(plan_vmem, plan, sems.at[0])
    plan_copy.start()
    late_refs = [late.at[i] for i in range(len(chunks))]
    loads = w_copies(w_hbm, chunks, late_refs, sems, 2)
    for copy in loads:
        copy.start()

    def placed(act):
        for s in range(z.inst_count - 1):
            for j in range(z.per_rank):
                slot = read(plan, z.at_place + s * z.per_rank + j)

                @pl.when(slot >= 0)
                def _():
                    act(copy_of(arrived[s].at[j], kv_out.at[slot], sems.at[1]))

    def early(columns):
        acc[:, columns] = acc_in[:, columns] + product(z, mixed, weights, columns)

    column_tiles(z.out_columns, early)
    plan_copy.wait()
    placed(lambda copy: copy.start())
    for i, copy in enumerate(loads):
        copy.wait()

        def body(columns):
            total = acc[:, columns] + product(z, mixed, [late_refs[i]], columns, held + i)
            if i < len(loads) - 1:
                acc[:, columns] = total
            else:
                first_ref[:, columns] = total[: z.rows_of].astype(BF16)
                second_ref[:, columns] = total[z.step_rows : z.step_rows + z.rows_of].astype(BF16)

        column_tiles(z.out_columns, body, min(WIDE, z.out_columns))
    placed(lambda copy: copy.wait())


def steps(qkv_first, qkv_second, w_out, kv_cache, lengths, page_table, moves, dest_pages):
    n = lax.axis_size("tp")
    inst_count = lax.axis_size("inst")
    moves = moves.T
    rows_of, max_pages = page_table.shape
    z = Sizes(n, inst_count, rows_of, max_pages // n, kv_cache.shape, w_out.shape)
    smem = pltpu.SMEM
    dma = pltpu.SemaphoreType.DMA
    page = kv_cache.shape[1:]

    def swap(x, d):
        return lax.ppermute(x, "tp", [(i, i ^ d) for i in range(n)])

    stages = []
    while (1 << len(stages)) < n:
        stages.append(1 << len(stages))

    w_hbm = in_hbm(w_out)
    chunk = (shape((z.chunk_rows, z.out_columns)), VMEM)
    have = {0: (qkv_first, qkv_second)}
    for d in range(1, z.early):
        have[d] = tuple(swap(x, d) for x in have[0])
    far = [d for d in stages if d >= z.early]
    for d in far:
        have[d] = tuple(swap(x, d) for x in have[0])
    pages, rows, visible, plan, *more = run(
        functools.partial(prepare_kernel, z, (0,)),
        PREPARE,
        [HBM] * 8 + [VMEM] * (2 * z.early - 2),
        [
            (shape((z.pool + 2,) + page), VMEM),
            (shape((z.all_rows, z.q_width + 2 * z.kv_width)), VMEM),
            (shape((z.all_rows, z.positions), I32), VMEM),
            (shape((z.plan_rows, LANES), I32), VMEM),
        ]
        + [(shape((z.per_rank,) + page), VMEM)] * (inst_count - 1)
        + [chunk],
        [
            pltpu.VMEM(qkv_first.shape, BF16),
            pltpu.VMEM(qkv_second.shape, BF16),
            smem(lengths.shape, I32),
            smem(page_table.shape, I32),
            smem(moves.shape, I32),
            smem(dest_pages.shape, I32),
            smem((z.plan_rows * LANES,), I32),
            dma((9,)),
        ],
        [w_hbm]
        + [
            in_hbm(x)
            for x in (kv_cache, lengths, page_table, moves, dest_pages, qkv_first, qkv_second)
        ]
        + [x for d in range(1, z.early) for x in have[d]],
    )
    outgoing, weights = more[:-1], more[-1:]
    for d in far:
        for e in range(1, d):
            have[d ^ e] = tuple(swap(behind(x, plan), e) for x in have[d])
    arrived = []
    for s in range(1, inst_count):
        arrived.append(
            lax.ppermute(outgoing[s - 1], "inst", [(i, i ^ s) for i in range(inst_count)])
        )

    send, acc, stats, _, _, kv_mid, *loaded = run(
        functools.partial(attend_kernel, z, (1,)),
        2,
        [HBM] + [VMEM] * (4 + 2 * (n - z.early)),
        [
            (shape((z.all_rows, z.packed)), VMEM),
            (shape((z.all_rows, z.part_width), F32), VMEM),
            (shape((z.all_rows, LANES), F32), VMEM),
            (shape(rows.shape), VMEM),
            (shape(pages.shape), VMEM),
            (shape(kv_cache.shape), HBM),
            chunk,
        ],
        [smem((z.plan_rows, LANES), I32), dma((3,))],
        [w_hbm, plan, visible, pages, rows] + [x for d in range(z.early, n) for x in have[d]],
        aliases={3: 4, 4: 3},
    )
    weights += loaded
    for d in stages[:-1]:
        theirs = swap(send, d)
        acc, stats, send = run(
            functools.partial(merge_kernel, z),
            0.2,
            [VMEM] * 3,
            [
                (shape((z.all_rows, z.part_width), F32), VMEM),
                (shape((z.all_rows, LANES), F32), VMEM),
                (shape((z.all_rows, z.packed)), VMEM),
            ],
            [],
            [acc, stats, theirs],
        )
    theirs = swap(send, stages[-1])
    weights += run(
        functools.partial(stage_kernel, (2, 3, 4)),
        3,
        [HBM],
        [chunk] * 3,
        [dma((3,))],
        [w_hbm],
        after=[stats],
    )
    (mixed,) = run(
        functools.partial(finish_kernel, z),
        0.3,
        [VMEM] * 3,
        [(shape((z.all_rows, z.part_width)), VMEM)],
        [],
        [acc, stats, theirs],
        after=weights[-1:],
    )
    other = swap(mixed, 1)
    total, *held = run(
        functools.partial(project_kernel, z, (5, 6)),
        3.4,
        [HBM] + [VMEM] * (1 + CHUNKS // 2),
        [(shape((z.all_rows, z.out_columns), F32), VMEM)] + [chunk] * 2,
        [dma((2,))],
        [w_hbm, mixed, *weights[:-1]],
    )
    held = weights[-1:] + held
    return tuple(
        run(
            functools.partial(last_kernel, z, 3, (7,)),
            3.4,
            [HBM] + [VMEM] * (5 + inst_count) + [HBM],
            [(shape((rows_of, z.out_columns)), VMEM)] * 2 + [(shape(kv_cache.shape), HBM)],
            [
                pltpu.VMEM((1, z.chunk_rows, z.out_columns), BF16),
                pltpu.VMEM((z.all_rows, z.out_columns), F32),
                smem((z.plan_rows, LANES), I32),
                dma((3,)),
            ],
            [w_hbm, total, other, plan, *held, *arrived, kv_mid],
            aliases={6 + inst_count: 2},
            limit=12,
        )
    )


def solution(mesh):
    placed = (
        P(("groups", "inst"), "tp"),
        P(("groups", "inst"), "tp"),
        P(None, "tp"),
        P(("groups", "inst", "tp"), None, None, None),
        P("groups"),
        P(("groups", "inst"), None),
        P("groups", None),
        P("groups", None),
    )
    return jax.shard_map(
        steps,
        mesh=mesh,
        in_specs=placed,
        out_specs=(
            P(("groups", "inst"), "tp"),
            P(("groups", "inst"), "tp"),
            P(("groups", "inst", "tp"), None, None, None),
        ),
        check_vma=False,
    )
```

```python
import functools
import math

import jax
import jax.numpy as jnp
from jax import lax
from jax.experimental import pallas as pl
from jax.experimental.pallas import tpu as pltpu
from jax.sharding import PartitionSpec as P

HEAD_SIZE = 128
LANES = 128
NEG_LARGE = -1e30
BF16 = jnp.bfloat16
F32 = jnp.float32
I32 = jnp.int32
VMEM = pltpu.VMEM
HBM = pltpu.HBM
TILE = 512
WIDE = 1024
PARTS = 1
PREPARE = 0.05
UNITS = 16
READS = {
    "prepare": ((0, 2), (2, 2)),
    "attend": ((4, 1),),
    "stage": ((5, 3), (8, 3)),
    "project": ((11, 3),),
    "last": ((14, 2),),
}
FLOPS = 3e8
BYTES = 0
copy_of = pltpu.make_async_copy


def spec(space):
    return pl.BlockSpec(memory_space=space)


def in_hbm(x):
    return pltpu.with_memory_space_constraint(x, HBM)


def shape(dims, dtype=BF16):
    return jax.ShapeDtypeStruct(dims, dtype)


def run(kernel, micros, ins, outs, scratch, args, aliases=None, after=(), limit=8):
    count = len(ins)

    def body(*refs):
        kernel(*refs[:count], *refs[count + len(after) :])

    ins = list(ins) + [pl.ANY] * len(after)
    args = list(args) + list(after)
    return pl.pallas_call(
        body,
        out_shape=tuple(s for s, _ in outs),
        in_specs=[spec(space) for space in ins],
        out_specs=tuple(spec(space) for _, space in outs),
        scratch_shapes=scratch,
        input_output_aliases=aliases or {},
        compiler_params=pltpu.CompilerParams(vmem_limit_bytes=limit << 20),
        cost_estimate=pl.CostEstimate(
            flops=int(micros * FLOPS), bytes_accessed=int(micros * BYTES), transcendentals=0
        ),
    )(*args)


def behind(x, token):
    return lax.optimization_barrier((x, token))[0]


def rounded_up(x, to):
    return -(-x // to) * to


class Sizes:
    def __init__(self, n, inst_count, rows_of, per_rank, kv_shape, w_shape):
        self.n = n
        self.inst_count = inst_count
        self.rows_of = rows_of
        self.per_rank = per_rank
        self.pool, _, self.extent, self.kv_width = kv_shape
        self.q_width, self.out_columns = w_shape
        self.q_heads = self.q_width // HEAD_SIZE
        self.kv_heads = self.kv_width // HEAD_SIZE
        self.group = self.q_heads // self.kv_heads
        self.step_rows = rounded_up(rows_of, 8)
        self.all_rows = 2 * self.step_rows
        self.positions = self.pool * self.extent
        self.part_groups = self.kv_heads // (2 * PARTS)
        self.part_heads = self.part_groups * self.group
        self.part_width = self.part_heads * HEAD_SIZE
        self.per_tile = LANES // (2 * self.part_heads)
        self.packed = self.part_width + LANES * -(-3 // self.per_tile)
        self.unit_rows = self.q_width // UNITS
        self.early = 2
        while self.early * (self.q_width + 2 * self.kv_width) < n * 2 * self.kv_width:
            self.early *= 2
        self.at_offset = 2 * rows_of
        self.at_source = 4 * rows_of
        self.at_place = self.at_source + self.pool
        self.plan_rows = rounded_up(
            -(-(self.at_place + (inst_count - 1) * per_rank) // LANES), 8
        )


def w_copies(w_hbm, reads, refs, sems, first=0):
    rows = w_hbm.shape[0] // UNITS
    side = lax.rem(lax.axis_index("tp"), 2)
    copies = []
    for i, (unit, count) in enumerate(reads):
        half = side if unit < UNITS // 2 else 1 - side
        start = half * (w_hbm.shape[0] // 2) + (unit % (UNITS // 2)) * rows
        source = w_hbm.at[pl.ds(pl.multiple_of(start, LANES), count * rows)]
        copies.append(copy_of(source, refs[i], sems.at[first + i]))
    return copies


def prepare_kernel(z, chunks, *refs):
    m = 2 * z.early
    w_hbm, kv_hbm, lengths_hbm, table_hbm, moves_hbm, dest_hbm, first_hbm, second_hbm = refs[:8]
    pieces = (None, None) + refs[8 : 6 + m]
    pages, rows, visible_ref, plan_ref = refs[6 + m : 10 + m]
    outgoing = refs[10 + m : 9 + m + z.inst_count]
    w_refs = refs[9 + m + z.inst_count : 9 + m + z.inst_count + len(chunks)]
    first, second, lengths, table, moves, dest, plan, sems = refs[9 + m + z.inst_count + len(chunks) :]
    me = lax.axis_index("tp")
    inst = lax.axis_index("inst")
    small = [
        copy_of(table_hbm, table, sems.at[1]),
        copy_of(moves_hbm, moves, sems.at[2]),
        copy_of(lengths_hbm, lengths, sems.at[0]),
        copy_of(dest_hbm, dest, sems.at[3]),
    ]
    own = [copy_of(first_hbm, first, sems.at[5]), copy_of(second_hbm, second, sems.at[6])]
    kv_copy = copy_of(kv_hbm, pages.at[pl.ds(0, z.pool)], sems.at[4])
    w_loads = w_copies(w_hbm, chunks, w_refs, sems, 8)
    for copy in small + own + [kv_copy] + w_loads[:1]:
        copy.start()
    pages[z.pool] = jnp.zeros_like(pages[z.pool])
    rows[...] = jnp.zeros_like(rows)
    for copy in small:
        copy.wait()

    def sends(i, act):
        request = moves[0, i]
        origin = lax.div(request, z.rows_of)
        slot = lax.bitwise_xor(moves[1, i], origin)
        row = request - inst * z.rows_of
        for s in range(1, z.inst_count):

            @pl.when((origin == inst) & (slot == s))
            def _():
                for j in range(z.per_rank):
                    local = table[row, me + z.n * j] - me * z.pool
                    act(copy_of(kv_hbm.at[local], outgoing[s - 1].at[j], sems.at[7]))

    for i in range(moves.shape[1]):
        sends(i, lambda copy: copy.start())
    for copy in w_loads[1:]:
        copy.start()

    grid = (z.all_rows, z.positions)
    at = lax.broadcasted_iota(I32, grid, 1)
    row = lax.broadcasted_iota(I32, grid, 0)
    step = lax.div(row, z.step_rows)
    row_of = row - step * z.step_rows
    page_of = lax.div(at, z.extent)
    offset = at - page_of * z.extent
    newest = jnp.full(grid, -1, I32)
    place = jnp.full(grid, 1 << 30, I32)
    for r in range(z.rows_of):
        here = row_of == r
        newest = jnp.where(here, lengths[inst * z.rows_of + r], newest)
        for j in range(z.per_rank):
            number = me + z.n * j
            local = table[r, number] - me * z.pool
            place = jnp.where(here & (page_of == local), number * z.extent + offset, place)
    visible_ref[...] = (place <= newest + step).astype(I32)

    for k in range(2):
        for r in range(z.rows_of):
            position = lengths[inst * z.rows_of + r] + k
            local = table[r, lax.div(position, z.extent)] - me * z.pool
            mine = (local >= 0) & (local < z.pool)
            plan[k * z.rows_of + r] = jnp.where(mine, local, z.pool + 1)
            plan[z.at_offset + k * z.rows_of + r] = lax.rem(position, z.extent)
    for p in range(z.pool):
        plan[z.at_source + p] = p
    for k in range((z.inst_count - 1) * z.per_rank):
        plan[z.at_place + k] = -1
    for i in range(moves.shape[1]):
        request = moves[0, i]
        target = moves[1, i]
        origin = lax.div(request, z.rows_of)
        slot = lax.bitwise_xor(target, origin)

        @pl.when((origin == inst) & (slot > 0))
        def _():
            for j in range(z.per_rank):
                local = table[request - inst * z.rows_of, me + z.n * j] - me * z.pool
                plan[z.at_source + local] = z.pool

        @pl.when((target == inst) & (slot > 0))
        def _():
            for j in range(z.per_rank):
                plan[z.at_place + (slot - 1) * z.per_rank + j] = dest[i, me + z.n * j] - me * z.pool

    where = lax.broadcasted_iota(I32, plan_ref.shape, 0) * LANES + lax.broadcasted_iota(
        I32, plan_ref.shape, 1
    )
    packed = jnp.zeros(plan_ref.shape, I32)
    for k in range(z.at_place + (z.inst_count - 1) * z.per_rank):
        packed = jnp.where(where == k, plan[k], packed)
    plan_ref[...] = packed

    for copy in own:
        copy.wait()
    put_pieces(z, rows, range(z.early), (first, second) + pieces[2:])
    fresh = rows[:, z.q_width :].astype(F32)
    line_id = lax.broadcasted_iota(I32, fresh.shape, 0)
    row_id = lax.broadcasted_iota(I32, (z.extent, z.kv_width), 0)
    for i in range(moves.shape[1]):
        sends(i, lambda copy: copy.wait())
    for i in range(moves.shape[1]):
        request = moves[0, i]
        origin = lax.div(request, z.rows_of)
        slot = lax.bitwise_xor(moves[1, i], origin)
        r = request - inst * z.rows_of
        for s in range(1, z.inst_count):

            @pl.when((origin == inst) & (slot == s) & (me >= z.n - 2))
            def _():
                for k in range(2):
                    position = lengths[request] + k
                    number = lax.div(position, z.extent)
                    chosen = line_id == k * z.step_rows + r
                    new = jnp.sum(jnp.where(chosen, fresh, 0.0), axis=0, keepdims=True)
                    target = jnp.where(
                        number == me + z.n * (z.per_rank - 1), lax.rem(position, z.extent), -1
                    )
                    for kv in range(2):
                        old = outgoing[s - 1][z.per_rank - 1, kv].astype(F32)
                        outgoing[s - 1][z.per_rank - 1, kv] = jnp.where(
                            row_id == target, new[:, kv * z.kv_width : (kv + 1) * z.kv_width], old
                        ).astype(BF16)

    for copy in [kv_copy] + w_loads:
        copy.wait()


def put_pieces(z, rows, which, pieces):
    me = lax.axis_index("tp")
    width = pieces[0].shape[1]
    for i, d in enumerate(which):
        start = pl.multiple_of((me ^ d) * width, LANES)
        for k in range(2):
            rows[k * z.step_rows : k * z.step_rows + z.rows_of, pl.ds(start, width)] = pieces[
                2 * i + k
            ][...]


def read(plan, k):
    return plan[k // LANES, k % LANES]


def attend_part(z, part, rows, pages, visible, send_ref, keep_ref, stats_ref):
    side = lax.rem(lax.axis_index("tp"), 2)
    half = z.kv_heads // 2
    lane = lax.broadcasted_iota(I32, (z.all_rows, LANES), 1)
    scale = 1.0 / math.sqrt(HEAD_SIZE)
    stats = [jnp.zeros((z.all_rows, LANES), F32) for _ in range(2)]
    for i in range(2 * z.part_groups):
        kept, k = divmod(i, z.part_groups)
        g = (side if kept else 1 - side) * half + part * z.part_groups + k
        q = jnp.concatenate(
            [
                rows[:, pl.ds(pl.multiple_of((g * z.group + h) * HEAD_SIZE, LANES), HEAD_SIZE)]
                for h in range(z.group)
            ],
            axis=0,
        )
        columns = pl.ds(pl.multiple_of(g * HEAD_SIZE, LANES), HEAD_SIZE)
        keys = pages[0 : z.pool, 0, :, columns].reshape(z.positions, HEAD_SIZE)
        values = pages[0 : z.pool, 1, :, columns].reshape(z.positions, HEAD_SIZE)
        scores = lax.dot_general(q, keys, (((1,), (1,)), ((), ())), preferred_element_type=F32)
        scores = (scores * scale).reshape(z.group, z.all_rows, z.positions)
        scores = jnp.where(visible, scores, NEG_LARGE)
        top = jnp.max(scores, axis=2, keepdims=True)
        exponent = jnp.where(visible, jnp.exp(scores - top), 0.0)
        total = jnp.sum(exponent, axis=2, keepdims=True)
        summed = jnp.dot(
            exponent.astype(BF16).reshape(z.group * z.all_rows, z.positions),
            values,
            preferred_element_type=F32,
        )
        for h in range(z.group):
            head = k * z.group + h
            piece = summed[h * z.all_rows : (h + 1) * z.all_rows]
            out_columns = slice(head * HEAD_SIZE, (head + 1) * HEAD_SIZE)
            if kept:
                keep_ref[:, out_columns] = piece
            else:
                send_ref[:, out_columns] = piece.astype(BF16)
            stats[kept] = jnp.where(lane == head, top[h], stats[kept])
            stats[kept] = jnp.where(lane == z.part_heads + head, total[h], stats[kept])
    put_stats(z, send_ref, stats[0])
    stats_ref[...] = stats[1]


def put_stats(z, ref, stats):
    used = 2 * z.part_heads
    lane = lax.broadcasted_iota(I32, stats.shape, 1)
    rest = stats
    tiles = {}
    for k in range(3):
        term = rest.astype(BF16).astype(F32)
        rest = rest - term
        tile, at = divmod(k, z.per_tile)
        if at:
            term = jnp.where(lane < at * used, tiles[tile], pltpu.roll(term, at * used, 1))
        tiles[tile] = term
    for tile, value in tiles.items():
        start = z.part_width + tile * LANES
        ref[:, start : start + LANES] = value.astype(BF16)


def get_stats(z, ref):
    used = 2 * z.part_heads
    stats = 0.0
    for k in range(3):
        tile, at = divmod(k, z.per_tile)
        start = z.part_width + tile * LANES
        term = ref[:, start : start + LANES].astype(F32)
        stats += pltpu.roll(term, LANES - at * used, 1) if at else term
    lane = lax.broadcasted_iota(I32, stats.shape, 1)
    return jnp.where(lane < used, stats, 0.0)


def attend_kernel(z, chunks, *refs):
    m = 2 * (z.n - z.early)
    w_hbm, plan_vmem, visible_ref, _, _ = refs[:5]
    pieces = refs[5 : 5 + m]
    send_ref, keep_ref, stats_ref, rows, pages, kv_out = refs[5 + m : 11 + m]
    w_refs = refs[11 + m : 11 + m + len(chunks)]
    plan, sems = refs[11 + m + len(chunks) :]
    w_loads = w_copies(w_hbm, chunks, w_refs, sems, 2)
    for copy in w_loads:
        copy.start()
    plan_copy = copy_of(plan_vmem, plan, sems.at[0])
    plan_copy.start()
    put_pieces(z, rows, range(z.early, z.n), pieces)
    plan_copy.wait()

    fresh = rows[:, z.q_width :].astype(F32)
    row_id = lax.broadcasted_iota(I32, (z.extent, z.kv_width), 0)
    for k in range(2):
        for r in range(z.rows_of):
            slot = read(plan, k * z.rows_of + r)
            here = row_id == read(plan, z.at_offset + k * z.rows_of + r)
            line = k * z.step_rows + r
            for kv in range(2):
                new = fresh[line : line + 1, kv * z.kv_width : (kv + 1) * z.kv_width]
                old = pages[slot, kv].astype(F32)
                pages[slot, kv] = jnp.where(here, new, old).astype(BF16)

    writes = [
        copy_of(pages.at[read(plan, z.at_source + p)], kv_out.at[p], sems.at[1])
        for p in range(z.pool)
    ]
    for copy in writes:
        copy.start()
    visible = (visible_ref[...] > 0)[None]
    attend_part(z, 0, rows, pages, visible, send_ref, keep_ref, stats_ref)
    for copy in writes + w_loads:
        copy.wait()


def joined(z, acc_ref, stats_ref, other_ref):
    mine = stats_ref[...]
    theirs = get_stats(z, other_ref)
    lane = lax.broadcasted_iota(I32, mine.shape, 1)
    top = jnp.maximum(mine, theirs)
    scale_mine = jnp.exp(mine - top)
    scale_theirs = jnp.exp(theirs - top)
    total = mine * pltpu.roll(scale_mine, z.part_heads, 1) + theirs * pltpu.roll(
        scale_theirs, z.part_heads, 1
    )
    stats = jnp.where(
        lane < z.part_heads, top, jnp.where(lane < 2 * z.part_heads, total, 0.0)
    )
    for h in range(z.part_heads):
        columns = slice(h * HEAD_SIZE, (h + 1) * HEAD_SIZE)
        piece = acc_ref[:, columns] * scale_mine[:, h : h + 1] + other_ref[:, columns].astype(
            F32
        ) * scale_theirs[:, h : h + 1]
        yield columns, piece, stats, h


def merge_kernel(z, acc_ref, stats_ref, other_ref, acc_out, stats_out, send_ref):
    for columns, piece, stats, _ in joined(z, acc_ref, stats_ref, other_ref):
        acc_out[:, columns] = piece
        send_ref[:, columns] = piece.astype(BF16)
    stats_out[...] = stats
    put_stats(z, send_ref, stats)


def finish_kernel(z, acc_ref, stats_ref, other_ref, mixed_ref):
    for columns, piece, stats, h in joined(z, acc_ref, stats_ref, other_ref):
        total = stats[:, z.part_heads + h : z.part_heads + h + 1]
        mixed_ref[:, columns] = (piece / total).astype(BF16)


def stage_kernel(chunks, w_hbm, *refs):
    loads = w_copies(w_hbm, chunks, refs, refs[-1])
    for copy in loads:
        copy.start()
    for copy in loads:
        copy.wait()


def column_tiles(width, body, tile=TILE):
    tile = min(tile, width)

    @pl.loop(0, width // tile)
    def _(t):
        body(pl.ds(pl.multiple_of(t * tile, tile), tile))


def product(mixed, weights, columns, begin=0):
    total = None
    for w in weights:
        rows = w.shape[0]
        term = jnp.dot(mixed[:, begin : begin + rows], w[:, columns], preferred_element_type=F32)
        total = term if total is None else total + term
        begin += rows
    return total


def project_kernel(z, held, chunks, *refs):
    w_hbm, mixed = refs[:2]
    weights = refs[2 : 2 + held]
    acc_ref = refs[2 + held]
    loads = w_copies(w_hbm, chunks, refs[3 + held :], refs[-1])
    for copy in loads:
        copy.start()

    def body(columns):
        acc_ref[:, columns] = product(mixed, weights, columns)

    column_tiles(z.out_columns, body)
    for copy in loads:
        copy.wait()


def last_kernel(z, held, chunks, *refs):
    w_hbm, acc_in, mixed, plan_vmem = refs[:4]
    weights = refs[4 : 4 + held]
    arrived = refs[4 + held : 3 + held + z.inst_count]
    first_ref, second_ref, kv_out, late, acc, plan, sems = refs[4 + held + z.inst_count :]
    plan_copy = copy_of(plan_vmem, plan, sems.at[0])
    plan_copy.start()
    (load,) = w_copies(w_hbm, chunks, [late], sems, 2)
    load.start()

    def placed(act):
        for s in range(z.inst_count - 1):
            for j in range(z.per_rank):
                slot = read(plan, z.at_place + s * z.per_rank + j)

                @pl.when(slot >= 0)
                def _():
                    act(copy_of(arrived[s].at[j], kv_out.at[slot], sems.at[1]))

    def early(columns):
        acc[:, columns] = acc_in[:, columns] + product(mixed, weights, columns)

    column_tiles(z.out_columns, early)
    plan_copy.wait()
    placed(lambda copy: copy.start())
    load.wait()

    def body(columns):
        begin = mixed.shape[1] - late.shape[0]
        total = acc[:, columns] + product(mixed, [late], columns, begin)
        first_ref[:, columns] = total[: z.rows_of].astype(BF16)
        second_ref[:, columns] = total[z.step_rows : z.step_rows + z.rows_of].astype(BF16)

    column_tiles(z.out_columns, body, WIDE)
    placed(lambda copy: copy.wait())


def steps(qkv_first, qkv_second, w_out, kv_cache, lengths, page_table, moves, dest_pages):
    n = lax.axis_size("tp")
    inst_count = lax.axis_size("inst")
    moves = moves.T
    rows_of, max_pages = page_table.shape
    z = Sizes(n, inst_count, rows_of, max_pages // n, kv_cache.shape, w_out.shape)
    smem = pltpu.SMEM
    dma = pltpu.SemaphoreType.DMA
    page = kv_cache.shape[1:]

    def swap(x, d):
        return lax.ppermute(x, "tp", [(i, i ^ d) for i in range(n)])

    stages = []
    while (1 << len(stages)) < n:
        stages.append(1 << len(stages))

    w_hbm = in_hbm(w_out)
    parts = {
        name: [(shape((count * z.unit_rows, z.out_columns)), VMEM) for _, count in reads]
        for name, reads in READS.items()
    }
    have = {0: (qkv_first, qkv_second)}
    for d in range(1, z.early):
        have[d] = tuple(swap(x, d) for x in have[0])
    far = [d for d in stages if d >= z.early]
    for d in far:
        have[d] = tuple(swap(x, d) for x in have[0])
    pages, rows, visible, plan, *more = run(
        functools.partial(prepare_kernel, z, READS["prepare"]),
        PREPARE,
        [HBM] * 8 + [VMEM] * (2 * z.early - 2),
        [
            (shape((z.pool + 2,) + page), VMEM),
            (shape((z.all_rows, z.q_width + 2 * z.kv_width)), VMEM),
            (shape((z.all_rows, z.positions), I32), VMEM),
            (shape((z.plan_rows, LANES), I32), VMEM),
        ]
        + [(shape((z.per_rank,) + page), VMEM)] * (inst_count - 1)
        + parts["prepare"],
        [
            pltpu.VMEM(qkv_first.shape, BF16),
            pltpu.VMEM(qkv_second.shape, BF16),
            smem(lengths.shape, I32),
            smem(page_table.shape, I32),
            smem(moves.shape, I32),
            smem(dest_pages.shape, I32),
            smem((z.plan_rows * LANES,), I32),
            dma((8 + len(READS["prepare"]),)),
        ],
        [w_hbm]
        + [
            in_hbm(x)
            for x in (kv_cache, lengths, page_table, moves, dest_pages, qkv_first, qkv_second)
        ]
        + [x for d in range(1, z.early) for x in have[d]],
    )
    outgoing, weights = more[: inst_count - 1], more[inst_count - 1 :]
    for d in far:
        for e in range(1, d):
            have[d ^ e] = tuple(swap(behind(x, plan), e) for x in have[d])
    arrived = []
    for s in range(1, inst_count):
        arrived.append(
            lax.ppermute(outgoing[s - 1], "inst", [(i, i ^ s) for i in range(inst_count)])
        )

    send, acc, stats, _, _, kv_mid, *loaded = run(
        functools.partial(attend_kernel, z, READS["attend"]),
        2,
        [HBM] + [VMEM] * (4 + 2 * (n - z.early)),
        [
            (shape((z.all_rows, z.packed)), VMEM),
            (shape((z.all_rows, z.part_width), F32), VMEM),
            (shape((z.all_rows, LANES), F32), VMEM),
            (shape(rows.shape), VMEM),
            (shape(pages.shape), VMEM),
            (shape(kv_cache.shape), HBM),
        ]
        + parts["attend"],
        [smem((z.plan_rows, LANES), I32), dma((2 + len(READS["attend"]),))],
        [w_hbm, plan, visible, pages, rows] + [x for d in range(z.early, n) for x in have[d]],
        aliases={3: 4, 4: 3},
    )
    weights += loaded
    for d in stages[:-1]:
        theirs = swap(send, d)
        acc, stats, send = run(
            functools.partial(merge_kernel, z),
            0.2,
            [VMEM] * 3,
            [
                (shape((z.all_rows, z.part_width), F32), VMEM),
                (shape((z.all_rows, LANES), F32), VMEM),
                (shape((z.all_rows, z.packed)), VMEM),
            ],
            [],
            [acc, stats, theirs],
        )
    theirs = swap(send, stages[-1])
    weights += run(
        functools.partial(stage_kernel, READS["stage"]),
        3,
        [HBM],
        parts["stage"],
        [dma((len(READS["stage"]),))],
        [w_hbm],
        after=[stats],
    )
    (mixed,) = run(
        functools.partial(finish_kernel, z),
        0.3,
        [VMEM] * 3,
        [(shape((z.all_rows, z.part_width)), VMEM)],
        [],
        [acc, stats, theirs],
        after=weights[-1:],
    )
    other = swap(mixed, 1)
    near, far = weights[:-1], weights[-1:]
    total, *held = run(
        functools.partial(project_kernel, z, len(near), READS["project"]),
        3,
        [HBM] + [VMEM] * (1 + len(near)),
        [(shape((z.all_rows, z.out_columns), F32), VMEM)] + parts["project"],
        [dma((len(READS["project"]),))],
        [w_hbm, mixed, *near],
    )
    held = far + held
    return tuple(
        run(
            functools.partial(last_kernel, z, len(held), READS["last"]),
            3.4,
            [HBM] + [VMEM] * (2 + len(held) + inst_count) + [HBM],
            [(shape((rows_of, z.out_columns)), VMEM)] * 2 + [(shape(kv_cache.shape), HBM)],
            [
                pltpu.VMEM(parts["last"][0][0].shape, BF16),
                pltpu.VMEM((z.all_rows, z.out_columns), F32),
                smem((z.plan_rows, LANES), I32),
                dma((3,)),
            ],
            [w_hbm, total, other, plan, *held, *arrived, kv_mid],
            aliases={3 + len(held) + inst_count: 2},
            limit=12,
        )
    )


def solution(mesh):
    placed = (
        P(("groups", "inst"), "tp"),
        P(("groups", "inst"), "tp"),
        P(None, "tp"),
        P(("groups", "inst", "tp"), None, None, None),
        P("groups"),
        P(("groups", "inst"), None),
        P("groups", None),
        P("groups", None),
    )
    return jax.shard_map(
        steps,
        mesh=mesh,
        in_specs=placed,
        out_specs=(
            P(("groups", "inst"), "tp"),
            P(("groups", "inst"), "tp"),
            P(("groups", "inst", "tp"), None, None, None),
        ),
        check_vma=False,
    )
```

```python
import functools
import math

import jax
import jax.numpy as jnp
from jax import lax
from jax.experimental import pallas as pl
from jax.experimental.pallas import tpu as pltpu
from jax.sharding import PartitionSpec as P

HEAD_SIZE = 128
LANES = 128
NEG_LARGE = -1e30
BF16 = jnp.bfloat16
F32 = jnp.float32
I32 = jnp.int32
VMEM = pltpu.VMEM
HBM = pltpu.HBM
TILE = 512
WIDE = 1024
PARTS = 1
PREPARE = 0.05
UNITS = 16
READS = {
    "prepare": ((0, 2), (2, 1)),
    "attend": ((3, 2),),
    "stage": ((5, 3), (8, 3)),
    "project": ((11, 3),),
    "last": ((14, 2),),
}
FLOPS = 3e8
BYTES = 0
copy_of = pltpu.make_async_copy


def spec(space):
    return pl.BlockSpec(memory_space=space)


def in_hbm(x):
    return pltpu.with_memory_space_constraint(x, HBM)


def shape(dims, dtype=BF16):
    return jax.ShapeDtypeStruct(dims, dtype)


def run(kernel, micros, ins, outs, scratch, args, aliases=None, after=(), limit=8):
    count = len(ins)

    def body(*refs):
        kernel(*refs[:count], *refs[count + len(after) :])

    ins = list(ins) + [pl.ANY] * len(after)
    args = list(args) + list(after)
    return pl.pallas_call(
        body,
        out_shape=tuple(s for s, _ in outs),
        in_specs=[spec(space) for space in ins],
        out_specs=tuple(spec(space) for _, space in outs),
        scratch_shapes=scratch,
        input_output_aliases=aliases or {},
        compiler_params=pltpu.CompilerParams(vmem_limit_bytes=limit << 20),
        cost_estimate=pl.CostEstimate(
            flops=int(micros * FLOPS), bytes_accessed=int(micros * BYTES), transcendentals=0
        ),
    )(*args)


def behind(x, token):
    return lax.optimization_barrier((x, token))[0]


def rounded_up(x, to):
    return -(-x // to) * to


class Sizes:
    def __init__(self, n, inst_count, rows_of, per_rank, kv_shape, w_shape):
        self.n = n
        self.inst_count = inst_count
        self.rows_of = rows_of
        self.per_rank = per_rank
        self.pool, _, self.extent, self.kv_width = kv_shape
        self.q_width, self.out_columns = w_shape
        self.q_heads = self.q_width // HEAD_SIZE
        self.kv_heads = self.kv_width // HEAD_SIZE
        self.group = self.q_heads // self.kv_heads
        self.step_rows = rounded_up(rows_of, 8)
        self.all_rows = 2 * self.step_rows
        self.positions = self.pool * self.extent
        self.part_groups = self.kv_heads // (2 * PARTS)
        self.part_heads = self.part_groups * self.group
        self.part_width = self.part_heads * HEAD_SIZE
        self.per_tile = LANES // (2 * self.part_heads)
        self.packed = self.part_width + LANES * -(-3 // self.per_tile)
        self.unit_rows = self.q_width // UNITS
        self.early = 2
        while self.early * (self.q_width + 2 * self.kv_width) < n * 2 * self.kv_width:
            self.early *= 2
        self.at_offset = 2 * rows_of
        self.at_source = 4 * rows_of
        self.at_place = self.at_source + self.pool
        self.plan_rows = rounded_up(
            -(-(self.at_place + (inst_count - 1) * per_rank) // LANES), 8
        )


def w_copies(w_hbm, reads, refs, sems, first=0):
    rows = w_hbm.shape[0] // UNITS
    side = lax.rem(lax.axis_index("tp"), 2)
    copies = []
    for i, (unit, count) in enumerate(reads):
        half = side if unit < UNITS // 2 else 1 - side
        start = half * (w_hbm.shape[0] // 2) + (unit % (UNITS // 2)) * rows
        source = w_hbm.at[pl.ds(pl.multiple_of(start, LANES), count * rows)]
        copies.append(copy_of(source, refs[i], sems.at[first + i]))
    return copies


def prepare_kernel(z, chunks, *refs):
    m = 2 * z.early
    w_hbm, kv_hbm, lengths_hbm, table_hbm, moves_hbm, dest_hbm, first_hbm, second_hbm = refs[:8]
    pieces = (None, None) + refs[8 : 6 + m]
    pages, rows, visible_ref, plan_ref = refs[6 + m : 10 + m]
    outgoing = refs[10 + m : 9 + m + z.inst_count]
    w_refs = refs[9 + m + z.inst_count : 9 + m + z.inst_count + len(chunks)]
    first, second, lengths, table, moves, dest, plan, sems = refs[9 + m + z.inst_count + len(chunks) :]
    me = lax.axis_index("tp")
    inst = lax.axis_index("inst")
    small = [
        copy_of(table_hbm, table, sems.at[1]),
        copy_of(moves_hbm, moves, sems.at[2]),
        copy_of(lengths_hbm, lengths, sems.at[0]),
        copy_of(dest_hbm, dest, sems.at[3]),
    ]
    own = [copy_of(first_hbm, first, sems.at[5]), copy_of(second_hbm, second, sems.at[6])]
    kv_copy = copy_of(kv_hbm, pages.at[pl.ds(0, z.pool)], sems.at[4])
    w_loads = w_copies(w_hbm, chunks, w_refs, sems, 8)
    for copy in small + own + [kv_copy] + w_loads[:1]:
        copy.start()
    pages[z.pool] = jnp.zeros_like(pages[z.pool])
    rows[...] = jnp.zeros_like(rows)
    for copy in small:
        copy.wait()

    def sends(i, act):
        request = moves[0, i]
        origin = lax.div(request, z.rows_of)
        slot = lax.bitwise_xor(moves[1, i], origin)
        row = request - inst * z.rows_of
        for s in range(1, z.inst_count):

            @pl.when((origin == inst) & (slot == s))
            def _():
                for j in range(z.per_rank):
                    local = table[row, me + z.n * j] - me * z.pool
                    act(copy_of(kv_hbm.at[local], outgoing[s - 1].at[j], sems.at[7]))

    for i in range(moves.shape[1]):
        sends(i, lambda copy: copy.start())
    for copy in w_loads[1:]:
        copy.start()

    grid = (z.all_rows, z.positions)
    at = lax.broadcasted_iota(I32, grid, 1)
    row = lax.broadcasted_iota(I32, grid, 0)
    step = lax.div(row, z.step_rows)
    row_of = row - step * z.step_rows
    page_of = lax.div(at, z.extent)
    offset = at - page_of * z.extent
    newest = jnp.full(grid, -1, I32)
    place = jnp.full(grid, 1 << 30, I32)
    for r in range(z.rows_of):
        here = row_of == r
        newest = jnp.where(here, lengths[inst * z.rows_of + r], newest)
        for j in range(z.per_rank):
            number = me + z.n * j
            local = table[r, number] - me * z.pool
            place = jnp.where(here & (page_of == local), number * z.extent + offset, place)
    visible_ref[...] = (place <= newest + step).astype(I32)

    for k in range(2):
        for r in range(z.rows_of):
            position = lengths[inst * z.rows_of + r] + k
            local = table[r, lax.div(position, z.extent)] - me * z.pool
            mine = (local >= 0) & (local < z.pool)
            plan[k * z.rows_of + r] = jnp.where(mine, local, z.pool + 1)
            plan[z.at_offset + k * z.rows_of + r] = lax.rem(position, z.extent)
    for p in range(z.pool):
        plan[z.at_source + p] = p
    for k in range((z.inst_count - 1) * z.per_rank):
        plan[z.at_place + k] = -1
    for i in range(moves.shape[1]):
        request = moves[0, i]
        target = moves[1, i]
        origin = lax.div(request, z.rows_of)
        slot = lax.bitwise_xor(target, origin)

        @pl.when((origin == inst) & (slot > 0))
        def _():
            for j in range(z.per_rank):
                local = table[request - inst * z.rows_of, me + z.n * j] - me * z.pool
                plan[z.at_source + local] = z.pool

        @pl.when((target == inst) & (slot > 0))
        def _():
            for j in range(z.per_rank):
                plan[z.at_place + (slot - 1) * z.per_rank + j] = dest[i, me + z.n * j] - me * z.pool

    where = lax.broadcasted_iota(I32, plan_ref.shape, 0) * LANES + lax.broadcasted_iota(
        I32, plan_ref.shape, 1
    )
    packed = jnp.zeros(plan_ref.shape, I32)
    for k in range(z.at_place + (z.inst_count - 1) * z.per_rank):
        packed = jnp.where(where == k, plan[k], packed)
    plan_ref[...] = packed

    for copy in own:
        copy.wait()
    put_pieces(z, rows, range(z.early), (first, second) + pieces[2:])
    fresh = rows[:, z.q_width :].astype(F32)
    line_id = lax.broadcasted_iota(I32, fresh.shape, 0)
    row_id = lax.broadcasted_iota(I32, (z.extent, z.kv_width), 0)
    for i in range(moves.shape[1]):
        sends(i, lambda copy: copy.wait())
    for i in range(moves.shape[1]):
        request = moves[0, i]
        origin = lax.div(request, z.rows_of)
        slot = lax.bitwise_xor(moves[1, i], origin)
        r = request - inst * z.rows_of
        for s in range(1, z.inst_count):

            @pl.when((origin == inst) & (slot == s) & (me >= z.n - 2))
            def _():
                for k in range(2):
                    position = lengths[request] + k
                    number = lax.div(position, z.extent)
                    chosen = line_id == k * z.step_rows + r
                    new = jnp.sum(jnp.where(chosen, fresh, 0.0), axis=0, keepdims=True)
                    target = jnp.where(
                        number == me + z.n * (z.per_rank - 1), lax.rem(position, z.extent), -1
                    )
                    for kv in range(2):
                        old = outgoing[s - 1][z.per_rank - 1, kv].astype(F32)
                        outgoing[s - 1][z.per_rank - 1, kv] = jnp.where(
                            row_id == target, new[:, kv * z.kv_width : (kv + 1) * z.kv_width], old
                        ).astype(BF16)

    for copy in [kv_copy] + w_loads:
        copy.wait()


def put_pieces(z, rows, which, pieces):
    me = lax.axis_index("tp")
    width = pieces[0].shape[1]
    for i, d in enumerate(which):
        start = pl.multiple_of((me ^ d) * width, LANES)
        for k in range(2):
            rows[k * z.step_rows : k * z.step_rows + z.rows_of, pl.ds(start, width)] = pieces[
                2 * i + k
            ][...]


def read(plan, k):
    return plan[k // LANES, k % LANES]


def attend_part(z, part, rows, pages, visible, send_ref, keep_ref, stats_ref):
    side = lax.rem(lax.axis_index("tp"), 2)
    half = z.kv_heads // 2
    lane = lax.broadcasted_iota(I32, (z.all_rows, LANES), 1)
    scale = 1.0 / math.sqrt(HEAD_SIZE)
    stats = [jnp.zeros((z.all_rows, LANES), F32) for _ in range(2)]
    for i in range(2 * z.part_groups):
        kept, k = divmod(i, z.part_groups)
        g = (side if kept else 1 - side) * half + part * z.part_groups + k
        q = jnp.concatenate(
            [
                rows[:, pl.ds(pl.multiple_of((g * z.group + h) * HEAD_SIZE, LANES), HEAD_SIZE)]
                for h in range(z.group)
            ],
            axis=0,
        )
        columns = pl.ds(pl.multiple_of(g * HEAD_SIZE, LANES), HEAD_SIZE)
        keys = pages[0 : z.pool, 0, :, columns].reshape(z.positions, HEAD_SIZE)
        values = pages[0 : z.pool, 1, :, columns].reshape(z.positions, HEAD_SIZE)
        scores = lax.dot_general(q, keys, (((1,), (1,)), ((), ())), preferred_element_type=F32)
        scores = (scores * scale).reshape(z.group, z.all_rows, z.positions)
        scores = jnp.where(visible, scores, NEG_LARGE)
        top = jnp.max(scores, axis=2, keepdims=True)
        exponent = jnp.where(visible, jnp.exp(scores - top), 0.0)
        total = jnp.sum(exponent, axis=2, keepdims=True)
        summed = jnp.dot(
            exponent.astype(BF16).reshape(z.group * z.all_rows, z.positions),
            values,
            preferred_element_type=F32,
        )
        for h in range(z.group):
            head = k * z.group + h
            piece = summed[h * z.all_rows : (h + 1) * z.all_rows]
            out_columns = slice(head * HEAD_SIZE, (head + 1) * HEAD_SIZE)
            if kept:
                keep_ref[:, out_columns] = piece
            else:
                send_ref[:, out_columns] = piece.astype(BF16)
            stats[kept] = jnp.where(lane == head, top[h], stats[kept])
            stats[kept] = jnp.where(lane == z.part_heads + head, total[h], stats[kept])
    put_stats(z, send_ref, stats[0])
    stats_ref[...] = stats[1]


def put_stats(z, ref, stats):
    used = 2 * z.part_heads
    lane = lax.broadcasted_iota(I32, stats.shape, 1)
    rest = stats
    tiles = {}
    for k in range(3):
        term = rest.astype(BF16).astype(F32)
        rest = rest - term
        tile, at = divmod(k, z.per_tile)
        if at:
            term = jnp.where(lane < at * used, tiles[tile], pltpu.roll(term, at * used, 1))
        tiles[tile] = term
    for tile, value in tiles.items():
        start = z.part_width + tile * LANES
        ref[:, start : start + LANES] = value.astype(BF16)


def get_stats(z, ref):
    used = 2 * z.part_heads
    stats = 0.0
    for k in range(3):
        tile, at = divmod(k, z.per_tile)
        start = z.part_width + tile * LANES
        term = ref[:, start : start + LANES].astype(F32)
        stats += pltpu.roll(term, LANES - at * used, 1) if at else term
    lane = lax.broadcasted_iota(I32, stats.shape, 1)
    return jnp.where(lane < used, stats, 0.0)


def attend_kernel(z, chunks, *refs):
    m = 2 * (z.n - z.early)
    w_hbm, plan_vmem, visible_ref, _, _ = refs[:5]
    pieces = refs[5 : 5 + m]
    send_ref, keep_ref, stats_ref, rows, pages = refs[5 + m : 10 + m]
    w_refs = refs[10 + m : 10 + m + len(chunks)]
    plan, sems = refs[10 + m + len(chunks) :]
    w_loads = w_copies(w_hbm, chunks, w_refs, sems, 1)
    for copy in w_loads:
        copy.start()
    plan_copy = copy_of(plan_vmem, plan, sems.at[0])
    plan_copy.start()
    put_pieces(z, rows, range(z.early, z.n), pieces)
    plan_copy.wait()

    fresh = rows[:, z.q_width :].astype(F32)
    row_id = lax.broadcasted_iota(I32, (z.extent, z.kv_width), 0)
    for k in range(2):
        for r in range(z.rows_of):
            slot = read(plan, k * z.rows_of + r)
            here = row_id == read(plan, z.at_offset + k * z.rows_of + r)
            line = k * z.step_rows + r
            for kv in range(2):
                new = fresh[line : line + 1, kv * z.kv_width : (kv + 1) * z.kv_width]
                old = pages[slot, kv].astype(F32)
                pages[slot, kv] = jnp.where(here, new, old).astype(BF16)

    visible = (visible_ref[...] > 0)[None]
    attend_part(z, 0, rows, pages, visible, send_ref, keep_ref, stats_ref)
    for copy in w_loads:
        copy.wait()


def joined(z, acc_ref, stats_ref, other_ref):
    mine = stats_ref[...]
    theirs = get_stats(z, other_ref)
    lane = lax.broadcasted_iota(I32, mine.shape, 1)
    top = jnp.maximum(mine, theirs)
    scale_mine = jnp.exp(mine - top)
    scale_theirs = jnp.exp(theirs - top)
    total = mine * pltpu.roll(scale_mine, z.part_heads, 1) + theirs * pltpu.roll(
        scale_theirs, z.part_heads, 1
    )
    stats = jnp.where(
        lane < z.part_heads, top, jnp.where(lane < 2 * z.part_heads, total, 0.0)
    )
    for h in range(z.part_heads):
        columns = slice(h * HEAD_SIZE, (h + 1) * HEAD_SIZE)
        piece = acc_ref[:, columns] * scale_mine[:, h : h + 1] + other_ref[:, columns].astype(
            F32
        ) * scale_theirs[:, h : h + 1]
        yield columns, piece, stats, h


def merge_kernel(z, acc_ref, stats_ref, other_ref, acc_out, stats_out, send_ref):
    for columns, piece, stats, _ in joined(z, acc_ref, stats_ref, other_ref):
        acc_out[:, columns] = piece
        send_ref[:, columns] = piece.astype(BF16)
    stats_out[...] = stats
    put_stats(z, send_ref, stats)


def finish_kernel(z, acc_ref, stats_ref, other_ref, mixed_ref):
    for columns, piece, stats, h in joined(z, acc_ref, stats_ref, other_ref):
        total = stats[:, z.part_heads + h : z.part_heads + h + 1]
        mixed_ref[:, columns] = (piece / total).astype(BF16)


def stage_kernel(z, reads, *refs):
    w_hbm, pages, plan_vmem, kv_out = refs[:4]
    plan, sems = refs[4 + len(reads) :]
    plan_copy = copy_of(plan_vmem, plan, sems.at[0])
    plan_copy.start()
    copies = w_copies(w_hbm, reads, refs[4:], sems, 2)
    for copy in copies:
        copy.start()
    plan_copy.wait()
    for p in range(z.pool):
        write = copy_of(pages.at[read(plan, z.at_source + p)], kv_out.at[p], sems.at[1])
        write.start()
        copies.append(write)
    for copy in copies:
        copy.wait()


def column_tiles(width, body, tile=TILE):
    tile = min(tile, width)

    @pl.loop(0, width // tile)
    def _(t):
        body(pl.ds(pl.multiple_of(t * tile, tile), tile))


def product(mixed, weights, columns, begin=0):
    total = None
    for w in weights:
        rows = w.shape[0]
        term = jnp.dot(mixed[:, begin : begin + rows], w[:, columns], preferred_element_type=F32)
        total = term if total is None else total + term
        begin += rows
    return total


def project_kernel(z, held, chunks, *refs):
    w_hbm, mixed = refs[:2]
    weights = refs[2 : 2 + held]
    acc_ref = refs[2 + held]
    loads = w_copies(w_hbm, chunks, refs[3 + held :], refs[-1])
    for copy in loads:
        copy.start()

    def body(columns):
        acc_ref[:, columns] = product(mixed, weights, columns)

    column_tiles(z.out_columns, body)
    for copy in loads:
        copy.wait()


def last_kernel(z, held, chunks, *refs):
    w_hbm, acc_in, mixed, plan_vmem = refs[:4]
    weights = refs[4 : 4 + held]
    arrived = refs[4 + held : 3 + held + z.inst_count]
    first_ref, second_ref, kv_out, late, acc, plan, sems = refs[4 + held + z.inst_count :]
    plan_copy = copy_of(plan_vmem, plan, sems.at[0])
    plan_copy.start()
    (load,) = w_copies(w_hbm, chunks, [late], sems, 2)
    load.start()

    def placed(act):
        for s in range(z.inst_count - 1):
            for j in range(z.per_rank):
                slot = read(plan, z.at_place + s * z.per_rank + j)

                @pl.when(slot >= 0)
                def _():
                    act(copy_of(arrived[s].at[j], kv_out.at[slot], sems.at[1]))

    def first_product(columns):
        acc[:, columns] = acc_in[:, columns] + product(mixed, weights[:1], columns)

    def next_product(columns):
        acc[:, columns] += product(mixed, weights[1:], columns, weights[0].shape[0])

    column_tiles(z.out_columns, first_product)
    plan_copy.wait()
    placed(lambda copy: copy.start())
    column_tiles(z.out_columns, next_product)
    load.wait()

    def body(columns):
        begin = mixed.shape[1] - late.shape[0]
        total = acc[:, columns] + product(mixed, [late], columns, begin)
        first_ref[:, columns] = total[: z.rows_of].astype(BF16)
        second_ref[:, columns] = total[z.step_rows : z.step_rows + z.rows_of].astype(BF16)

    column_tiles(z.out_columns, body, WIDE)
    placed(lambda copy: copy.wait())


def steps(qkv_first, qkv_second, w_out, kv_cache, lengths, page_table, moves, dest_pages):
    n = lax.axis_size("tp")
    inst_count = lax.axis_size("inst")
    moves = moves.T
    rows_of, max_pages = page_table.shape
    z = Sizes(n, inst_count, rows_of, max_pages // n, kv_cache.shape, w_out.shape)
    smem = pltpu.SMEM
    dma = pltpu.SemaphoreType.DMA
    page = kv_cache.shape[1:]

    def swap(x, d):
        return lax.ppermute(x, "tp", [(i, i ^ d) for i in range(n)])

    stages = []
    while (1 << len(stages)) < n:
        stages.append(1 << len(stages))

    w_hbm = in_hbm(w_out)
    parts = {
        name: [(shape((count * z.unit_rows, z.out_columns)), VMEM) for _, count in reads]
        for name, reads in READS.items()
    }
    have = {0: (qkv_first, qkv_second)}
    for d in range(1, z.early):
        have[d] = tuple(swap(x, d) for x in have[0])
    far = [d for d in stages if d >= z.early]
    for d in far:
        have[d] = tuple(swap(x, d) for x in have[0])
    pages, rows, visible, plan, *more = run(
        functools.partial(prepare_kernel, z, READS["prepare"]),
        PREPARE,
        [HBM] * 8 + [VMEM] * (2 * z.early - 2),
        [
            (shape((z.pool + 2,) + page), VMEM),
            (shape((z.all_rows, z.q_width + 2 * z.kv_width)), VMEM),
            (shape((z.all_rows, z.positions), I32), VMEM),
            (shape((z.plan_rows, LANES), I32), VMEM),
        ]
        + [(shape((z.per_rank,) + page), VMEM)] * (inst_count - 1)
        + parts["prepare"],
        [
            pltpu.VMEM(qkv_first.shape, BF16),
            pltpu.VMEM(qkv_second.shape, BF16),
            smem(lengths.shape, I32),
            smem(page_table.shape, I32),
            smem(moves.shape, I32),
            smem(dest_pages.shape, I32),
            smem((z.plan_rows * LANES,), I32),
            dma((8 + len(READS["prepare"]),)),
        ],
        [w_hbm]
        + [
            in_hbm(x)
            for x in (kv_cache, lengths, page_table, moves, dest_pages, qkv_first, qkv_second)
        ]
        + [x for d in range(1, z.early) for x in have[d]],
    )
    outgoing, weights = more[: inst_count - 1], more[inst_count - 1 :]
    for d in far:
        for e in range(1, d):
            have[d ^ e] = tuple(swap(behind(x, plan), e) for x in have[d])
    arrived = []
    for s in range(1, inst_count):
        arrived.append(
            lax.ppermute(outgoing[s - 1], "inst", [(i, i ^ s) for i in range(inst_count)])
        )

    send, acc, stats, _, pages, *loaded = run(
        functools.partial(attend_kernel, z, READS["attend"]),
        2,
        [HBM] + [VMEM] * (4 + 2 * (n - z.early)),
        [
            (shape((z.all_rows, z.packed)), VMEM),
            (shape((z.all_rows, z.part_width), F32), VMEM),
            (shape((z.all_rows, LANES), F32), VMEM),
            (shape(rows.shape), VMEM),
            (shape(pages.shape), VMEM),
        ]
        + parts["attend"],
        [smem((z.plan_rows, LANES), I32), dma((1 + len(READS["attend"]),))],
        [w_hbm, plan, visible, pages, rows] + [x for d in range(z.early, n) for x in have[d]],
        aliases={3: 4, 4: 3},
    )
    weights += loaded
    for d in stages[:-1]:
        theirs = swap(send, d)
        acc, stats, send = run(
            functools.partial(merge_kernel, z),
            0.2,
            [VMEM] * 3,
            [
                (shape((z.all_rows, z.part_width), F32), VMEM),
                (shape((z.all_rows, LANES), F32), VMEM),
                (shape((z.all_rows, z.packed)), VMEM),
            ],
            [],
            [acc, stats, theirs],
        )
    theirs = swap(send, stages[-1])
    kv_mid, *loaded = run(
        functools.partial(stage_kernel, z, READS["stage"]),
        3,
        [HBM, VMEM, VMEM],
        [(shape(kv_cache.shape), HBM)] + parts["stage"],
        [smem((z.plan_rows, LANES), I32), dma((2 + len(READS["stage"]),))],
        [w_hbm, pages, plan],
        after=[stats],
    )
    weights += loaded
    (mixed,) = run(
        functools.partial(finish_kernel, z),
        0.3,
        [VMEM] * 3,
        [(shape((z.all_rows, z.part_width)), VMEM)],
        [],
        [acc, stats, theirs],
        after=weights[-1:],
    )
    other = swap(mixed, 1)
    near, far = weights[:-1], weights[-1:]
    total, *held = run(
        functools.partial(project_kernel, z, len(near), READS["project"]),
        3,
        [HBM] + [VMEM] * (1 + len(near)),
        [(shape((z.all_rows, z.out_columns), F32), VMEM)] + parts["project"],
        [dma((len(READS["project"]),))],
        [w_hbm, mixed, *near],
    )
    held = far + held
    return tuple(
        run(
            functools.partial(last_kernel, z, len(held), READS["last"]),
            3.4,
            [HBM] + [VMEM] * (2 + len(held) + inst_count) + [HBM],
            [(shape((rows_of, z.out_columns)), VMEM)] * 2 + [(shape(kv_cache.shape), HBM)],
            [
                pltpu.VMEM(parts["last"][0][0].shape, BF16),
                pltpu.VMEM((z.all_rows, z.out_columns), F32),
                smem((z.plan_rows, LANES), I32),
                dma((3,)),
            ],
            [w_hbm, total, other, plan, *held, *arrived, kv_mid],
            aliases={3 + len(held) + inst_count: 2},
            limit=12,
        )
    )


def solution(mesh):
    placed = (
        P(("groups", "inst"), "tp"),
        P(("groups", "inst"), "tp"),
        P(None, "tp"),
        P(("groups", "inst", "tp"), None, None, None),
        P("groups"),
        P(("groups", "inst"), None),
        P("groups", None),
        P("groups", None),
    )
    return jax.shard_map(
        steps,
        mesh=mesh,
        in_specs=placed,
        out_specs=(
            P(("groups", "inst"), "tp"),
            P(("groups", "inst"), "tp"),
            P(("groups", "inst", "tp"), None, None, None),
        ),
        check_vma=False,
    )
```

```python
import functools
import math

import jax
import jax.numpy as jnp
from jax import lax
from jax.experimental import pallas as pl
from jax.experimental.pallas import tpu as pltpu
from jax.sharding import PartitionSpec as P

HEAD_SIZE = 128
LANES = 128
NEG_LARGE = -1e30
BF16 = jnp.bfloat16
F32 = jnp.float32
I32 = jnp.int32
VMEM = pltpu.VMEM
HBM = pltpu.HBM
TILE = 512
WIDE = 1024
PARTS = 1
PREPARE = 0.05
UNITS = 16
READS = {
    "prepare": ((0, 2), (2, 1)),
    "attend": ((3, 2),),
    "stage": ((5, 3), (8, 3)),
    "project": ((11, 3),),
    "last": ((14, 2),),
}
FLOPS = 3e8
BYTES = 0
copy_of = pltpu.make_async_copy


def spec(space):
    return pl.BlockSpec(memory_space=space)


def in_hbm(x):
    return pltpu.with_memory_space_constraint(x, HBM)


def shape(dims, dtype=BF16):
    return jax.ShapeDtypeStruct(dims, dtype)


def run(kernel, micros, ins, outs, scratch, args, aliases=None, after=(), limit=8):
    count = len(ins)

    def body(*refs):
        kernel(*refs[:count], *refs[count + len(after) :])

    ins = list(ins) + [pl.ANY] * len(after)
    args = list(args) + list(after)
    return pl.pallas_call(
        body,
        out_shape=tuple(s for s, _ in outs),
        in_specs=[spec(space) for space in ins],
        out_specs=tuple(spec(space) for _, space in outs),
        scratch_shapes=scratch,
        input_output_aliases=aliases or {},
        compiler_params=pltpu.CompilerParams(vmem_limit_bytes=limit << 20),
        cost_estimate=pl.CostEstimate(
            flops=int(micros * FLOPS), bytes_accessed=int(micros * BYTES), transcendentals=0
        ),
    )(*args)


def behind(x, token):
    return lax.optimization_barrier((x, token))[0]


def rounded_up(x, to):
    return -(-x // to) * to


class Sizes:
    def __init__(self, n, inst_count, rows_of, per_rank, kv_shape, w_shape):
        self.n = n
        self.inst_count = inst_count
        self.rows_of = rows_of
        self.per_rank = per_rank
        self.pool, _, self.extent, self.kv_width = kv_shape
        self.q_width, self.out_columns = w_shape
        self.q_heads = self.q_width // HEAD_SIZE
        self.kv_heads = self.kv_width // HEAD_SIZE
        self.group = self.q_heads // self.kv_heads
        self.step_rows = rounded_up(rows_of, 8)
        self.all_rows = 2 * self.step_rows
        self.positions = self.pool * self.extent
        self.part_groups = self.kv_heads // (2 * PARTS)
        self.part_heads = self.part_groups * self.group
        self.part_width = self.part_heads * HEAD_SIZE
        self.per_tile = LANES // (2 * self.part_heads)
        self.packed = self.part_width + LANES * -(-3 // self.per_tile)
        self.unit_rows = self.q_width // UNITS
        self.early = 2
        while self.early * (self.q_width + 2 * self.kv_width) < n * 2 * self.kv_width:
            self.early *= 2
        self.at_offset = 2 * rows_of
        self.at_source = 4 * rows_of
        self.at_place = self.at_source + self.pool
        self.plan_rows = rounded_up(
            -(-(self.at_place + (inst_count - 1) * per_rank) // LANES), 8
        )


def w_copies(w_hbm, reads, refs, sems, first=0):
    rows = w_hbm.shape[0] // UNITS
    side = lax.rem(lax.axis_index("tp"), 2)
    copies = []
    for i, (unit, count) in enumerate(reads):
        half = side if unit < UNITS // 2 else 1 - side
        start = half * (w_hbm.shape[0] // 2) + (unit % (UNITS // 2)) * rows
        source = w_hbm.at[pl.ds(pl.multiple_of(start, LANES), count * rows)]
        copies.append(copy_of(source, refs[i], sems.at[first + i]))
    return copies


def prepare_kernel(z, chunks, *refs):
    m = 2 * z.early
    w_hbm, kv_hbm, lengths_hbm, table_hbm, moves_hbm, dest_hbm, first_hbm, second_hbm = refs[:8]
    pieces = (None, None) + refs[8 : 6 + m]
    pages, rows, visible_ref, plan_ref = refs[6 + m : 10 + m]
    outgoing = refs[10 + m : 9 + m + z.inst_count]
    w_refs = refs[9 + m + z.inst_count : 9 + m + z.inst_count + len(chunks)]
    first, second, lengths, table, moves, dest, plan, sems = refs[9 + m + z.inst_count + len(chunks) :]
    me = lax.axis_index("tp")
    inst = lax.axis_index("inst")
    small = [
        copy_of(table_hbm, table, sems.at[1]),
        copy_of(moves_hbm, moves, sems.at[2]),
        copy_of(lengths_hbm, lengths, sems.at[0]),
        copy_of(dest_hbm, dest, sems.at[3]),
    ]
    own = [copy_of(first_hbm, first, sems.at[5]), copy_of(second_hbm, second, sems.at[6])]
    kv_copy = copy_of(kv_hbm, pages.at[pl.ds(0, z.pool)], sems.at[4])
    w_loads = w_copies(w_hbm, chunks, w_refs, sems, 8)
    for copy in small + own + [kv_copy] + w_loads[:1]:
        copy.start()
    pages[z.pool] = jnp.zeros_like(pages[z.pool])
    rows[...] = jnp.zeros_like(rows)
    for copy in small:
        copy.wait()

    def sends(i, act):
        request = moves[0, i]
        origin = lax.div(request, z.rows_of)
        slot = lax.bitwise_xor(moves[1, i], origin)
        row = request - inst * z.rows_of
        for s in range(1, z.inst_count):

            @pl.when((origin == inst) & (slot == s))
            def _():
                for j in range(z.per_rank):
                    local = table[row, me + z.n * j] - me * z.pool
                    act(copy_of(kv_hbm.at[local], outgoing[s - 1].at[j], sems.at[7]))

    for i in range(moves.shape[1]):
        sends(i, lambda copy: copy.start())
    for copy in w_loads[1:]:
        copy.start()

    grid = (z.all_rows, z.positions)
    at = lax.broadcasted_iota(I32, grid, 1)
    row = lax.broadcasted_iota(I32, grid, 0)
    step = lax.div(row, z.step_rows)
    row_of = row - step * z.step_rows
    page_of = lax.div(at, z.extent)
    offset = at - page_of * z.extent
    newest = jnp.full(grid, -1, I32)
    place = jnp.full(grid, 1 << 30, I32)
    for r in range(z.rows_of):
        here = row_of == r
        newest = jnp.where(here, lengths[inst * z.rows_of + r], newest)
        for j in range(z.per_rank):
            number = me + z.n * j
            local = table[r, number] - me * z.pool
            place = jnp.where(here & (page_of == local), number * z.extent + offset, place)
    visible_ref[...] = (place <= newest + step).astype(I32)

    for k in range(2):
        for r in range(z.rows_of):
            position = lengths[inst * z.rows_of + r] + k
            local = table[r, lax.div(position, z.extent)] - me * z.pool
            mine = (local >= 0) & (local < z.pool)
            plan[k * z.rows_of + r] = jnp.where(mine, local, z.pool + 1)
            plan[z.at_offset + k * z.rows_of + r] = lax.rem(position, z.extent)
    for p in range(z.pool):
        plan[z.at_source + p] = p
    for k in range((z.inst_count - 1) * z.per_rank):
        plan[z.at_place + k] = -1
    for i in range(moves.shape[1]):
        request = moves[0, i]
        target = moves[1, i]
        origin = lax.div(request, z.rows_of)
        slot = lax.bitwise_xor(target, origin)

        @pl.when((origin == inst) & (slot > 0))
        def _():
            for j in range(z.per_rank):
                local = table[request - inst * z.rows_of, me + z.n * j] - me * z.pool
                plan[z.at_source + local] = z.pool

        @pl.when((target == inst) & (slot > 0))
        def _():
            for j in range(z.per_rank):
                plan[z.at_place + (slot - 1) * z.per_rank + j] = dest[i, me + z.n * j] - me * z.pool

    where = lax.broadcasted_iota(I32, plan_ref.shape, 0) * LANES + lax.broadcasted_iota(
        I32, plan_ref.shape, 1
    )
    packed = jnp.zeros(plan_ref.shape, I32)
    for k in range(z.at_place + (z.inst_count - 1) * z.per_rank):
        packed = jnp.where(where == k, plan[k], packed)
    plan_ref[...] = packed

    for copy in own:
        copy.wait()
    put_pieces(z, rows, range(z.early), (first, second) + pieces[2:])
    fresh = rows[:, z.q_width :].astype(F32)
    line_id = lax.broadcasted_iota(I32, fresh.shape, 0)
    row_id = lax.broadcasted_iota(I32, (z.extent, z.kv_width), 0)
    for i in range(moves.shape[1]):
        sends(i, lambda copy: copy.wait())
    for i in range(moves.shape[1]):
        request = moves[0, i]
        origin = lax.div(request, z.rows_of)
        slot = lax.bitwise_xor(moves[1, i], origin)
        r = request - inst * z.rows_of
        for s in range(1, z.inst_count):

            @pl.when((origin == inst) & (slot == s) & (me >= z.n - 2))
            def _():
                for k in range(2):
                    position = lengths[request] + k
                    number = lax.div(position, z.extent)
                    chosen = line_id == k * z.step_rows + r
                    new = jnp.sum(jnp.where(chosen, fresh, 0.0), axis=0, keepdims=True)
                    target = jnp.where(
                        number == me + z.n * (z.per_rank - 1), lax.rem(position, z.extent), -1
                    )
                    for kv in range(2):
                        old = outgoing[s - 1][z.per_rank - 1, kv].astype(F32)
                        outgoing[s - 1][z.per_rank - 1, kv] = jnp.where(
                            row_id == target, new[:, kv * z.kv_width : (kv + 1) * z.kv_width], old
                        ).astype(BF16)

    for copy in [kv_copy] + w_loads:
        copy.wait()


def put_pieces(z, rows, which, pieces):
    me = lax.axis_index("tp")
    width = pieces[0].shape[1]
    for i, d in enumerate(which):
        start = pl.multiple_of((me ^ d) * width, LANES)
        for k in range(2):
            rows[k * z.step_rows : k * z.step_rows + z.rows_of, pl.ds(start, width)] = pieces[
                2 * i + k
            ][...]


def read(plan, k):
    return plan[k // LANES, k % LANES]


def attend_part(z, part, rows, pages, visible, send_ref, keep_ref, stats_ref):
    side = lax.rem(lax.axis_index("tp"), 2)
    half = z.kv_heads // 2
    lane = lax.broadcasted_iota(I32, (z.all_rows, LANES), 1)
    scale = 1.0 / math.sqrt(HEAD_SIZE)
    stats = [jnp.zeros((z.all_rows, LANES), F32) for _ in range(2)]
    for i in range(2 * z.part_groups):
        kept, k = divmod(i, z.part_groups)
        g = (side if kept else 1 - side) * half + part * z.part_groups + k
        q = jnp.concatenate(
            [
                rows[:, pl.ds(pl.multiple_of((g * z.group + h) * HEAD_SIZE, LANES), HEAD_SIZE)]
                for h in range(z.group)
            ],
            axis=0,
        )
        columns = pl.ds(pl.multiple_of(g * HEAD_SIZE, LANES), HEAD_SIZE)
        keys = pages[0 : z.pool, 0, :, columns].reshape(z.positions, HEAD_SIZE)
        values = pages[0 : z.pool, 1, :, columns].reshape(z.positions, HEAD_SIZE)
        scores = lax.dot_general(q, keys, (((1,), (1,)), ((), ())), preferred_element_type=F32)
        scores = (scores * scale).reshape(z.group, z.all_rows, z.positions)
        scores = jnp.where(visible, scores, NEG_LARGE)
        top = jnp.max(scores, axis=2, keepdims=True)
        exponent = jnp.where(visible, jnp.exp(scores - top), 0.0)
        total = jnp.sum(exponent, axis=2, keepdims=True)
        summed = jnp.dot(
            exponent.astype(BF16).reshape(z.group * z.all_rows, z.positions),
            values,
            preferred_element_type=F32,
        )
        for h in range(z.group):
            head = k * z.group + h
            piece = summed[h * z.all_rows : (h + 1) * z.all_rows]
            out_columns = slice(head * HEAD_SIZE, (head + 1) * HEAD_SIZE)
            if kept:
                keep_ref[:, out_columns] = piece
            else:
                send_ref[:, out_columns] = piece.astype(BF16)
            stats[kept] = jnp.where(lane == head, top[h], stats[kept])
            stats[kept] = jnp.where(lane == z.part_heads + head, total[h], stats[kept])
    put_stats(z, send_ref, stats[0])
    stats_ref[...] = stats[1]


def put_stats(z, ref, stats):
    used = 2 * z.part_heads
    lane = lax.broadcasted_iota(I32, stats.shape, 1)
    rest = stats
    tiles = {}
    for k in range(3):
        term = rest.astype(BF16).astype(F32)
        rest = rest - term
        tile, at = divmod(k, z.per_tile)
        if at:
            term = jnp.where(lane < at * used, tiles[tile], pltpu.roll(term, at * used, 1))
        tiles[tile] = term
    for tile, value in tiles.items():
        start = z.part_width + tile * LANES
        ref[:, start : start + LANES] = value.astype(BF16)


def get_stats(z, ref):
    used = 2 * z.part_heads
    stats = 0.0
    for k in range(3):
        tile, at = divmod(k, z.per_tile)
        start = z.part_width + tile * LANES
        term = ref[:, start : start + LANES].astype(F32)
        stats += pltpu.roll(term, LANES - at * used, 1) if at else term
    lane = lax.broadcasted_iota(I32, stats.shape, 1)
    return jnp.where(lane < used, stats, 0.0)


def attend_kernel(z, chunks, *refs):
    m = 2 * (z.n - z.early)
    w_hbm, plan_vmem, visible_ref, _, _ = refs[:5]
    pieces = refs[5 : 5 + m]
    send_ref, keep_ref, stats_ref, rows, pages = refs[5 + m : 10 + m]
    w_refs = refs[10 + m : 10 + m + len(chunks)]
    plan, sems = refs[10 + m + len(chunks) :]
    w_loads = w_copies(w_hbm, chunks, w_refs, sems, 1)
    for copy in w_loads:
        copy.start()
    plan_copy = copy_of(plan_vmem, plan, sems.at[0])
    plan_copy.start()
    put_pieces(z, rows, range(z.early, z.n), pieces)
    plan_copy.wait()

    fresh = rows[:, z.q_width :].astype(F32)
    row_id = lax.broadcasted_iota(I32, (z.extent, z.kv_width), 0)
    for k in range(2):
        for r in range(z.rows_of):
            slot = read(plan, k * z.rows_of + r)
            here = row_id == read(plan, z.at_offset + k * z.rows_of + r)
            line = k * z.step_rows + r
            for kv in range(2):
                new = fresh[line : line + 1, kv * z.kv_width : (kv + 1) * z.kv_width]
                old = pages[slot, kv].astype(F32)
                pages[slot, kv] = jnp.where(here, new, old).astype(BF16)

    visible = (visible_ref[...] > 0)[None]
    attend_part(z, 0, rows, pages, visible, send_ref, keep_ref, stats_ref)
    for copy in w_loads:
        copy.wait()


def joined(z, acc_ref, stats_ref, other_ref):
    mine = stats_ref[...]
    theirs = get_stats(z, other_ref)
    lane = lax.broadcasted_iota(I32, mine.shape, 1)
    top = jnp.maximum(mine, theirs)
    scale_mine = jnp.exp(mine - top)
    scale_theirs = jnp.exp(theirs - top)
    total = mine * pltpu.roll(scale_mine, z.part_heads, 1) + theirs * pltpu.roll(
        scale_theirs, z.part_heads, 1
    )
    stats = jnp.where(
        lane < z.part_heads, top, jnp.where(lane < 2 * z.part_heads, total, 0.0)
    )
    for h in range(z.part_heads):
        columns = slice(h * HEAD_SIZE, (h + 1) * HEAD_SIZE)
        piece = acc_ref[:, columns] * scale_mine[:, h : h + 1] + other_ref[:, columns].astype(
            F32
        ) * scale_theirs[:, h : h + 1]
        yield columns, piece, stats, h


def merge_kernel(z, acc_ref, stats_ref, other_ref, acc_out, stats_out, send_ref):
    for columns, piece, stats, _ in joined(z, acc_ref, stats_ref, other_ref):
        acc_out[:, columns] = piece
        send_ref[:, columns] = piece.astype(BF16)
    stats_out[...] = stats
    put_stats(z, send_ref, stats)


def finish_kernel(z, acc_ref, stats_ref, other_ref, mixed_ref):
    for columns, piece, stats, h in joined(z, acc_ref, stats_ref, other_ref):
        total = stats[:, z.part_heads + h : z.part_heads + h + 1]
        mixed_ref[:, columns] = (piece / total).astype(BF16)


def stage_kernel(z, reads, *refs):
    w_hbm, pages, plan_vmem, kv_out = refs[:4]
    plan, sems = refs[4 + len(reads) :]
    plan_copy = copy_of(plan_vmem, plan, sems.at[0])
    plan_copy.start()
    copies = w_copies(w_hbm, reads, refs[4:], sems, 2)
    for copy in copies:
        copy.start()
    plan_copy.wait()
    for p in range(z.pool):
        write = copy_of(pages.at[read(plan, z.at_source + p)], kv_out.at[p], sems.at[1])
        write.start()
        copies.append(write)
    for copy in copies:
        copy.wait()


def column_tiles(width, body, tile=TILE):
    tile = min(tile, width)

    @pl.loop(0, width // tile)
    def _(t):
        body(pl.ds(pl.multiple_of(t * tile, tile), tile))


def product(mixed, weights, columns, begin=0):
    total = None
    for w in weights:
        rows = w.shape[0]
        term = jnp.dot(mixed[:, begin : begin + rows], w[:, columns], preferred_element_type=F32)
        total = term if total is None else total + term
        begin += rows
    return total


def project_kernel(z, held, chunks, *refs):
    w_hbm, mixed = refs[:2]
    weights = refs[2 : 2 + held]
    acc_ref = refs[2 + held]
    loads = w_copies(w_hbm, chunks, refs[3 + held :], refs[-1])
    for copy in loads:
        copy.start()

    def body(columns):
        acc_ref[:, columns] = product(mixed, weights, columns)

    column_tiles(z.out_columns, body)
    for copy in loads:
        copy.wait()


def last_kernel(z, held, chunks, *refs):
    w_hbm, acc_in, mixed, plan_vmem = refs[:4]
    weights = refs[4 : 4 + held]
    arrived = refs[4 + held : 3 + held + z.inst_count]
    first_ref, second_ref, kv_out, late, acc, plan, sems = refs[4 + held + z.inst_count :]
    plan_copy = copy_of(plan_vmem, plan, sems.at[0])
    plan_copy.start()
    (load,) = w_copies(w_hbm, chunks, [late], sems, 2)
    load.start()

    def placed(act):
        for s in range(z.inst_count - 1):
            for j in range(z.per_rank):
                slot = read(plan, z.at_place + s * z.per_rank + j)

                @pl.when(slot >= 0)
                def _():
                    act(copy_of(arrived[s].at[j], kv_out.at[slot], sems.at[1]))

    def early(columns):
        acc[:, columns] = acc_in[:, columns] + product(mixed, weights, columns)

    column_tiles(z.out_columns, early, WIDE)
    plan_copy.wait()
    placed(lambda copy: copy.start())
    load.wait()

    def body(columns):
        begin = mixed.shape[1] - late.shape[0]
        total = acc[:, columns] + product(mixed, [late], columns, begin)
        first_ref[:, columns] = total[: z.rows_of].astype(BF16)
        second_ref[:, columns] = total[z.step_rows : z.step_rows + z.rows_of].astype(BF16)

    column_tiles(z.out_columns, body, 2 * WIDE)
    placed(lambda copy: copy.wait())


def steps(qkv_first, qkv_second, w_out, kv_cache, lengths, page_table, moves, dest_pages):
    n = lax.axis_size("tp")
    inst_count = lax.axis_size("inst")
    moves = moves.T
    rows_of, max_pages = page_table.shape
    z = Sizes(n, inst_count, rows_of, max_pages // n, kv_cache.shape, w_out.shape)
    smem = pltpu.SMEM
    dma = pltpu.SemaphoreType.DMA
    page = kv_cache.shape[1:]

    def swap(x, d):
        return lax.ppermute(x, "tp", [(i, i ^ d) for i in range(n)])

    stages = []
    while (1 << len(stages)) < n:
        stages.append(1 << len(stages))

    w_hbm = in_hbm(w_out)
    parts = {
        name: [(shape((count * z.unit_rows, z.out_columns)), VMEM) for _, count in reads]
        for name, reads in READS.items()
    }
    have = {0: (qkv_first, qkv_second)}
    for d in range(1, z.early):
        have[d] = tuple(swap(x, d) for x in have[0])
    far = [d for d in stages if d >= z.early]
    for d in far:
        have[d] = tuple(swap(x, d) for x in have[0])
    pages, rows, visible, plan, *more = run(
        functools.partial(prepare_kernel, z, READS["prepare"]),
        PREPARE,
        [HBM] * 8 + [VMEM] * (2 * z.early - 2),
        [
            (shape((z.pool + 2,) + page), VMEM),
            (shape((z.all_rows, z.q_width + 2 * z.kv_width)), VMEM),
            (shape((z.all_rows, z.positions), I32), VMEM),
            (shape((z.plan_rows, LANES), I32), VMEM),
        ]
        + [(shape((z.per_rank,) + page), VMEM)] * (inst_count - 1)
        + parts["prepare"],
        [
            pltpu.VMEM(qkv_first.shape, BF16),
            pltpu.VMEM(qkv_second.shape, BF16),
            smem(lengths.shape, I32),
            smem(page_table.shape, I32),
            smem(moves.shape, I32),
            smem(dest_pages.shape, I32),
            smem((z.plan_rows * LANES,), I32),
            dma((8 + len(READS["prepare"]),)),
        ],
        [w_hbm]
        + [
            in_hbm(x)
            for x in (kv_cache, lengths, page_table, moves, dest_pages, qkv_first, qkv_second)
        ]
        + [x for d in range(1, z.early) for x in have[d]],
    )
    outgoing, weights = more[: inst_count - 1], more[inst_count - 1 :]
    for d in far:
        for e in range(1, d):
            have[d ^ e] = tuple(swap(behind(x, plan), e) for x in have[d])
    arrived = []
    for s in range(1, inst_count):
        arrived.append(
            lax.ppermute(outgoing[s - 1], "inst", [(i, i ^ s) for i in range(inst_count)])
        )

    send, acc, stats, _, pages, *loaded = run(
        functools.partial(attend_kernel, z, READS["attend"]),
        2,
        [HBM] + [VMEM] * (4 + 2 * (n - z.early)),
        [
            (shape((z.all_rows, z.packed)), VMEM),
            (shape((z.all_rows, z.part_width), F32), VMEM),
            (shape((z.all_rows, LANES), F32), VMEM),
            (shape(rows.shape), VMEM),
            (shape(pages.shape), VMEM),
        ]
        + parts["attend"],
        [smem((z.plan_rows, LANES), I32), dma((1 + len(READS["attend"]),))],
        [w_hbm, plan, visible, pages, rows] + [x for d in range(z.early, n) for x in have[d]],
        aliases={3: 4, 4: 3},
    )
    weights += loaded
    for d in stages[:-1]:
        theirs = swap(send, d)
        acc, stats, send = run(
            functools.partial(merge_kernel, z),
            0.2,
            [VMEM] * 3,
            [
                (shape((z.all_rows, z.part_width), F32), VMEM),
                (shape((z.all_rows, LANES), F32), VMEM),
                (shape((z.all_rows, z.packed)), VMEM),
            ],
            [],
            [acc, stats, theirs],
        )
    theirs = swap(send, stages[-1])
    kv_mid, *loaded = run(
        functools.partial(stage_kernel, z, READS["stage"]),
        3,
        [HBM, VMEM, VMEM],
        [(shape(kv_cache.shape), HBM)] + parts["stage"],
        [smem((z.plan_rows, LANES), I32), dma((2 + len(READS["stage"]),))],
        [w_hbm, pages, plan],
        after=[stats],
    )
    weights += loaded
    (mixed,) = run(
        functools.partial(finish_kernel, z),
        0.3,
        [VMEM] * 3,
        [(shape((z.all_rows, z.part_width)), VMEM)],
        [],
        [acc, stats, theirs],
        after=weights[-1:],
    )
    other = swap(mixed, 1)
    near, far = weights[:-1], weights[-1:]
    total, *held = run(
        functools.partial(project_kernel, z, len(near), READS["project"]),
        3,
        [HBM] + [VMEM] * (1 + len(near)),
        [(shape((z.all_rows, z.out_columns), F32), VMEM)] + parts["project"],
        [dma((len(READS["project"]),))],
        [w_hbm, mixed, *near],
    )
    held = far + held
    return tuple(
        run(
            functools.partial(last_kernel, z, len(held), READS["last"]),
            3.4,
            [HBM] + [VMEM] * (2 + len(held) + inst_count) + [HBM],
            [(shape((rows_of, z.out_columns)), VMEM)] * 2 + [(shape(kv_cache.shape), HBM)],
            [
                pltpu.VMEM(parts["last"][0][0].shape, BF16),
                pltpu.VMEM((z.all_rows, z.out_columns), F32),
                smem((z.plan_rows, LANES), I32),
                dma((3,)),
            ],
            [w_hbm, total, other, plan, *held, *arrived, kv_mid],
            aliases={3 + len(held) + inst_count: 2},
            limit=12,
        )
    )


def solution(mesh):
    placed = (
        P(("groups", "inst"), "tp"),
        P(("groups", "inst"), "tp"),
        P(None, "tp"),
        P(("groups", "inst", "tp"), None, None, None),
        P("groups"),
        P(("groups", "inst"), None),
        P("groups", None),
        P("groups", None),
    )
    return jax.shard_map(
        steps,
        mesh=mesh,
        in_specs=placed,
        out_specs=(
            P(("groups", "inst"), "tp"),
            P(("groups", "inst"), "tp"),
            P(("groups", "inst", "tp"), None, None, None),
        ),
        check_vma=False,
    )
```
